32 devices in a mesh: col: 8 (over z, y), row: 4 (over x, core).
Axes of the slice: x: 2, y: 2, z: 4, core: 2. Of those that a mesh axis runs over, the one named last changes fastest.
Arguments:
- hyper_params: float32 [3], replicated
- w_in: float32 [4, 1024, 16384], P(None, 'row', 'col')
- x_in: bfloat16 [4, 1024, 1024], P(None, None, 'row')
- dy_in: bfloat16 [4, 1024, 16384], P(None, None, 'col')
- row_in: float32 [4, 1024], P(None, 'row')
- col_in: float32 [4, 16384], P(None, 'col')
- w_out: float32 [4, 16384, 1024], P(None, 'col', 'row')
- x_out: bfloat16 [4, 1024, 16384], P(None, None, 'col')
- dy_out: bfloat16 [4, 1024, 1024], P(None, None, 'row')
- row_out: float32 [4, 16384], P(None, 'col')
- col_out: float32 [4, 1024], P(None, 'row')
Outputs:
- output 1: float32 [4, 1024, 16384], P(None, 'row', 'col')
- output 2: float32 [4, 1024], P(None, 'row')
- output 3: float32 [4, 16384], P(None, 'col')
- output 4: float32 [4, 16384, 1024], P(None, 'col', 'row')
- output 5: float32 [4, 16384], P(None, 'col')
- output 6: float32 [4, 1024], P(None, 'row')
All inputs are finite; a program needn't handle non-finite values.
Results may differ from the reference program's by a relative error of at most 0.001.
Values are sent between devices in bfloat16 or wider.
A program may use at most 1 GiB of HBM per device.

```python
import jax
import jax.numpy as jnp
from jax import lax

LAYERS = 4
TOKENS = 1024
D_MODEL = 1024
D_FF = 16384
LATENT_RANK = 4
EPS_ONE = 1e-30
EPS_TWO = 1e-3
TWO_PI = 6.283185307179586


def profile(draw_key, length):
    phase_off = jax.random.uniform(draw_key, (LAYERS, LATENT_RANK, 1), jnp.float32) * TWO_PI
    freq_rank = (jnp.arange(LATENT_RANK) + 1).astype(jnp.float32)[None, :, None]
    position = (jnp.arange(length).astype(jnp.float32) / length)[None, None, :]
    return 1.0 + 0.9 * jnp.sin(TWO_PI * freq_rank * position + phase_off)


def draw_matrix(draw_key, n_rows, n_cols):
    sub_keys = jax.random.split(draw_key, 10)
    latent = jax.random.normal(sub_keys[0], (LAYERS, TOKENS, LATENT_RANK), jnp.float32)
    load_rows = jax.random.normal(sub_keys[1], (LAYERS, LATENT_RANK, n_rows), jnp.float32) * profile(sub_keys[2], n_rows)
    load_cols = jax.random.normal(sub_keys[3], (LAYERS, LATENT_RANK, n_cols), jnp.float32) * profile(sub_keys[4], n_cols)
    x_act = jnp.einsum('ltk,lkm->ltm', latent, load_rows) + jax.random.normal(sub_keys[5], (LAYERS, TOKENS, n_rows), jnp.float32)
    dy_act = (jnp.einsum('ltk,lkn->ltn', latent, load_cols) + jax.random.normal(sub_keys[6], (LAYERS, TOKENS, n_cols), jnp.float32)) / TOKENS
    w_mat = jax.random.normal(sub_keys[7], (LAYERS, n_rows, n_cols), jnp.float32) * n_rows ** -0.5
    row_stat = 6.0 * jnp.exp(0.5 * jax.random.normal(sub_keys[8], (LAYERS, n_rows), jnp.float32))
    col_stat = 6.0 * jnp.exp(0.5 * jax.random.normal(sub_keys[9], (LAYERS, n_cols), jnp.float32))
    return w_mat, x_act.astype(jnp.bfloat16), dy_act.astype(jnp.bfloat16), row_stat, col_stat


def setup_inputs(seed: int = 0) -> dict:
    sub_keys = jax.random.split(jax.random.key(seed), 3)
    low_end = jnp.array([0.5, 0.5, 0.2], dtype=jnp.float32)
    span_width = jnp.array([0.3, 0.5, 0.2], dtype=jnp.float32)
    hyper_params = low_end + span_width * jax.random.uniform(sub_keys[0], (3,), jnp.float32)
    w_in, x_in, dy_in, row_in, col_in = draw_matrix(sub_keys[1], D_MODEL, D_FF)
    w_out, x_out, dy_out, row_out, col_out = draw_matrix(sub_keys[2], D_FF, D_MODEL)
    return {'hyper_params': hyper_params, 'w_in': w_in, 'x_in': x_in, 'dy_in': dy_in, 'row_in': row_in, 'col_in': col_in, 'w_out': w_out, 'x_out': x_out, 'dy_out': dy_out, 'row_out': row_out, 'col_out': col_out}


def adafactor_one(w_mat, x_act, dy_act, row_old, col_old, hyper_params):
    beta_two = hyper_params[0]
    rho_step = hyper_params[1]
    clip_max = hyper_params[2]
    grad_mat = jnp.dot(x_act.T, dy_act, preferred_element_type=jnp.float32)
    sq_grad = grad_mat * grad_mat + EPS_ONE
    row_new = beta_two * row_old + (1.0 - beta_two) * jnp.mean(sq_grad, axis=1)
    col_new = beta_two * col_old + (1.0 - beta_two) * jnp.mean(sq_grad, axis=0)
    row_mean = jnp.mean(row_new)
    update = grad_mat * lax.rsqrt((row_new / row_mean)[:, None] * col_new[None, :])
    upd_rms = jnp.sqrt(jnp.mean(update * update))
    w_rms = jnp.sqrt(jnp.mean(w_mat * w_mat))
    step_size = rho_step * jnp.maximum(EPS_TWO, w_rms) / jnp.maximum(1.0, upd_rms / clip_max)
    return w_mat - step_size * update, row_new, col_new


def reference(hyper_params, w_in, x_in, dy_in, row_in, col_in, w_out, x_out, dy_out, row_out, col_out):
    def one_layer(layer_args):
        w_first, x_first, dy_first, row_first, col_first, w_second, x_second, dy_second, row_second, col_second = layer_args
        in_result = adafactor_one(w_first, x_first, dy_first, row_first, col_first, hyper_params)
        out_result = adafactor_one(w_second, x_second, dy_second, row_second, col_second, hyper_params)
        return in_result + out_result
    results = lax.map(one_layer, (w_in, x_in, dy_in, row_in, col_in, w_out, x_out, dy_out, row_out, col_out))
    return (results[0], results[1], results[2], results[3], results[4], results[5])
```

```python
import functools

import jax
import jax.numpy as jnp
from jax import lax
from jax.experimental import pallas as pl
from jax.experimental.pallas import tpu as pltpu
from jax.sharding import PartitionSpec as P

EPS_ONE = 1e-30
EPS_TWO = 1e-3
F32 = jnp.float32
BF16 = jnp.bfloat16
MESH = pl.DeviceIdType.MESH
LOOKAHEAD = 3
SLOTS = 4
GRANT = 24 * 2**20


def stats_kernel(dims, hp_hbm, w_in, x_in, dy_in, row_in, col_in, w_out, x_out, dy_out, row_out, col_out,
                 g_ref, wi_ref, wo_ref, sa_ref, sb_ref, fac_ref, na_ref, nb_ref,
                 hp_ref, small_ref, big_ref, xt_ref, acc_ref, rec_a, rec_b, rec_s, pay_ref,
                 old_ri, old_ci, old_ro, old_co,
                 load_sem, w_sem, old_sem, send_a, recv_a, send_b, recv_b, send_s, recv_s):
    n_col, n_row, layers, m_loc, n_loc, tokens, len_a, len_b = dims
    n_mat = 2 * layers
    n_dev = n_col * n_row
    my_col = lax.axis_index('col')
    my_row = lax.axis_index('row')
    me = my_col * n_row + my_row

    def load_copies(layer, part):
        slot = lax.rem(2 * layer + part, SLOTS)
        small = (x_in if part == 0 else dy_out).at[layer]
        big = (dy_in if part == 0 else x_out).at[layer]
        return (pltpu.make_async_copy(small, small_ref.at[slot], load_sem.at[slot, 0]),
                pltpu.make_async_copy(big, big_ref.at[slot], load_sem.at[slot, 1]))

    def w_copy(layer, part):
        if part == 0:
            return pltpu.make_async_copy(w_in.at[layer], wi_ref.at[layer], w_sem.at[layer, 0])
        return pltpu.make_async_copy(w_out.at[layer], wo_ref.at[layer], w_sem.at[layer, 1])

    def start_load(layer, part):
        for copy in load_copies(layer, part):
            copy.start()

    barrier = pltpu.get_barrier_semaphore()
    for idx in range(LOOKAHEAD):
        start_load(idx // 2, idx % 2)
    for step in range(1, n_dev):
        peer = lax.rem(me + step, n_dev)
        pl.semaphore_signal(barrier, inc=1, device_id=(peer // n_row, lax.rem(peer, n_row)), device_id_type=MESH)
    old_copies = [pltpu.make_async_copy(src, dst, old_sem.at[k]) for k, (src, dst) in enumerate(
        ((row_in, old_ri), (col_in, old_ci), (row_out, old_ro), (col_out, old_co), (hp_hbm, hp_ref)))]
    for copy in old_copies:
        copy.start()

    def a_copy(layer, step, sending):
        peer = lax.rem(my_col + step, n_col)
        slot = my_col if sending else lax.rem(my_col + n_col - step, n_col)
        return pltpu.make_async_remote_copy(
            rec_a.at[layer, slot], rec_a.at[layer, slot], send_a.at[layer, peer], recv_a.at[layer, slot],
            device_id=(peer, my_row), device_id_type=MESH)

    def b_copy(layer, step, sending):
        peer = lax.rem(my_row + step, n_row)
        slot = my_row if sending else lax.rem(my_row + n_row - step, n_row)
        return pltpu.make_async_remote_copy(
            rec_b.at[layer, slot], rec_b.at[layer, slot], send_b.at[layer, peer], recv_b.at[layer, slot],
            device_id=(my_col, peer), device_id_type=MESH)

    def s_copy(step, sending):
        peer = lax.rem(me + step, n_dev)
        slot = me if sending else lax.rem(me + n_dev - step, n_dev)
        return pltpu.make_async_remote_copy(
            rec_s.at[slot], rec_s.at[slot], send_s.at[peer], recv_s.at[slot],
            device_id=(peer // n_row, lax.rem(peer, n_row)), device_id_type=MESH)

    def ab_copies(layer, sending):
        return [b_copy(layer, step, sending) for step in range(1, n_row)] + [
            a_copy(layer, step, sending) for step in range(1, n_col)]

    def s_copies(sending):
        return [s_copy(step, sending) for step in range(1, n_dev)]

    lane = lax.broadcasted_iota(jnp.int32, (1, 128), 1)

    def put(section, mat, val):
        cols = pl.ds(128 * section, 128)
        pay_ref[:, cols] = jnp.where(lane == mat, val, pay_ref[:, cols])

    pay_ref[...] = jnp.zeros_like(pay_ref)

    def grad_part(layer, part):
        mat = 2 * layer + part
        slot = lax.rem(mat, SLOTS)
        for copy in load_copies(layer, part):
            copy.wait()
        xt_ref[...] = small_ref[slot].T
        for blk in range(n_loc // 256):
            cols = pl.ds(256 * blk, 256)
            grad = jnp.dot(xt_ref[...], big_ref[slot, :, cols], preferred_element_type=F32)
            g_ref[mat, :, cols] = grad
            sq = grad * grad
            rec_b[layer, my_row, :, pl.ds(n_loc * part + 256 * blk, 256)] = jnp.sum(sq, axis=0, keepdims=True)
            lanes = sq[:, :128] + sq[:, 128:]
            if blk == 0:
                acc_ref[...] = lanes
            else:
                acc_ref[...] += lanes
        rec_a[layer, my_col, :, pl.ds(m_loc * part, m_loc)] = jnp.sum(acc_ref[...].T, axis=0, keepdims=True)

    def stats_part(layer):
        beta = hp_ref[0]
        for copy in ab_copies(layer, False):
            copy.wait_recv()
        sum_a = rec_a[layer, 0]
        for idx in range(1, n_col):
            sum_a += rec_a[layer, idx]
        sum_b = rec_b[layer, 0]
        for idx in range(1, n_row):
            sum_b += rec_b[layer, idx]
        for part in range(2):
            mat = 2 * layer + part
            old_a = (old_ri if part == 0 else old_co)[pl.ds(layer, 1), :]
            old_b = (old_ci if part == 0 else old_ro)[pl.ds(layer, 1), :]
            part_a = sum_a[:, m_loc * part:m_loc * (part + 1)]
            part_b = sum_b[:, n_loc * part:n_loc * (part + 1)]
            new_a = beta * old_a + (1.0 - beta) * (part_a / len_b + EPS_ONE)
            new_b = beta * old_b + (1.0 - beta) * (part_b / len_a + EPS_ONE)
            na_ref[part, pl.ds(layer, 1), :] = new_a
            nb_ref[part, pl.ds(layer, 1), :] = new_b
            if part == 0:
                norm = jnp.sum(new_a, axis=1, keepdims=True) / m_loc
                scale_a = lax.rsqrt(new_a / norm)
                scale_b = lax.rsqrt(new_b)
            else:
                norm = jnp.sum(new_b, axis=1, keepdims=True) / n_loc
                scale_a = lax.rsqrt(new_a)
                scale_b = lax.rsqrt(new_b / norm)
            put(1, mat, norm)
            sb_ref[mat] = scale_b
            sa_ref[mat] = jnp.broadcast_to(scale_a, (128, m_loc)).T

        def body(idx, accs):
            part = idx // (m_loc // 64)
            mat = 2 * layer + part
            rows = pl.ds(pl.multiple_of(64 * lax.rem(idx, m_loc // 64), 64), 64)
            row_scale = sa_ref[mat, rows, :]
            total = jnp.zeros((64, 128), F32)
            for blk in range(n_loc // 128):
                cols = pl.ds(128 * blk, 128)
                upd = g_ref[mat, rows, cols] * row_scale * sb_ref[mat, :, cols]
                total += upd * upd
            return total

        for part in range(2):
            total = jnp.zeros((64, 128), F32)
            for idx in range(m_loc // 64):
                total += body(part * (m_loc // 64) + idx, None)
            one = jnp.sum(total, axis=0, keepdims=True)
            put(0, 2 * layer + part, jnp.sum(one, axis=1, keepdims=True))

    def w_part(layer, part):
        w_copy(layer, part).wait()
        ref = wi_ref if part == 0 else wo_ref
        rows_all, cols_all = ref.shape[1], ref.shape[2]

        def body(idx, total):
            rows = pl.ds(pl.multiple_of(idx * (rows_all // 8), 8), rows_all // 8)
            val = ref[layer, rows, :]
            sq = (val * val).reshape(rows_all // 64, 8, cols_all)
            sq = jnp.sum(sq, axis=0)
            for blk in range(cols_all // 128):
                total += sq[:, 128 * blk:128 * (blk + 1)]
            return total

        total = lax.fori_loop(0, 8, body, jnp.zeros((8, 128), F32))
        one = jnp.sum(total, axis=0, keepdims=True)
        put(2, 2 * layer + part, jnp.sum(one, axis=1, keepdims=True))

    def layer_body(layer, carry):
        for part in range(2):
            ahead = 2 * layer + part + LOOKAHEAD
            ahead_part = (part + LOOKAHEAD) % 2
            ahead_layer = (ahead - ahead_part) // 2
            grad_part(layer, part)

            @pl.when(ahead < n_mat)
            def _():
                start_load(ahead_layer, ahead_part)

            if part == 0:
                @pl.when(layer == layers - 2)
                def _():
                    for idx in range(layers):
                        w_copy(idx, 0).start()

                @pl.when(layer == layers - 1)
                def _():
                    for idx in range(layers):
                        w_copy(idx, 1).start()

        @pl.when(layer == 0)
        def _():
            pl.semaphore_wait(barrier, n_dev - 1)
            for copy in old_copies:
                copy.wait()

        for copy in ab_copies(layer, True):
            copy.start()

        @pl.when(layer > 0)
        def _():
            stats_part(layer - 1)

        return carry

    lax.fori_loop(0, layers, layer_body, 0)

    def w_body(layer, carry):
        w_part(layer, 0)
        w_part(layer, 1)
        return carry

    lax.fori_loop(0, layers, w_body, 0)
    stats_part(layers - 1)

    rec_s[me] = pay_ref[...]
    for copy in s_copies(True):
        copy.start()

    def drain(layer, carry):
        for copy in ab_copies(layer, True):
            copy.wait_send()
        return carry

    lax.fori_loop(0, layers, drain, 0)
    for copy in s_copies(False):
        copy.wait_recv()
    norm_sum = jnp.zeros((1, 128), F32)
    w_sum = jnp.zeros((1, 128), F32)
    for dev in range(n_dev):
        norm_sum += rec_s[dev, :, 128:256]
        w_sum += rec_s[dev, :, 256:384]
    used = lane < n_mat
    mean_s = norm_sum / n_dev
    upd_sum = jnp.zeros((1, 128), F32)
    for dev in range(n_dev):
        norm = jnp.where(used, rec_s[dev, :, 128:256], 1.0)
        upd_sum += rec_s[dev, :, 0:128] * (mean_s / norm)
    n_total = float(len_a * len_b)
    upd_rms = jnp.sqrt(upd_sum / n_total)
    w_rms = jnp.sqrt(w_sum / n_total)
    step_size = hp_ref[1] * jnp.maximum(EPS_TWO, w_rms) / jnp.maximum(1.0, upd_rms / hp_ref[2])
    norm = jnp.where(used, pay_ref[:, 128:256], 1.0)
    fac_ref[...] = step_size * jnp.sqrt(mean_s / norm)
    for copy in s_copies(True):
        copy.wait_send()


def update_kernel(dims, g_ref, wi_ref, wo_ref, sa_ref, sb_ref, fac_ref, na_ref, nb_ref,
                  w_in_new, row_in_new, col_in_new, w_out_new, row_out_new, col_out_new,
                  stage_i, stage_o, sem_i, sem_o, stat_sem):
    layers, m_loc, n_loc = dims
    stat_copies = [pltpu.make_async_copy(src, dst, stat_sem.at[k]) for k, (src, dst) in enumerate(
        ((na_ref.at[0], row_in_new), (nb_ref.at[0], col_in_new), (nb_ref.at[1], row_out_new), (na_ref.at[1], col_out_new)))]
    for copy in stat_copies:
        copy.start()
    lane = lax.broadcasted_iota(jnp.int32, (1, 128), 1)
    chunk_i = m_loc // 4
    chunk_o = n_loc // 4

    def factor(mat):
        return jnp.sum(jnp.where(lane == mat, fac_ref[...], 0.0), axis=1, keepdims=True)

    def copy_in(layer, idx, slot):
        return pltpu.make_async_copy(stage_i.at[slot], w_in_new.at[layer, pl.ds(chunk_i * idx, chunk_i)], sem_i.at[slot])

    def copy_out(layer, idx, slot):
        return pltpu.make_async_copy(stage_o.at[slot], w_out_new.at[layer, pl.ds(chunk_o * idx, chunk_o)], sem_o.at[slot])

    def body(layer, carry):
        mat = 2 * layer
        fac = factor(mat)
        for idx in range(4):
            slot = idx

            @pl.when(layer > 0)
            def _():
                copy_in(layer - 1, idx, slot).wait()

            rows = pl.ds(chunk_i * idx, chunk_i)
            row_scale = sa_ref[mat, rows, :] * fac
            for blk in range(n_loc // 128):
                cols = pl.ds(128 * blk, 128)
                upd = g_ref[mat, rows, cols] * row_scale * sb_ref[mat, :, cols]
                stage_i[slot, :, cols] = wi_ref[layer, rows, cols] - upd
            copy_in(layer, idx, slot).start()
        mat = 2 * layer + 1
        fac = factor(mat)
        for idx in range(4):
            slot = idx

            @pl.when(layer > 0)
            def _():
                copy_out(layer - 1, idx, slot).wait()

            for sub in range(m_loc // 128):
                rows = pl.ds(128 * sub, 128)
                row_scale = sa_ref[mat, rows, :] * fac
                for blk in range(chunk_o // 128):
                    cols = pl.ds(chunk_o * idx + 128 * blk, 128)
                    upd = g_ref[mat, rows, cols] * row_scale * sb_ref[mat, :, cols]
                    here = pl.ds(128 * blk, 128)
                    stage_o[slot, here, rows] = wo_ref[layer, cols, rows] - upd.T
            copy_out(layer, idx, slot).start()
        return carry

    lax.fori_loop(0, layers, body, 0)
    for idx in range(4):
        copy_in(layers - 1, idx, idx).wait()
        copy_out(layers - 1, idx, idx).wait()
    for copy in stat_copies:
        copy.wait()


def solution(mesh):
    n_col = mesh.shape['col']
    n_row = mesh.shape['row']
    n_dev = n_col * n_row
    tile_in = P(None, 'row', 'col')
    tile_out = P(None, 'col', 'row')
    lane_row = P(None, None, 'row')
    lane_col = P(None, None, 'col')
    vec_row = P(None, 'row')
    vec_col = P(None, 'col')

    def local_step(hyper_params, w_in, x_in, dy_in, row_in, col_in, w_out, x_out, dy_out, row_out, col_out):
        layers, m_loc, n_loc = w_in.shape
        tokens = x_in.shape[1]
        n_mat = 2 * layers
        len_a, len_b = m_loc * n_row, n_loc * n_col
        dims = (n_col, n_row, layers, m_loc, n_loc, tokens, len_a, len_b)
        hbm = pl.BlockSpec(memory_space=pl.ANY)
        vmem = pl.BlockSpec(memory_space=pltpu.VMEM)
        mid = pl.pallas_call(
            functools.partial(stats_kernel, dims),
            out_shape=[
                pltpu.VMEM((n_mat, m_loc, n_loc), F32),
                pltpu.VMEM((layers, m_loc, n_loc), F32),
                pltpu.VMEM((layers, n_loc, m_loc), F32),
                pltpu.VMEM((n_mat, m_loc, 128), F32),
                pltpu.VMEM((n_mat, 1, n_loc), F32),
                pltpu.VMEM((1, 128), F32),
                pltpu.VMEM((2, layers, m_loc), F32),
                pltpu.VMEM((2, layers, n_loc), F32),
            ],
            in_specs=[hbm] * 11,
            out_specs=[vmem] * 8,
            scratch_shapes=[
                pltpu.SMEM((3,), F32),
                pltpu.VMEM((SLOTS, tokens, m_loc), BF16),
                pltpu.VMEM((SLOTS, tokens, n_loc), BF16),
                pltpu.VMEM((m_loc, tokens), BF16),
                pltpu.VMEM((m_loc, 128), F32),
                pltpu.VMEM((layers, n_col, 1, 2 * m_loc), F32),
                pltpu.VMEM((layers, n_row, 1, 2 * n_loc), F32),
                pltpu.VMEM((n_dev, 1, 384), F32),
                pltpu.VMEM((1, 384), F32),
                pltpu.VMEM((layers, m_loc), F32),
                pltpu.VMEM((layers, n_loc), F32),
                pltpu.VMEM((layers, n_loc), F32),
                pltpu.VMEM((layers, m_loc), F32),
                pltpu.SemaphoreType.DMA((SLOTS, 2)),
                pltpu.SemaphoreType.DMA((layers, 2)),
                pltpu.SemaphoreType.DMA((5,)),
                pltpu.SemaphoreType.DMA((layers, n_col)),
                pltpu.SemaphoreType.DMA((layers, n_col)),
                pltpu.SemaphoreType.DMA((layers, n_row)),
                pltpu.SemaphoreType.DMA((layers, n_row)),
                pltpu.SemaphoreType.DMA((n_dev,)),
                pltpu.SemaphoreType.DMA((n_dev,)),
            ],
            compiler_params=pltpu.CompilerParams(collective_id=0, has_side_effects=True, vmem_limit_bytes=GRANT),
            name='adafactor_stats',
        )(*[pltpu.with_memory_space_constraint(item, pltpu.HBM) for item in (
            hyper_params, w_in, x_in, dy_in, row_in, col_in, w_out, x_out, dy_out, row_out, col_out)])
        mid = [pltpu.with_memory_space_constraint(item, pltpu.VMEM) for item in mid]
        out = pl.pallas_call(
            functools.partial(update_kernel, (layers, m_loc, n_loc)),
            out_shape=[
                jax.ShapeDtypeStruct(w_in.shape, F32),
                jax.ShapeDtypeStruct(row_in.shape, F32),
                jax.ShapeDtypeStruct(col_in.shape, F32),
                jax.ShapeDtypeStruct(w_out.shape, F32),
                jax.ShapeDtypeStruct(row_out.shape, F32),
                jax.ShapeDtypeStruct(col_out.shape, F32),
            ],
            in_specs=[vmem] * 8,
            out_specs=[hbm] * 6,
            scratch_shapes=[
                pltpu.VMEM((4, m_loc // 4, n_loc), F32),
                pltpu.VMEM((4, n_loc // 4, m_loc), F32),
                pltpu.SemaphoreType.DMA((4,)),
                pltpu.SemaphoreType.DMA((4,)),
                pltpu.SemaphoreType.DMA((4,)),
            ],
            compiler_params=pltpu.CompilerParams(vmem_limit_bytes=GRANT),
            name='adafactor_update',
        )(*mid)
        return tuple(out)

    return jax.shard_map(local_step, mesh=mesh, in_specs=(P(), tile_in, lane_row, lane_col, vec_row, vec_col, tile_out, lane_col, lane_row, vec_col, vec_row), out_specs=(tile_in, vec_row, vec_col, tile_out, vec_col, vec_row), check_vma=False)
```

```python
import functools

import jax
import jax.numpy as jnp
from jax import lax
from jax.experimental import pallas as pl
from jax.experimental.pallas import tpu as pltpu
from jax.sharding import PartitionSpec as P

EPS_ONE = 1e-30
EPS_TWO = 1e-3
F32 = jnp.float32
BF16 = jnp.bfloat16
MESH = pl.DeviceIdType.MESH
LOOKAHEAD = 3
SLOTS = 4
FIRST = 4
LATE = 5
T_SCALE = 2.0 ** -16
GRANT = 24 * 2**20


def stats_kernel(dims, hp_hbm, w_in, x_in, dy_in, row_in, col_in, w_out, x_out, dy_out, row_out, col_out,
                 gi_ref, go_ref, wi_ref, wo_ref, sa_ref, sb_ref, fac_ref, na_ref, nb_ref,
                 hp_ref, small_ref, big_ref, xt_ref, acc_ref, rec_a, rec_b, rec_s, pay_ref,
                 old_ri, old_ci, old_ro, old_co,
                 small_sem, big_sem, first_sem, w_sem, old_sem, send_a, recv_a, send_b, recv_b, send_s, recv_s):
    n_col, n_row, layers, m_loc, n_loc, tokens, len_a, len_b = dims
    n_mat = 2 * layers
    n_dev = n_col * n_row
    my_col = lax.axis_index('col')
    my_row = lax.axis_index('row')
    me = my_col * n_row + my_row
    first_cols = n_loc // FIRST

    def small_copy(mat):
        src = (dy_out if mat % 2 else x_in).at[mat // 2]
        return pltpu.make_async_copy(src, small_ref.at[mat % SLOTS], small_sem.at[mat % SLOTS])

    def big_copy(mat):
        src = (x_out if mat % 2 else dy_in).at[mat // 2]
        return pltpu.make_async_copy(src, big_ref.at[mat % SLOTS], big_sem.at[mat % SLOTS])

    def first_copy(idx):
        cols = pl.ds(first_cols * idx, first_cols)
        return pltpu.make_async_copy(dy_in.at[0, :, cols], big_ref.at[0, :, cols], first_sem.at[idx])

    def w_copy(mat):
        src, dst = (w_out, wo_ref) if mat % 2 else (w_in, wi_ref)
        return pltpu.make_async_copy(src.at[mat // 2], dst.at[mat // 2], w_sem.at[mat])

    small_copy(0).start()
    first_copy(0).start()
    small_copy(1).start()
    for idx in range(1, FIRST):
        first_copy(idx).start()
    for mat in range(1, LOOKAHEAD):
        small_copy(mat + 1).start()
        big_copy(mat).start()
    old_copies = [pltpu.make_async_copy(src, dst, old_sem.at[k]) for k, (src, dst) in enumerate(
        ((row_in, old_ri), (col_in, old_ci), (row_out, old_ro), (col_out, old_co), (hp_hbm, hp_ref)))]
    for copy in old_copies:
        copy.start()
    barrier = pltpu.get_barrier_semaphore()
    for col in range(n_col):
        for row in range(n_row):
            pl.semaphore_signal(barrier, inc=1, device_id=(col, row), device_id_type=MESH)

    def a_send(mat, step):
        return pltpu.make_async_remote_copy(
            rec_a.at[mat, my_col], rec_a.at[mat, my_col], send_a.at[0], recv_a.at[mat],
            device_id=(lax.rem(my_col + step, n_col), my_row), device_id_type=MESH)

    def b_send(mat, step):
        return pltpu.make_async_remote_copy(
            rec_b.at[mat, my_row], rec_b.at[mat, my_row], send_b.at[0], recv_b.at[mat],
            device_id=(my_col, lax.rem(my_row + step, n_row)), device_id_type=MESH)

    def s_send(step):
        peer = lax.rem(me + step, n_dev)
        return pltpu.make_async_remote_copy(
            rec_s.at[me], rec_s.at[me], send_s.at[0], recv_s.at[0],
            device_id=(peer // n_row, lax.rem(peer, n_row)), device_id_type=MESH)

    def take(ref, sem):
        pltpu.make_async_copy(ref, ref, sem).wait()

    lane = lax.broadcasted_iota(jnp.int32, (1, 128), 1)

    def put(place, val):
        pay_ref[...] = jnp.where(lane == place, val, pay_ref[...])

    pay_ref[...] = jnp.zeros_like(pay_ref)

    def g_of(mat):
        return (go_ref if mat % 2 else gi_ref).at[mat // 2]

    def row_sums(mat):
        rec_a[mat, my_col] = jnp.sum(acc_ref[mat % 2].T, axis=0, keepdims=True)

    def transpose_small(mat):
        xt_ref[mat % 2] = small_ref[mat % SLOTS].T

    def stats_scales(mat):
        beta = hp_ref[0]
        sum_a = rec_a[mat, 0]
        for idx in range(1, n_col):
            sum_a += rec_a[mat, idx]
        sum_b = rec_b[mat, 0]
        for idx in range(1, n_row):
            sum_b += rec_b[mat, idx]
        part, layer = mat % 2, mat // 2
        old_a = (old_co if part else old_ri)[pl.ds(layer, 1), :]
        old_b = (old_ro if part else old_ci)[pl.ds(layer, 1), :]
        new_a = beta * old_a + (1.0 - beta) * (sum_a / len_b + EPS_ONE)
        new_b = beta * old_b + (1.0 - beta) * (sum_b / len_a + EPS_ONE)
        na_ref[part, pl.ds(layer, 1), :] = new_a
        nb_ref[part, pl.ds(layer, 1), :] = new_b
        if part:
            norm = jnp.sum(new_b, axis=1, keepdims=True) / n_loc
            scale_a = lax.rsqrt(new_a)
            scale_b = lax.rsqrt(new_b / norm)
        else:
            norm = jnp.sum(new_a, axis=1, keepdims=True) / m_loc
            scale_a = lax.rsqrt(new_a / norm)
            scale_b = lax.rsqrt(new_b)
        sb_ref[mat] = scale_b
        sa_ref[mat] = jnp.broadcast_to(scale_a, (128, m_loc)).T
        return norm

    def square_piece(mat, idx, total):
        grad = g_of(mat)
        if mat % 2:
            for blk in range(n_loc // 128 // 8):
                cols = pl.ds(n_loc // 8 * idx + 128 * blk, 128)
                acc = jnp.zeros((8, 128), F32)
                for sub in range(m_loc // 64):
                    rows = pl.ds(64 * sub, 64)
                    upd = grad[rows, cols] * sa_ref[mat, rows, :]
                    acc += jnp.sum((upd * upd).reshape(8, 8, 128), axis=0)
                scale = sb_ref[mat, :, cols]
                total += acc * (scale * scale)
        else:
            rows = pl.ds(m_loc // 8 * idx, m_loc // 8)
            acc = jnp.zeros((m_loc // 8, 128), F32)
            for blk in range(n_loc // 128):
                cols = pl.ds(128 * blk, 128)
                upd = grad[rows, cols] * sb_ref[mat, :, cols]
                acc += upd * upd
            scale = sa_ref[mat, rows, :]
            total += jnp.sum((acc * (scale * scale)).reshape(m_loc // 64, 8, 128), axis=0)
        return total

    def all_sum(tile):
        one = jnp.sum(tile, axis=0, keepdims=True)
        return jnp.sum(one, axis=1, keepdims=True)

    def square_done(mat, total, norm):
        put(mat, all_sum(total) * T_SCALE / norm)
        put(n_mat + mat, norm)

    def take_round(mat):
        take(rec_a.at[mat, pl.ds(0, n_col - 1)], recv_a.at[mat])
        take(rec_b.at[mat, pl.ds(0, n_row - 1)], recv_b.at[mat])

    def send_round(mat):
        for step in range(1, n_row):
            b_send(mat, step).start()
        for step in range(1, n_col):
            a_send(mat, step).start()

    def step(mat):
        with jax.named_scope(f'load_wait#m={mat}'):
            if mat == 0:
                small_copy(0).wait()
                transpose_small(0)
                first_copy(0).wait()
            else:
                big_copy(mat).wait()
                if mat + 1 < n_mat:
                    small_copy(mat + 1).wait()
        if mat + LOOKAHEAD + 1 < n_mat:
            small_copy(mat + LOOKAHEAD + 1).start()
        if mat + LOOKAHEAD < n_mat:
            big_copy(mat + LOOKAHEAD).start()
        if mat == n_mat - 2:
            w_copy(0).start()
        if mat == n_mat - 1:
            for idx in range(1, n_mat):
                w_copy(idx).start()
        if mat + 1 < n_mat and mat > 0:
            transpose_small(mat + 1)
        if mat > 0:
            row_sums(mat - 1)
        late = mat - LATE
        if late >= 0:
            with jax.named_scope(f'round_wait#m={late}'):
                take_round(late)
            norm = stats_scales(late)
            total = jnp.zeros((8, 128), F32)
        grad_ref = g_of(mat)
        for blk in range(n_loc // 256):
            if mat == 0 and blk and (256 * blk) % first_cols == 0:
                first_copy(256 * blk // first_cols).wait()
            cols = pl.ds(256 * blk, 256)
            grad = jnp.dot(xt_ref[mat % 2], big_ref[mat % SLOTS, :, cols], preferred_element_type=F32)
            grad_ref[:, cols] = grad
            sq = grad * grad
            rec_b[mat, my_row, :, cols] = jnp.sum(sq, axis=0, keepdims=True)
            lanes = sq[:, :128] + sq[:, 128:]
            if blk == 0:
                acc_ref[mat % 2] = lanes
            else:
                acc_ref[mat % 2] += lanes
            if late >= 0:
                total = square_piece(late, blk, total)
        if late >= 0:
            square_done(late, total, norm)
        if mat == 0:
            small_copy(1).wait()
            transpose_small(1)
        if mat == 1:
            with jax.named_scope('barrier_wait'):
                pl.semaphore_wait(barrier, n_dev)
        if mat > 0:
            send_round(mat - 1)

    for mat in range(n_mat):
        with jax.named_scope(f'step#m={mat}'):
            if mat == LATE:
                for copy in old_copies:
                    copy.wait()
            step(mat)
    last = n_mat - 1
    with jax.named_scope('last_send'):
        row_sums(last)
        send_round(last)

    with jax.named_scope('w_sums'):
        for mat in range(n_mat):
            late = mat + n_mat - LATE
            if late < last:
                with jax.named_scope(f'round_wait#m={late}'):
                    take_round(late)
                norm = stats_scales(late)
                total = jnp.zeros((8, 128), F32)
                for idx in range(8):
                    total = square_piece(late, idx, total)
                square_done(late, total, norm)
            with jax.named_scope(f'w_wait#m={mat}'):
                w_copy(mat).wait()
            ref = (wo_ref if mat % 2 else wi_ref).at[mat // 2]
            rows_all, cols_all = ref.shape
            total = jnp.zeros((8, 128), F32)
            for idx in range(8):
                val = ref[pl.ds(rows_all // 8 * idx, rows_all // 8), :]
                sq = jnp.sum((val * val).reshape(rows_all // 64, 8, cols_all), axis=0)
                for blk in range(cols_all // 128):
                    total += sq[:, 128 * blk:128 * (blk + 1)]
            put(2 * n_mat + mat, all_sum(total))

    with jax.named_scope('last_wait'):
        take_round(last)
    with jax.named_scope('last_stats'):
        norm = stats_scales(last)
        total = jnp.zeros((8, 128), F32)
        for idx in range(8):
            total = square_piece(last, idx, total)
        square_done(last, total, norm)

    with jax.named_scope('s_send'):
        rec_s[me] = pay_ref[...]
        for step_idx in range(1, n_dev):
            s_send(step_idx).start()
    take(rec_a.at[:, pl.ds(0, n_col - 1)], send_a.at[0])
    take(rec_b.at[:, pl.ds(0, n_row - 1)], send_b.at[0])
    with jax.named_scope('s_wait'):
        take(rec_s.at[pl.ds(0, n_dev - 1)], recv_s.at[0])
    parts = [rec_s[dev] for dev in range(n_dev)]
    while len(parts) > 1:
        parts = [parts[k] + parts[k + 1] for k in range(0, len(parts), 2)]
    total = parts[0]
    used = lane < n_mat
    mean_s = pltpu.roll(total, 128 - n_mat, 1) / n_dev
    w_sum = pltpu.roll(total, 128 - 2 * n_mat, 1)
    norm = jnp.where(used, pltpu.roll(pay_ref[...], 128 - n_mat, 1), 1.0)
    n_total = float(len_a * len_b)
    upd_rms = jnp.sqrt(total * mean_s / (T_SCALE * n_total))
    w_rms = jnp.sqrt(w_sum / n_total)
    step_size = hp_ref[1] * jnp.maximum(EPS_TWO, w_rms) / jnp.maximum(1.0, upd_rms / hp_ref[2])
    fac_ref[...] = jnp.where(used, step_size * jnp.sqrt(mean_s / norm), 0.0)
    take(rec_s.at[pl.ds(0, n_dev - 1)], send_s.at[0])


def update_kernel(dims, gi_ref, go_ref, wi_ref, wo_ref, sa_ref, sb_ref, fac_ref, na_ref, nb_ref,
                  w_in_new, row_in_new, col_in_new, w_out_new, row_out_new, col_out_new,
                  stage_i, stage_o, sem_i, sem_o, stat_sem):
    layers, m_loc, n_loc = dims
    stat_copies = [pltpu.make_async_copy(src, dst, stat_sem.at[k]) for k, (src, dst) in enumerate(
        ((na_ref.at[0], row_in_new), (nb_ref.at[0], col_in_new), (nb_ref.at[1], row_out_new), (na_ref.at[1], col_out_new)))]
    for copy in stat_copies:
        copy.start()
    lane = lax.broadcasted_iota(jnp.int32, (1, 128), 1)
    chunk_i = m_loc // 4
    chunk_o = n_loc // 4

    def factor(mat):
        return jnp.sum(jnp.where(lane == mat, fac_ref[...], 0.0), axis=1, keepdims=True)

    def copy_in(layer, idx, slot):
        return pltpu.make_async_copy(stage_i.at[slot], w_in_new.at[layer, pl.ds(chunk_i * idx, chunk_i)], sem_i.at[slot])

    def copy_out(layer, idx, slot):
        return pltpu.make_async_copy(stage_o.at[slot], w_out_new.at[layer, pl.ds(chunk_o * idx, chunk_o)], sem_o.at[slot])

    def body(layer, carry):
        mat = 2 * layer
        fac = factor(mat)
        for idx in range(4):
            slot = idx

            @pl.when(layer > 0)
            def _():
                copy_in(layer - 1, idx, slot).wait()

            rows = pl.ds(chunk_i * idx, chunk_i)
            row_scale = sa_ref[mat, rows, :] * fac
            for blk in range(n_loc // 128):
                cols = pl.ds(128 * blk, 128)
                upd = gi_ref[layer, rows, cols] * row_scale * sb_ref[mat, :, cols]
                stage_i[slot, :, cols] = wi_ref[layer, rows, cols] - upd
            copy_in(layer, idx, slot).start()
        mat = 2 * layer + 1
        fac = factor(mat)
        for idx in range(4):
            slot = idx

            @pl.when(layer > 0)
            def _():
                copy_out(layer - 1, idx, slot).wait()

            for sub in range(m_loc // 128):
                rows = pl.ds(128 * sub, 128)
                row_scale = sa_ref[mat, rows, :] * fac
                for blk in range(chunk_o // 128):
                    cols = pl.ds(chunk_o * idx + 128 * blk, 128)
                    upd = go_ref[layer, rows, cols] * row_scale * sb_ref[mat, :, cols]
                    here = pl.ds(128 * blk, 128)
                    stage_o[slot, here, rows] = wo_ref[layer, cols, rows] - upd.T
            copy_out(layer, idx, slot).start()
        return carry

    lax.fori_loop(0, layers, body, 0)
    for idx in range(4):
        copy_in(layers - 1, idx, idx).wait()
        copy_out(layers - 1, idx, idx).wait()
    for copy in stat_copies:
        copy.wait()


def solution(mesh):
    n_col = mesh.shape['col']
    n_row = mesh.shape['row']
    n_dev = n_col * n_row
    tile_in = P(None, 'row', 'col')
    tile_out = P(None, 'col', 'row')
    lane_row = P(None, None, 'row')
    lane_col = P(None, None, 'col')
    vec_row = P(None, 'row')
    vec_col = P(None, 'col')

    def local_step(hyper_params, w_in, x_in, dy_in, row_in, col_in, w_out, x_out, dy_out, row_out, col_out):
        layers, m_loc, n_loc = w_in.shape
        tokens = x_in.shape[1]
        n_mat = 2 * layers
        len_a, len_b = m_loc * n_row, n_loc * n_col
        dims = (n_col, n_row, layers, m_loc, n_loc, tokens, len_a, len_b)
        hbm = pl.BlockSpec(memory_space=pl.ANY)
        vmem = pl.BlockSpec(memory_space=pltpu.VMEM)
        mid = pl.pallas_call(
            functools.partial(stats_kernel, dims),
            out_shape=[
                pltpu.VMEM((layers, m_loc, n_loc), F32),
                pltpu.VMEM((layers, m_loc, n_loc), F32),
                pltpu.VMEM((layers, m_loc, n_loc), F32),
                pltpu.VMEM((layers, n_loc, m_loc), F32),
                pltpu.VMEM((n_mat, m_loc, 128), F32),
                pltpu.VMEM((n_mat, 1, n_loc), F32),
                pltpu.VMEM((1, 128), F32),
                pltpu.VMEM((2, layers, m_loc), F32),
                pltpu.VMEM((2, layers, n_loc), F32),
            ],
            in_specs=[hbm] * 11,
            out_specs=[vmem] * 9,
            scratch_shapes=[
                pltpu.SMEM((3,), F32),
                pltpu.VMEM((SLOTS, tokens, m_loc), BF16),
                pltpu.VMEM((SLOTS, tokens, n_loc), BF16),
                pltpu.VMEM((2, m_loc, tokens), BF16),
                pltpu.VMEM((2, m_loc, 128), F32),
                pltpu.VMEM((n_mat, n_col, 1, m_loc), F32),
                pltpu.VMEM((n_mat, n_row, 1, n_loc), F32),
                pltpu.VMEM((n_dev, 1, 128), F32),
                pltpu.VMEM((1, 128), F32),
                pltpu.VMEM((layers, m_loc), F32),
                pltpu.VMEM((layers, n_loc), F32),
                pltpu.VMEM((layers, n_loc), F32),
                pltpu.VMEM((layers, m_loc), F32),
                pltpu.SemaphoreType.DMA((SLOTS,)),
                pltpu.SemaphoreType.DMA((SLOTS,)),
                pltpu.SemaphoreType.DMA((FIRST,)),
                pltpu.SemaphoreType.DMA((n_mat,)),
                pltpu.SemaphoreType.DMA((5,)),
                pltpu.SemaphoreType.DMA((1,)),
                pltpu.SemaphoreType.DMA((n_mat,)),
                pltpu.SemaphoreType.DMA((1,)),
                pltpu.SemaphoreType.DMA((n_mat,)),
                pltpu.SemaphoreType.DMA((1,)),
                pltpu.SemaphoreType.DMA((1,)),
            ],
            compiler_params=pltpu.CompilerParams(collective_id=0, has_side_effects=True, vmem_limit_bytes=GRANT),
            name='adafactor_stats',
        )(*[pltpu.with_memory_space_constraint(item, pltpu.HBM) for item in (
            hyper_params, w_in, x_in, dy_in, row_in, col_in, w_out, x_out, dy_out, row_out, col_out)])
        mid = [pltpu.with_memory_space_constraint(item, pltpu.VMEM) for item in mid]
        out = pl.pallas_call(
            functools.partial(update_kernel, (layers, m_loc, n_loc)),
            out_shape=[
                jax.ShapeDtypeStruct(w_in.shape, F32),
                jax.ShapeDtypeStruct(row_in.shape, F32),
                jax.ShapeDtypeStruct(col_in.shape, F32),
                jax.ShapeDtypeStruct(w_out.shape, F32),
                jax.ShapeDtypeStruct(row_out.shape, F32),
                jax.ShapeDtypeStruct(col_out.shape, F32),
            ],
            in_specs=[vmem] * 9,
            out_specs=[hbm] * 6,
            scratch_shapes=[
                pltpu.VMEM((4, m_loc // 4, n_loc), F32),
                pltpu.VMEM((4, n_loc // 4, m_loc), F32),
                pltpu.SemaphoreType.DMA((4,)),
                pltpu.SemaphoreType.DMA((4,)),
                pltpu.SemaphoreType.DMA((4,)),
            ],
            compiler_params=pltpu.CompilerParams(vmem_limit_bytes=GRANT),
            name='adafactor_update',
        )(*mid)
        return tuple(out)

    return jax.shard_map(local_step, mesh=mesh, in_specs=(P(), tile_in, lane_row, lane_col, vec_row, vec_col, tile_out, lane_col, lane_row, vec_col, vec_row), out_specs=(tile_in, vec_row, vec_col, tile_out, vec_col, vec_row), check_vma=False)
```

```python
import functools

import jax
import jax.numpy as jnp
from jax import lax
from jax.experimental import pallas as pl
from jax.experimental.pallas import tpu as pltpu
from jax.sharding import PartitionSpec as P

EPS_ONE = 1e-30
EPS_TWO = 1e-3
F32 = jnp.float32
BF16 = jnp.bfloat16
MESH = pl.DeviceIdType.MESH
LOOKAHEAD = 2
SLOTS = 4
FIRST = 4
LATE = 4
CHUNKS = 8
T_SCALE = 2.0 ** -16
GRANT = 24 * 2**20


def stats_kernel(dims, hp_hbm, w_in, x_in, dy_in, row_in, col_in, w_out, x_out, dy_out, row_out, col_out,
                 gi_ref, go_ref, wi_ref, wo_ref, sa_ref, sb_ref, fac_ref, na_ref, nb_ref,
                 hp_ref, small_ref, big_ref, xt_ref, acc_ref, tot_ref, rec_a, rec_b, rec_s, pay_ref,
                 old_ri, old_ci, old_ro, old_co,
                 small_sem, big_sem, first_sem, w_sem, old_sem, send_sem, recv_a, recv_b, recv_s):
    n_col, n_row, layers, m_loc, n_loc, tokens, len_a, len_b = dims
    n_mat = 2 * layers
    n_dev = n_col * n_row
    my_col = lax.axis_index('col')
    my_row = lax.axis_index('row')
    me = my_col * n_row + my_row
    peer_col = [lax.rem(my_col + step, n_col) for step in range(n_col)]
    peer_row = [lax.rem(my_row + step, n_row) for step in range(n_row)]
    first_cols = n_loc // FIRST

    def small_copy(mat):
        src = (x_in if mat % 2 else dy_out).at[mat // 2]
        return pltpu.make_async_copy(src, small_ref.at[mat % SLOTS], small_sem.at[mat % SLOTS])

    def big_copy(mat):
        src = (dy_in if mat % 2 else x_out).at[mat // 2]
        return pltpu.make_async_copy(src, big_ref.at[mat % SLOTS], big_sem.at[mat % SLOTS])

    def first_copy(idx):
        cols = pl.ds(first_cols * idx, first_cols)
        return pltpu.make_async_copy(x_out.at[0, :, cols], big_ref.at[0, :, cols], first_sem.at[idx])

    def w_copy(mat):
        src, dst = (w_in, wi_ref) if mat % 2 else (w_out, wo_ref)
        return pltpu.make_async_copy(src.at[mat // 2], dst.at[mat // 2], w_sem.at[mat])

    small_copy(0).start()
    first_copy(0).start()
    barrier = pltpu.get_barrier_semaphore()
    for col in range(n_col):
        for row in range(n_row):
            pl.semaphore_signal(barrier, inc=1, device_id=(col, row), device_id_type=MESH)
    for idx in range(1, FIRST):
        first_copy(idx).start()
    small_copy(1).start()
    old_copies = [pltpu.make_async_copy(src, dst, old_sem.at[k]) for k, (src, dst) in enumerate(
        ((row_in, old_ri), (col_in, old_ci), (row_out, old_ro), (col_out, old_co), (hp_hbm, hp_ref)))]
    for copy in old_copies:
        copy.start()

    def send_round(mat):
        for step in range(1, n_col):
            pltpu.make_async_remote_copy(
                rec_a.at[mat, my_col], rec_a.at[mat, my_col], send_sem.at[0], recv_a.at[mat],
                device_id=(peer_col[step], my_row), device_id_type=MESH).start()
        for step in range(1, n_row):
            pltpu.make_async_remote_copy(
                rec_b.at[mat, my_row], rec_b.at[mat, my_row], send_sem.at[1], recv_b.at[mat],
                device_id=(my_col, peer_row[step]), device_id_type=MESH).start()

    def send_scalars():
        for col in reversed(range(n_col)):
            for row in range(n_row):
                if col or row:
                    pltpu.make_async_remote_copy(
                        rec_s.at[me], rec_s.at[me], send_sem.at[2], recv_s.at[0],
                        device_id=(peer_col[col], peer_row[row]), device_id_type=MESH).start()

    def take(ref, sem):
        pltpu.make_async_copy(ref, ref, sem).wait()

    def take_a(mat):
        take(rec_a.at[mat, pl.ds(0, n_col - 1)], recv_a.at[mat])

    def take_b(mat):
        take(rec_b.at[mat, pl.ds(0, n_row - 1)], recv_b.at[mat])

    lane = lax.broadcasted_iota(jnp.int32, (1, 128), 1)

    def put(place, val):
        pay_ref[...] = jnp.where(lane == place, val, pay_ref[...])

    pay_ref[...] = jnp.zeros_like(pay_ref)

    def g_of(mat):
        return (gi_ref if mat % 2 else go_ref).at[mat // 2]

    def row_sums(mat):
        rec_a[mat, my_col] = jnp.sum(acc_ref[mat % 2].T, axis=0, keepdims=True)

    def transpose_small(mat):
        xt_ref[mat % 2] = small_ref[mat % SLOTS].T

    def new_b(mat):
        beta = hp_ref[0]
        total = rec_b[mat, 0]
        for idx in range(1, n_row):
            total += rec_b[mat, idx]
        layer = mat // 2
        old = (old_ci if mat % 2 else old_ro)[pl.ds(layer, 1), :]
        new = beta * old + (1.0 - beta) * (total / len_a + EPS_ONE)
        nb_ref[mat % 2, pl.ds(layer, 1), :] = new
        sb_ref[mat] = lax.rsqrt(new)
        if mat % 2 == 0:
            put(n_mat + mat, jnp.sum(new, axis=1, keepdims=True) / n_loc)

    def square_piece(mat, idx):
        grad = g_of(mat)
        rows = pl.ds(m_loc // 8 * idx, m_loc // 8)
        acc = jnp.zeros((m_loc // 8, 128), F32)
        for blk in range(n_loc // 128):
            cols = pl.ds(128 * blk, 128)
            upd = grad[rows, cols] * sb_ref[mat, :, cols]
            acc += upd * upd
        tot_ref[mat, rows, :] = acc

    def new_a(mat):
        beta = hp_ref[0]
        total = rec_a[mat, 0]
        for idx in range(1, n_col):
            total += rec_a[mat, idx]
        layer = mat // 2
        old = (old_ri if mat % 2 else old_co)[pl.ds(layer, 1), :]
        new = beta * old + (1.0 - beta) * (total / len_b + EPS_ONE)
        na_ref[mat % 2, pl.ds(layer, 1), :] = new
        inv = lax.rsqrt(new)
        rows = jnp.sum(tot_ref[mat].T, axis=0, keepdims=True) * T_SCALE
        put(mat, jnp.sum(rows * (inv * inv), axis=1, keepdims=True))
        if mat % 2:
            put(n_mat + mat, jnp.sum(new, axis=1, keepdims=True) / m_loc)

    def scale_a(mat):
        new = na_ref[mat % 2, pl.ds(mat // 2, 1), :]
        sa_ref[mat] = jnp.broadcast_to(lax.rsqrt(new), (128, m_loc)).T

    def weight_sum(mat):
        ref = (wi_ref if mat % 2 else wo_ref).at[mat // 2]
        rows_all, cols_all = ref.shape
        total = jnp.zeros((8, 128), F32)
        for idx in range(8):
            val = ref[pl.ds(rows_all // 8 * idx, rows_all // 8), :]
            sq = jnp.sum((val * val).reshape(rows_all // 64, 8, cols_all), axis=0)
            for blk in range(cols_all // 128):
                total += sq[:, 128 * blk:128 * (blk + 1)]
        one = jnp.sum(total, axis=0, keepdims=True)
        put(2 * n_mat + mat, jnp.sum(one, axis=1, keepdims=True))

    def product_piece(mat, blk):
        cols = pl.ds(256 * blk, 256)
        grad = jnp.dot(xt_ref[mat % 2], big_ref[mat % SLOTS, :, cols], preferred_element_type=F32)
        g_of(mat)[:, cols] = grad
        sq = grad * grad
        rec_b[mat, my_row, :, cols] = jnp.sum(sq, axis=0, keepdims=True)
        lanes = sq[:, :128] + sq[:, 128:]
        if blk == 0:
            acc_ref[mat % 2] = lanes
        else:
            acc_ref[mat % 2] += lanes

    def load_ahead(mat):
        if mat < n_mat:
            big_copy(mat).start()
        if mat + 1 < n_mat:
            small_copy(mat + 1).start()

    last = n_mat - 1
    pieces = n_loc // 256
    for mat in range(n_mat):
        late = mat - LATE
        with jax.named_scope(f'step#m={mat}'):
            with jax.named_scope(f'wait#m={mat}'):
                if mat == 0:
                    small_copy(0).wait()
                    transpose_small(0)
                    first_copy(0).wait()
                    load_ahead(1)
                else:
                    big_copy(mat).wait()
                    load_ahead(mat + LOOKAHEAD)
                    if mat < last:
                        small_copy(mat + 1).wait()
                if mat == 1:
                    pl.semaphore_wait(barrier, n_dev)
                if late == 0:
                    for copy in old_copies:
                        copy.wait()
                if late >= 0:
                    take_b(late)
            if mat == last - 1:
                w_copy(0).start()
                w_copy(1).start()
            if mat == last:
                for idx in range(2, n_mat):
                    w_copy(idx).start()
            if mat > 0:
                row_sums(mat - 1)
                send_round(mat - 1)
                if mat < last:
                    transpose_small(mat + 1)
            if late >= 0:
                new_b(late)
            for blk in range(pieces):
                if mat == 0 and blk and (256 * blk) % first_cols == 0:
                    idx = 256 * blk // first_cols
                    first_copy(idx).wait()
                    if idx == FIRST // 2:
                        load_ahead(2)
                product_piece(mat, blk)
                if late >= 0:
                    square_piece(late, blk)
            if mat == 0:
                small_copy(1).wait()
                transpose_small(1)
    with jax.named_scope('last_send'):
        row_sums(last)
        send_round(last)

    left = [mat for mat in range(n_mat - LATE, last)]
    for mat in range(n_mat):
        with jax.named_scope(f'left#m={mat}'):
            with jax.named_scope(f'wait_left#m={mat}'):
                if mat < len(left):
                    take_b(left[mat])
                if mat < last:
                    take_a(mat)
                else:
                    take_b(last)
                w_copy(mat).wait()
            if mat < len(left):
                new_b(left[mat])
                for idx in range(8):
                    square_piece(left[mat], idx)
            if mat < last and mat not in left:
                new_a(mat)
            if mat == last:
                new_b(last)
                for idx in range(8):
                    square_piece(last, idx)
                for idx in left:
                    new_a(idx)
            weight_sum(mat)

    with jax.named_scope('last_wait'):
        take_a(last)
    with jax.named_scope('last_stats'):
        new_a(last)
    with jax.named_scope('s_send'):
        rec_s[me] = pay_ref[...]
        send_scalars()
    with jax.named_scope('scales'):
        for mat in range(n_mat):
            scale_a(mat)
        take(rec_a.at[:, pl.ds(0, n_col - 1)], send_sem.at[0])
        take(rec_b.at[:, pl.ds(0, n_row - 1)], send_sem.at[1])
        take(rec_s.at[pl.ds(0, n_dev - 1)], send_sem.at[2])
    with jax.named_scope('s_wait'):
        take(rec_s.at[pl.ds(0, n_dev - 1)], recv_s.at[0])
    parts = [rec_s[dev] for dev in range(n_dev)]
    while len(parts) > 1:
        parts = [parts[k] + parts[k + 1] for k in range(0, len(parts), 2)]
    total = parts[0]
    mean_s = pltpu.roll(total, 128 - n_mat, 1) / n_dev
    w_sum = pltpu.roll(total, 128 - 2 * n_mat, 1)
    n_total = float(len_a * len_b)
    upd_rms = jnp.sqrt(total * mean_s / (T_SCALE * n_total))
    w_rms = jnp.sqrt(w_sum / n_total)
    step_size = hp_ref[1] * jnp.maximum(EPS_TWO, w_rms) / jnp.maximum(1.0, upd_rms / hp_ref[2])
    fac_ref[...] = jnp.where(lane < n_mat, step_size * jnp.sqrt(mean_s), 0.0)


def update_kernel(dims, gi_ref, go_ref, wi_ref, wo_ref, sa_ref, sb_ref, fac_ref, na_ref, nb_ref,
                  w_in_new, row_in_new, col_in_new, w_out_new, row_out_new, col_out_new,
                  stage_i, stage_o, sem_i, sem_o, stat_sem):
    layers, m_loc, n_loc = dims
    lane = lax.broadcasted_iota(jnp.int32, (1, 128), 1)
    chunk_i = m_loc // CHUNKS
    chunk_o = n_loc // CHUNKS
    stat_copies = [pltpu.make_async_copy(src, dst, stat_sem.at[k]) for k, (src, dst) in enumerate(
        ((na_ref.at[1], row_in_new), (nb_ref.at[1], col_in_new), (nb_ref.at[0], row_out_new), (na_ref.at[0], col_out_new)))]

    def factor(mat):
        return jnp.sum(jnp.where(lane == mat, fac_ref[...], 0.0), axis=1, keepdims=True)

    def copy_in(layer, idx):
        return pltpu.make_async_copy(stage_i.at[idx], w_in_new.at[layer, pl.ds(chunk_i * idx, chunk_i)], sem_i.at[idx])

    def copy_out(layer, idx):
        return pltpu.make_async_copy(stage_o.at[idx], w_out_new.at[layer, pl.ds(chunk_o * idx, chunk_o)], sem_o.at[idx])

    def body(layer, carry):
        fac_i = factor(2 * layer + 1)
        fac_o = factor(2 * layer)
        for idx in range(CHUNKS):
            @pl.when(layer > 0)
            def _():
                copy_in(layer - 1, idx).wait()

            mat = 2 * layer + 1
            rows = pl.ds(chunk_i * idx, chunk_i)
            row_scale = sa_ref[mat, rows, :] * fac_i
            for blk in range(n_loc // 128):
                cols = pl.ds(128 * blk, 128)
                upd = gi_ref[layer, rows, cols] * row_scale * sb_ref[mat, :, cols]
                stage_i[idx, :, cols] = wi_ref[layer, rows, cols] - upd
            copy_in(layer, idx).start()

            @pl.when(layer > 0)
            def _():
                copy_out(layer - 1, idx).wait()

            mat = 2 * layer
            for sub in range(m_loc // 128):
                rows = pl.ds(128 * sub, 128)
                row_scale = sa_ref[mat, rows, :] * fac_o
                for blk in range(chunk_o // 128):
                    cols = pl.ds(chunk_o * idx + 128 * blk, 128)
                    upd = go_ref[layer, rows, cols] * row_scale * sb_ref[mat, :, cols]
                    stage_o[idx, pl.ds(128 * blk, 128), rows] = wo_ref[layer, cols, rows] - upd.T
            copy_out(layer, idx).start()
        return carry

    lax.fori_loop(0, layers, body, 0)
    for copy in stat_copies:
        copy.start()
    for idx in range(CHUNKS):
        copy_in(layers - 1, idx).wait()
        copy_out(layers - 1, idx).wait()
    for copy in stat_copies:
        copy.wait()


def solution(mesh):
    n_col = mesh.shape['col']
    n_row = mesh.shape['row']
    n_dev = n_col * n_row
    tile_in = P(None, 'row', 'col')
    tile_out = P(None, 'col', 'row')
    lane_row = P(None, None, 'row')
    lane_col = P(None, None, 'col')
    vec_row = P(None, 'row')
    vec_col = P(None, 'col')

    def local_step(hyper_params, w_in, x_in, dy_in, row_in, col_in, w_out, x_out, dy_out, row_out, col_out):
        layers, m_loc, n_loc = w_in.shape
        tokens = x_in.shape[1]
        n_mat = 2 * layers
        len_a, len_b = m_loc * n_row, n_loc * n_col
        dims = (n_col, n_row, layers, m_loc, n_loc, tokens, len_a, len_b)
        hbm = pl.BlockSpec(memory_space=pl.ANY)
        vmem = pl.BlockSpec(memory_space=pltpu.VMEM)
        mid = pl.pallas_call(
            functools.partial(stats_kernel, dims),
            out_shape=[
                pltpu.VMEM((layers, m_loc, n_loc), F32),
                pltpu.VMEM((layers, m_loc, n_loc), F32),
                pltpu.VMEM((layers, m_loc, n_loc), F32),
                pltpu.VMEM((layers, n_loc, m_loc), F32),
                pltpu.VMEM((n_mat, m_loc, 128), F32),
                pltpu.VMEM((n_mat, 1, n_loc), F32),
                pltpu.VMEM((1, 128), F32),
                pltpu.VMEM((2, layers, m_loc), F32),
                pltpu.VMEM((2, layers, n_loc), F32),
            ],
            in_specs=[hbm] * 11,
            out_specs=[vmem] * 9,
            scratch_shapes=[
                pltpu.SMEM((3,), F32),
                pltpu.VMEM((SLOTS, tokens, m_loc), BF16),
                pltpu.VMEM((SLOTS, tokens, n_loc), BF16),
                pltpu.VMEM((2, m_loc, tokens), BF16),
                pltpu.VMEM((2, m_loc, 128), F32),
                pltpu.VMEM((n_mat, m_loc, 128), F32),
                pltpu.VMEM((n_mat, n_col, 1, m_loc), F32),
                pltpu.VMEM((n_mat, n_row, 1, n_loc), F32),
                pltpu.VMEM((n_dev, 1, 128), F32),
                pltpu.VMEM((1, 128), F32),
                pltpu.VMEM((layers, m_loc), F32),
                pltpu.VMEM((layers, n_loc), F32),
                pltpu.VMEM((layers, n_loc), F32),
                pltpu.VMEM((layers, m_loc), F32),
                pltpu.SemaphoreType.DMA((SLOTS,)),
                pltpu.SemaphoreType.DMA((SLOTS,)),
                pltpu.SemaphoreType.DMA((FIRST,)),
                pltpu.SemaphoreType.DMA((n_mat,)),
                pltpu.SemaphoreType.DMA((5,)),
                pltpu.SemaphoreType.DMA((3,)),
                pltpu.SemaphoreType.DMA((n_mat,)),
                pltpu.SemaphoreType.DMA((n_mat,)),
                pltpu.SemaphoreType.DMA((1,)),
            ],
            compiler_params=pltpu.CompilerParams(collective_id=0, has_side_effects=True, vmem_limit_bytes=GRANT),
            name='adafactor_stats',
        )(*[pltpu.with_memory_space_constraint(item, pltpu.HBM) for item in (
            hyper_params, w_in, x_in, dy_in, row_in, col_in, w_out, x_out, dy_out, row_out, col_out)])
        mid = [pltpu.with_memory_space_constraint(item, pltpu.VMEM) for item in mid]
        out = pl.pallas_call(
            functools.partial(update_kernel, (layers, m_loc, n_loc)),
            out_shape=[
                jax.ShapeDtypeStruct(w_in.shape, F32),
                jax.ShapeDtypeStruct(row_in.shape, F32),
                jax.ShapeDtypeStruct(col_in.shape, F32),
                jax.ShapeDtypeStruct(w_out.shape, F32),
                jax.ShapeDtypeStruct(row_out.shape, F32),
                jax.ShapeDtypeStruct(col_out.shape, F32),
            ],
            in_specs=[vmem] * 9,
            out_specs=[hbm] * 6,
            scratch_shapes=[
                pltpu.VMEM((CHUNKS, m_loc // CHUNKS, n_loc), F32),
                pltpu.VMEM((CHUNKS, n_loc // CHUNKS, m_loc), F32),
                pltpu.SemaphoreType.DMA((CHUNKS,)),
                pltpu.SemaphoreType.DMA((CHUNKS,)),
                pltpu.SemaphoreType.DMA((4,)),
            ],
            compiler_params=pltpu.CompilerParams(vmem_limit_bytes=GRANT),
            name='adafactor_update',
        )(*mid)
        return tuple(out)

    return jax.shard_map(local_step, mesh=mesh, in_specs=(P(), tile_in, lane_row, lane_col, vec_row, vec_col, tile_out, lane_col, lane_row, vec_col, vec_row), out_specs=(tile_in, vec_row, vec_col, tile_out, vec_col, vec_row), check_vma=False)
```

```python
import functools

import jax
import jax.numpy as jnp
from jax import lax
from jax.experimental import pallas as pl
from jax.experimental.pallas import tpu as pltpu
from jax.sharding import PartitionSpec as P

EPS_ONE = 1e-30
EPS_TWO = 1e-3
F32 = jnp.float32
BF16 = jnp.bfloat16
MESH = pl.DeviceIdType.MESH
LOOKAHEAD = 2
SLOTS = 4
FIRST = 2
LATE = 4
CHUNKS = 4
T_SCALE = 2.0 ** -16
GRANT = 24 * 2**20


def stats_kernel(dims, hp_hbm, w_in, x_in, dy_in, row_in, col_in, w_out, x_out, dy_out, row_out, col_out,
                 gi_ref, go_ref, wi_ref, wo_ref, sa_ref, sb_ref, fac_ref, na_ref, nb_ref,
                 hp_ref, small_ref, big_ref, xt_ref, acc_ref, tot_ref, rec_a, rec_b, rec_s, pay_ref,
                 old_ri, old_ci, old_ro, old_co,
                 small_sem, big_sem, first_sem, w_sem, old_sem, send_sem, recv_a, recv_b, recv_s):
    n_col, n_row, layers, m_loc, n_loc, tokens, len_a, len_b = dims
    n_mat = 2 * layers
    n_dev = n_col * n_row
    my_col = lax.axis_index('col')
    my_row = lax.axis_index('row')
    me = my_col * n_row + my_row
    peer_col = [lax.rem(my_col + step, n_col) for step in range(n_col)]
    peer_row = [lax.rem(my_row + step, n_row) for step in range(n_row)]
    first_cols = n_loc // FIRST

    def small_copy(mat):
        src = (x_in if mat % 2 else dy_out).at[mat // 2]
        return pltpu.make_async_copy(src, small_ref.at[mat % SLOTS], small_sem.at[mat % SLOTS])

    def big_copy(mat):
        src = (dy_in if mat % 2 else x_out).at[mat // 2]
        return pltpu.make_async_copy(src, big_ref.at[mat % SLOTS], big_sem.at[mat % SLOTS])

    def first_copy(idx):
        cols = pl.ds(first_cols * idx, first_cols)
        return pltpu.make_async_copy(x_out.at[0, :, cols], big_ref.at[0, :, cols], first_sem.at[idx])

    def w_copy(mat):
        src, dst = (w_in, wi_ref) if mat % 2 else (w_out, wo_ref)
        return pltpu.make_async_copy(src.at[mat // 2], dst.at[mat // 2], w_sem.at[mat])

    small_copy(0).start()
    first_copy(0).start()
    barrier = pltpu.get_barrier_semaphore()
    for col in range(n_col):
        for row in range(n_row):
            pl.semaphore_signal(barrier, inc=1, device_id=(col, row), device_id_type=MESH)
    for idx in range(1, FIRST):
        first_copy(idx).start()
    small_copy(1).start()
    old_copies = [pltpu.make_async_copy(src, dst, old_sem.at[k]) for k, (src, dst) in enumerate(
        ((row_in, old_ri), (col_in, old_ci), (row_out, old_ro), (col_out, old_co), (hp_hbm, hp_ref)))]
    for copy in old_copies:
        copy.start()

    def send_round(mat):
        for step in range(1, n_col):
            pltpu.make_async_remote_copy(
                rec_a.at[mat, my_col], rec_a.at[mat, my_col], send_sem.at[0], recv_a.at[mat],
                device_id=(peer_col[step], my_row), device_id_type=MESH).start()
        for step in range(1, n_row):
            pltpu.make_async_remote_copy(
                rec_b.at[mat, my_row], rec_b.at[mat, my_row], send_sem.at[1], recv_b.at[mat],
                device_id=(my_col, peer_row[step]), device_id_type=MESH).start()

    def send_scalars():
        rec = rec_s.at[me]

        def send(col, row):
            pltpu.make_async_remote_copy(
                rec, rec, send_sem.at[2], recv_s.at[0], device_id=(col, row), device_id_type=MESH).start()

        for pair in range(n_col // 2):
            same = 2 * pair + lax.rem(my_col, 2)
            other = 2 * pair + 1 - lax.rem(my_col, 2)

            @pl.when(same != my_col)
            def _():
                send(same, my_row)

            for row in range(1, n_row):
                send(same, peer_row[row])
            for row in range(n_row):
                send(other, peer_row[row])

    def take(ref, sem):
        pltpu.make_async_copy(ref, ref, sem).wait()

    def take_a(mat):
        take(rec_a.at[mat, pl.ds(0, n_col - 1)], recv_a.at[mat])

    def take_b(mat):
        take(rec_b.at[mat, pl.ds(0, n_row - 1)], recv_b.at[mat])

    lane = lax.broadcasted_iota(jnp.int32, (1, 128), 1)

    def put(place, val):
        pay_ref[...] = jnp.where(lane == place, val, pay_ref[...])

    pay_ref[...] = jnp.zeros_like(pay_ref)

    def g_of(mat):
        return (gi_ref if mat % 2 else go_ref).at[mat // 2]

    def row_sums(mat):
        rec_a[mat, my_col] = jnp.sum(acc_ref[mat % 2].T, axis=0, keepdims=True)

    def transpose_small(mat):
        xt_ref[mat % 2] = small_ref[mat % SLOTS].T

    def new_b(mat):
        beta = hp_ref[0]
        total = rec_b[mat, 0]
        for idx in range(1, n_row):
            total += rec_b[mat, idx]
        layer = mat // 2
        old = (old_ci if mat % 2 else old_ro)[pl.ds(layer, 1), :]
        new = beta * old + (1.0 - beta) * (total / len_a + EPS_ONE)
        nb_ref[mat % 2, pl.ds(layer, 1), :] = new
        sb_ref[mat] = lax.rsqrt(new)
        if mat % 2 == 0:
            put(n_mat + mat, jnp.sum(new, axis=1, keepdims=True) / n_loc)

    def square_piece(mat, idx):
        grad = g_of(mat)
        rows = pl.ds(m_loc // 8 * idx, m_loc // 8)
        acc = jnp.zeros((m_loc // 8, 128), F32)
        for blk in range(n_loc // 128):
            cols = pl.ds(128 * blk, 128)
            upd = grad[rows, cols] * sb_ref[mat, :, cols]
            acc += upd * upd
        tot_ref[mat, rows, :] = acc

    def new_a(mat):
        beta = hp_ref[0]
        total = rec_a[mat, 0]
        for idx in range(1, n_col):
            total += rec_a[mat, idx]
        layer = mat // 2
        old = (old_ri if mat % 2 else old_co)[pl.ds(layer, 1), :]
        new = beta * old + (1.0 - beta) * (total / len_b + EPS_ONE)
        na_ref[mat % 2, pl.ds(layer, 1), :] = new
        inv = lax.rsqrt(new)
        rows = jnp.sum(tot_ref[mat].T, axis=0, keepdims=True) * T_SCALE
        put(mat, jnp.sum(rows * (inv * inv), axis=1, keepdims=True))
        if mat % 2:
            put(n_mat + mat, jnp.sum(new, axis=1, keepdims=True) / m_loc)

    def scale_a(mat):
        new = na_ref[mat % 2, pl.ds(mat // 2, 1), :]
        sa_ref[mat] = jnp.broadcast_to(lax.rsqrt(new), (128, m_loc)).T

    def weight_sum(mat):
        ref = (wi_ref if mat % 2 else wo_ref).at[mat // 2]
        rows_all, cols_all = ref.shape
        total = jnp.zeros((8, 128), F32)
        for idx in range(8):
            val = ref[pl.ds(rows_all // 8 * idx, rows_all // 8), :]
            sq = jnp.sum((val * val).reshape(rows_all // 64, 8, cols_all), axis=0)
            for blk in range(cols_all // 128):
                total += sq[:, 128 * blk:128 * (blk + 1)]
        one = jnp.sum(total, axis=0, keepdims=True)
        put(2 * n_mat + mat, jnp.sum(one, axis=1, keepdims=True))

    def product_piece(mat, blk):
        cols = pl.ds(256 * blk, 256)
        grad = jnp.dot(xt_ref[mat % 2], big_ref[mat % SLOTS, :, cols], preferred_element_type=F32)
        g_of(mat)[:, cols] = grad
        sq = grad * grad
        rec_b[mat, my_row, :, cols] = jnp.sum(sq, axis=0, keepdims=True)
        lanes = sq[:, :128] + sq[:, 128:]
        if blk == 0:
            acc_ref[mat % 2] = lanes
        else:
            acc_ref[mat % 2] += lanes

    def load_ahead(mat):
        if mat < n_mat:
            big_copy(mat).start()
        if mat + 1 < n_mat:
            small_copy(mat + 1).start()

    last = n_mat - 1
    pieces = n_loc // 256
    for mat in range(n_mat):
        late = mat - LATE
        with jax.named_scope(f'step#m={mat}'):
            with jax.named_scope(f'wait#m={mat}'):
                if mat == 0:
                    small_copy(0).wait()
                    transpose_small(0)
                    first_copy(0).wait()
                    load_ahead(1)
                else:
                    big_copy(mat).wait()
                    load_ahead(mat + LOOKAHEAD)
                    if mat < last:
                        small_copy(mat + 1).wait()
                if mat == 1:
                    pl.semaphore_wait(barrier, n_dev)
                if late == 0:
                    for copy in old_copies:
                        copy.wait()
                if late >= 0:
                    take_b(late)
            if mat == last - 1:
                w_copy(0).start()
                w_copy(1).start()
            if mat == last:
                for idx in range(2, n_mat):
                    w_copy(idx).start()
            if mat > 0:
                row_sums(mat - 1)
                send_round(mat - 1)
                if mat < last:
                    transpose_small(mat + 1)
            if late >= 0:
                new_b(late)
            for blk in range(pieces):
                if mat == 0 and blk and (256 * blk) % first_cols == 0:
                    first_copy(256 * blk // first_cols).wait()
                    load_ahead(2)
                    small_copy(1).wait()
                    transpose_small(1)
                product_piece(mat, blk)
                if late >= 0:
                    square_piece(late, blk)
    with jax.named_scope('last_send'):
        row_sums(last)
        send_round(last)

    def second_pass(mat):
        new_b(mat)
        for idx in range(8):
            square_piece(mat, idx)

    left = list(range(n_mat - LATE, last))
    for mat in range(n_mat):
        with jax.named_scope(f'left#m={mat}'):
            if mat < len(left):
                with jax.named_scope(f'wait_left#m={mat}'):
                    take_b(left[mat])
                second_pass(left[mat])
            if mat < last - 1:
                take_a(mat)
                new_a(mat)
            if mat == last - 1:
                take_b(last)
                second_pass(last)
                take_a(mat)
                new_a(mat)
            with jax.named_scope(f'wait_w#m={mat}'):
                w_copy(mat).wait()
            weight_sum(mat)

    with jax.named_scope('last_wait'):
        take_a(last)
    with jax.named_scope('last_stats'):
        new_a(last)
    with jax.named_scope('s_send'):
        rec_s[me] = pay_ref[...]
        send_scalars()
    with jax.named_scope('scales'):
        for mat in range(n_mat):
            scale_a(mat)
        take(rec_a.at[:, pl.ds(0, n_col - 1)], send_sem.at[0])
        take(rec_b.at[:, pl.ds(0, n_row - 1)], send_sem.at[1])
        take(rec_s.at[pl.ds(0, n_dev - 1)], send_sem.at[2])
    with jax.named_scope('s_wait'):
        take(rec_s.at[pl.ds(0, n_dev - 1)], recv_s.at[0])
    parts = [rec_s[dev] for dev in range(n_dev)]
    while len(parts) > 1:
        parts = [parts[k] + parts[k + 1] for k in range(0, len(parts), 2)]
    total = parts[0]
    mean_s = pltpu.roll(total, 128 - n_mat, 1) / n_dev
    w_sum = pltpu.roll(total, 128 - 2 * n_mat, 1)
    n_total = float(len_a * len_b)
    upd_rms = jnp.sqrt(total * mean_s / (T_SCALE * n_total))
    w_rms = jnp.sqrt(w_sum / n_total)
    step_size = hp_ref[1] * jnp.maximum(EPS_TWO, w_rms) / jnp.maximum(1.0, upd_rms / hp_ref[2])
    fac_ref[...] = jnp.where(lane < n_mat, step_size * jnp.sqrt(mean_s), 0.0)


def update_kernel(dims, gi_ref, go_ref, wi_ref, wo_ref, sa_ref, sb_ref, fac_ref, na_ref, nb_ref,
                  w_in_new, row_in_new, col_in_new, w_out_new, row_out_new, col_out_new,
                  stage_i, stage_o, sem_i, sem_o, stat_sem):
    layers, m_loc, n_loc = dims
    lane = lax.broadcasted_iota(jnp.int32, (1, 128), 1)
    chunk_i = m_loc // CHUNKS
    chunk_o = n_loc // CHUNKS
    stat_copies = [pltpu.make_async_copy(src, dst, stat_sem.at[k]) for k, (src, dst) in enumerate(
        ((na_ref.at[1], row_in_new), (nb_ref.at[1], col_in_new), (nb_ref.at[0], row_out_new), (na_ref.at[0], col_out_new)))]

    def factor(mat):
        return jnp.sum(jnp.where(lane == mat, fac_ref[...], 0.0), axis=1, keepdims=True)

    def body(layer, carry):
        mat = 2 * layer + 1
        fac = factor(mat)
        for idx in range(CHUNKS):
            rows = pl.ds(chunk_i * idx, chunk_i)
            row_scale = sa_ref[mat, rows, :] * fac
            for blk in range(n_loc // 128):
                cols = pl.ds(128 * blk, 128)
                upd = gi_ref[layer, rows, cols] * row_scale * sb_ref[mat, :, cols]
                stage_i[layer, rows, cols] = wi_ref[layer, rows, cols] - upd
            pltpu.make_async_copy(stage_i.at[layer, rows], w_in_new.at[layer, rows], sem_i).start()
        mat = 2 * layer
        fac = factor(mat)
        for idx in range(CHUNKS):
            for sub in range(m_loc // 128):
                rows = pl.ds(128 * sub, 128)
                row_scale = sa_ref[mat, rows, :] * fac
                for blk in range(chunk_o // 128):
                    cols = pl.ds(chunk_o * idx + 128 * blk, 128)
                    upd = go_ref[layer, rows, cols] * row_scale * sb_ref[mat, :, cols]
                    stage_o[layer, cols, rows] = wo_ref[layer, cols, rows] - upd.T
            rows = pl.ds(chunk_o * idx, chunk_o)
            pltpu.make_async_copy(stage_o.at[layer, rows], w_out_new.at[layer, rows], sem_o).start()
        return carry

    lax.fori_loop(0, layers, body, 0)
    for copy in stat_copies:
        copy.start()
    pltpu.make_async_copy(stage_i, w_in_new, sem_i).wait()
    pltpu.make_async_copy(stage_o, w_out_new, sem_o).wait()
    for copy in stat_copies:
        copy.wait()


def solution(mesh):
    n_col = mesh.shape['col']
    n_row = mesh.shape['row']
    n_dev = n_col * n_row
    tile_in = P(None, 'row', 'col')
    tile_out = P(None, 'col', 'row')
    lane_row = P(None, None, 'row')
    lane_col = P(None, None, 'col')
    vec_row = P(None, 'row')
    vec_col = P(None, 'col')

    def local_step(hyper_params, w_in, x_in, dy_in, row_in, col_in, w_out, x_out, dy_out, row_out, col_out):
        layers, m_loc, n_loc = w_in.shape
        tokens = x_in.shape[1]
        n_mat = 2 * layers
        len_a, len_b = m_loc * n_row, n_loc * n_col
        dims = (n_col, n_row, layers, m_loc, n_loc, tokens, len_a, len_b)
        hbm = pl.BlockSpec(memory_space=pl.ANY)
        vmem = pl.BlockSpec(memory_space=pltpu.VMEM)
        mid = pl.pallas_call(
            functools.partial(stats_kernel, dims),
            out_shape=[
                pltpu.VMEM((layers, m_loc, n_loc), F32),
                pltpu.VMEM((layers, m_loc, n_loc), F32),
                pltpu.VMEM((layers, m_loc, n_loc), F32),
                pltpu.VMEM((layers, n_loc, m_loc), F32),
                pltpu.VMEM((n_mat, m_loc, 128), F32),
                pltpu.VMEM((n_mat, 1, n_loc), F32),
                pltpu.VMEM((1, 128), F32),
                pltpu.VMEM((2, layers, m_loc), F32),
                pltpu.VMEM((2, layers, n_loc), F32),
            ],
            in_specs=[hbm] * 11,
            out_specs=[vmem] * 9,
            scratch_shapes=[
                pltpu.SMEM((3,), F32),
                pltpu.VMEM((SLOTS, tokens, m_loc), BF16),
                pltpu.VMEM((SLOTS, tokens, n_loc), BF16),
                pltpu.VMEM((2, m_loc, tokens), BF16),
                pltpu.VMEM((2, m_loc, 128), F32),
                pltpu.VMEM((n_mat, m_loc, 128), F32),
                pltpu.VMEM((n_mat, n_col, 1, m_loc), F32),
                pltpu.VMEM((n_mat, n_row, 1, n_loc), F32),
                pltpu.VMEM((n_dev, 1, 128), F32),
                pltpu.VMEM((1, 128), F32),
                pltpu.VMEM((layers, m_loc), F32),
                pltpu.VMEM((layers, n_loc), F32),
                pltpu.VMEM((layers, n_loc), F32),
                pltpu.VMEM((layers, m_loc), F32),
                pltpu.SemaphoreType.DMA((SLOTS,)),
                pltpu.SemaphoreType.DMA((SLOTS,)),
                pltpu.SemaphoreType.DMA((FIRST,)),
                pltpu.SemaphoreType.DMA((n_mat,)),
                pltpu.SemaphoreType.DMA((5,)),
                pltpu.SemaphoreType.DMA((3,)),
                pltpu.SemaphoreType.DMA((n_mat,)),
                pltpu.SemaphoreType.DMA((n_mat,)),
                pltpu.SemaphoreType.DMA((1,)),
            ],
            compiler_params=pltpu.CompilerParams(collective_id=0, has_side_effects=True, vmem_limit_bytes=GRANT),
            name='adafactor_stats',
        )(*[pltpu.with_memory_space_constraint(item, pltpu.HBM) for item in (
            hyper_params, w_in, x_in, dy_in, row_in, col_in, w_out, x_out, dy_out, row_out, col_out)])
        mid = [pltpu.with_memory_space_constraint(item, pltpu.VMEM) for item in mid]
        out = pl.pallas_call(
            functools.partial(update_kernel, (layers, m_loc, n_loc)),
            out_shape=[
                jax.ShapeDtypeStruct(w_in.shape, F32),
                jax.ShapeDtypeStruct(row_in.shape, F32),
                jax.ShapeDtypeStruct(col_in.shape, F32),
                jax.ShapeDtypeStruct(w_out.shape, F32),
                jax.ShapeDtypeStruct(row_out.shape, F32),
                jax.ShapeDtypeStruct(col_out.shape, F32),
            ],
            in_specs=[vmem] * 9,
            out_specs=[hbm] * 6,
            scratch_shapes=[
                pltpu.VMEM((layers, m_loc, n_loc), F32),
                pltpu.VMEM((layers, n_loc, m_loc), F32),
                pltpu.SemaphoreType.DMA,
                pltpu.SemaphoreType.DMA,
                pltpu.SemaphoreType.DMA((4,)),
            ],
            compiler_params=pltpu.CompilerParams(vmem_limit_bytes=GRANT),
            name='adafactor_update',
        )(*mid)
        return tuple(out)

    return jax.shard_map(local_step, mesh=mesh, in_specs=(P(), tile_in, lane_row, lane_col, vec_row, vec_col, tile_out, lane_col, lane_row, vec_col, vec_row), out_specs=(tile_in, vec_row, vec_col, tile_out, vec_col, vec_row), check_vma=False)
```

```python
import functools

import jax
import jax.numpy as jnp
from jax import lax
from jax.experimental import pallas as pl
from jax.experimental.pallas import tpu as pltpu
from jax.sharding import PartitionSpec as P

EPS_ONE = 1e-30
EPS_TWO = 1e-3
F32 = jnp.float32
BF16 = jnp.bfloat16
MESH = pl.DeviceIdType.MESH
LOOKAHEAD = 2
SLOTS = 4
FIRST = 2
LATE = 5
CHUNKS = 4
T_SCALE = 2.0 ** -16
GRANT = 24 * 2**20


def stats_kernel(dims, hp_hbm, w_in, x_in, dy_in, row_in, col_in, w_out, x_out, dy_out, row_out, col_out,
                 gi_ref, go_ref, wi_ref, wo_ref, sa_ref, sb_ref, fac_ref, na_ref, nb_ref,
                 hp_ref, small_ref, big_ref, xt_ref, acc_ref, tot_ref, rec_a, rec_b, rec_s, pay_ref,
                 old_ri, old_ci, old_ro, old_co,
                 small_sem, big_sem, first_sem, w_sem, old_sem, send_sem, recv_a, recv_b, recv_s):
    n_col, n_row, layers, m_loc, n_loc, tokens, len_a, len_b = dims
    n_mat = 2 * layers
    n_dev = n_col * n_row
    my_col = lax.axis_index('col')
    my_row = lax.axis_index('row')
    me = my_col * n_row + my_row
    peer_col = [lax.rem(my_col + step, n_col) for step in range(n_col)]
    peer_row = [lax.rem(my_row + step, n_row) for step in range(n_row)]
    first_cols = n_loc // FIRST

    def small_copy(mat):
        src = (x_in if mat % 2 else dy_out).at[mat // 2]
        return pltpu.make_async_copy(src, small_ref.at[mat % SLOTS], small_sem.at[mat % 3])

    def big_copy(mat):
        src = (dy_in if mat % 2 else x_out).at[mat // 2]
        return pltpu.make_async_copy(src, big_ref.at[mat % SLOTS], big_sem.at[mat % LOOKAHEAD])

    def first_copy(idx):
        cols = pl.ds(first_cols * idx, first_cols)
        return pltpu.make_async_copy(x_out.at[0, :, cols], big_ref.at[0, :, cols], first_sem.at[idx])

    def w_copy(mat):
        src, dst = (w_in, wi_ref) if mat % 2 else (w_out, wo_ref)
        return pltpu.make_async_copy(src.at[mat // 2], dst.at[mat // 2], w_sem.at[mat // 2])

    small_copy(0).start()
    first_copy(0).start()
    barrier = pltpu.get_barrier_semaphore()
    for col in range(n_col):
        for row in range(n_row):
            pl.semaphore_signal(barrier, inc=1, device_id=(col, row), device_id_type=MESH)
    for idx in range(1, FIRST):
        first_copy(idx).start()
    small_copy(1).start()
    old_copies = [pltpu.make_async_copy(src, dst, old_sem.at[k]) for src, dst, k in (
        (row_in, old_ri, 0), (col_out, old_co, 0), (col_in, old_ci, 1), (row_out, old_ro, 1), (hp_hbm, hp_ref, 2))]
    for copy in old_copies:
        copy.start()

    def send_round(mat):
        for step in range(1, n_col):
            pltpu.make_async_remote_copy(
                rec_a.at[mat, my_col], rec_a.at[mat, my_col], send_sem.at[0], recv_a.at[mat // (n_mat - 2)],
                device_id=(peer_col[step], my_row), device_id_type=MESH).start()
        for step in range(1, n_row):
            pltpu.make_async_remote_copy(
                rec_b.at[mat, my_row], rec_b.at[mat, my_row], send_sem.at[1], recv_b.at[mat],
                device_id=(my_col, peer_row[step]), device_id_type=MESH).start()

    def send_scalars():
        rec = rec_s.at[me]

        def send(col, row):
            pltpu.make_async_remote_copy(
                rec, rec, send_sem.at[2], recv_s.at[0], device_id=(col, row), device_id_type=MESH).start()

        for pair in range(n_col // 2):
            same = 2 * pair + lax.rem(my_col, 2)
            other = 2 * pair + 1 - lax.rem(my_col, 2)

            @pl.when(same != my_col)
            def _():
                send(same, my_row)

            for row in range(1, n_row):
                send(same, peer_row[row])
            for row in range(n_row):
                send(other, peer_row[row])

    def take(ref, sem):
        pltpu.make_async_copy(ref, ref, sem).wait()

    def take_a(group):
        first, count = (n_mat - 2, 2) if group else (0, n_mat - 2)
        take(rec_a.at[pl.ds(first, count), pl.ds(0, n_col - 1)], recv_a.at[group])

    def take_b(mat):
        take(rec_b.at[mat, pl.ds(0, n_row - 1)], recv_b.at[mat])

    lane = lax.broadcasted_iota(jnp.int32, (1, 128), 1)

    def put(place, val):
        pay_ref[...] = jnp.where(lane == place, val, pay_ref[...])

    pay_ref[...] = jnp.zeros_like(pay_ref)

    def g_of(mat):
        return (gi_ref if mat % 2 else go_ref).at[mat // 2]

    def row_sums(mat):
        rec_a[mat, my_col] = jnp.sum(acc_ref[mat % 2].T, axis=0, keepdims=True)

    def transpose_small(mat):
        xt_ref[mat % 2] = small_ref[mat % SLOTS].T

    def new_b(mat):
        beta = hp_ref[0]
        total = rec_b[mat, 0]
        for idx in range(1, n_row):
            total += rec_b[mat, idx]
        layer = mat // 2
        old = (old_ci if mat % 2 else old_ro)[pl.ds(layer, 1), :]
        new = beta * old + (1.0 - beta) * (total / len_a + EPS_ONE)
        nb_ref[mat % 2, pl.ds(layer, 1), :] = new
        sb_ref[mat] = lax.rsqrt(new)
        if mat % 2 == 0:
            put(n_mat + mat, jnp.sum(new, axis=1, keepdims=True) / n_loc)

    def square_piece(mat, idx):
        grad = g_of(mat)
        rows = pl.ds(m_loc // 8 * idx, m_loc // 8)
        acc = jnp.zeros((m_loc // 8, 128), F32)
        for blk in range(n_loc // 128):
            cols = pl.ds(128 * blk, 128)
            upd = grad[rows, cols] * sb_ref[mat, :, cols]
            acc += upd * upd
        tot_ref[mat, rows, :] = acc

    def new_a(mat):
        beta = hp_ref[0]
        total = rec_a[mat, 0]
        for idx in range(1, n_col):
            total += rec_a[mat, idx]
        layer = mat // 2
        old = (old_ri if mat % 2 else old_co)[pl.ds(layer, 1), :]
        new = beta * old + (1.0 - beta) * (total / len_b + EPS_ONE)
        na_ref[mat % 2, pl.ds(layer, 1), :] = new
        inv = lax.rsqrt(new)
        rows = jnp.sum(tot_ref[mat].T, axis=0, keepdims=True) * T_SCALE
        put(mat, jnp.sum(rows * (inv * inv), axis=1, keepdims=True))
        if mat % 2:
            put(n_mat + mat, jnp.sum(new, axis=1, keepdims=True) / m_loc)

    def scale_a(mat):
        new = na_ref[mat % 2, pl.ds(mat // 2, 1), :]
        sa_ref[mat] = jnp.broadcast_to(lax.rsqrt(new), (128, m_loc)).T

    def weight_sum(mat):
        ref = (wi_ref if mat % 2 else wo_ref).at[mat // 2]
        rows_all, cols_all = ref.shape
        total = jnp.zeros((8, 128), F32)
        for idx in range(8):
            val = ref[pl.ds(rows_all // 8 * idx, rows_all // 8), :]
            sq = jnp.sum((val * val).reshape(rows_all // 64, 8, cols_all), axis=0)
            for blk in range(cols_all // 128):
                total += sq[:, 128 * blk:128 * (blk + 1)]
        one = jnp.sum(total, axis=0, keepdims=True)
        put(2 * n_mat + mat, jnp.sum(one, axis=1, keepdims=True))

    def product_piece(mat, blk):
        cols = pl.ds(256 * blk, 256)
        grad = jnp.dot(xt_ref[mat % 2], big_ref[mat % SLOTS, :, cols], preferred_element_type=F32)
        g_of(mat)[:, cols] = grad
        sq = grad * grad
        rec_b[mat, my_row, :, cols] = jnp.sum(sq, axis=0, keepdims=True)
        lanes = sq[:, :128] + sq[:, 128:]
        if blk == 0:
            acc_ref[mat % 2] = lanes
        else:
            acc_ref[mat % 2] += lanes

    def load_ahead(mat):
        if mat < n_mat:
            big_copy(mat).start()
        if mat + 1 < n_mat:
            small_copy(mat + 1).start()

    last = n_mat - 1
    pieces = n_loc // 256
    for mat in range(n_mat):
        late = mat - LATE
        with jax.named_scope(f'step#m={mat}'):
            with jax.named_scope(f'wait#m={mat}'):
                if mat == 0:
                    small_copy(0).wait()
                    transpose_small(0)
                    first_copy(0).wait()
                    load_ahead(1)
                else:
                    big_copy(mat).wait()
                    load_ahead(mat + LOOKAHEAD)
                    if mat < last:
                        small_copy(mat + 1).wait()
                if mat == 1:
                    pl.semaphore_wait(barrier, n_dev)
                if late == 0:
                    take(na_ref, old_sem.at[0])
                    take(nb_ref, old_sem.at[1])
                    old_copies[-1].wait()
                if late >= 0:
                    take_b(late)
            if mat == last - 1:
                w_copy(0).start()
                w_copy(1).start()
            if mat == last:
                for idx in range(2, n_mat):
                    w_copy(idx).start()
            if mat > 0:
                row_sums(mat - 1)
                if mat < last:
                    transpose_small(mat + 1)
            if late >= 0:
                new_b(late)
            for blk in range(pieces):
                if mat == 0 and blk and (256 * blk) % first_cols == 0:
                    first_copy(256 * blk // first_cols).wait()
                    load_ahead(2)
                    small_copy(1).wait()
                    transpose_small(1)
                product_piece(mat, blk)
                if late >= 0:
                    square_piece(late, blk)
            if mat > 0:
                send_round(mat - 1)
    with jax.named_scope('last_send'):
        row_sums(last)
        send_round(last)

    def second_pass(mat):
        new_b(mat)
        for idx in range(8):
            square_piece(mat, idx)

    def take_w(layer):
        take(wi_ref.at[pl.ds(0, 2)], w_sem.at[layer])

    left = list(range(n_mat - LATE, n_mat))
    for layer in range(layers):
        passes = left[:len(left) - layers + 1] if layer == 0 else left[len(left) - layers + layer:][:1]
        with jax.named_scope(f'left#m={layer}'):
            with jax.named_scope(f'wait_left#m={layer}'):
                for mat in passes:
                    take_b(mat)
                if layer == layers - 1:
                    take_a(0)
            with jax.named_scope(f'wait_w#m={layer}'):
                take_w(layer)
            for mat in passes:
                second_pass(mat)
            weight_sum(2 * layer)
            weight_sum(2 * layer + 1)
            if layer == layers - 1:
                for mat in range(n_mat - 2):
                    new_a(mat)

    with jax.named_scope('last_wait'):
        take_a(1)
    with jax.named_scope('last_stats'):
        new_a(last - 1)
        new_a(last)
    with jax.named_scope('s_send'):
        rec_s[me] = pay_ref[...]
        send_scalars()
    with jax.named_scope('scales'):
        for mat in range(n_mat):
            scale_a(mat)
        take(rec_a.at[:, pl.ds(0, n_col - 1)], send_sem.at[0])
        take(rec_b.at[:, pl.ds(0, n_row - 1)], send_sem.at[1])
        take(rec_s.at[pl.ds(0, n_dev - 1)], send_sem.at[2])
    with jax.named_scope('s_wait'):
        take(rec_s.at[pl.ds(0, n_dev - 1)], recv_s.at[0])
    parts = [rec_s[dev] for dev in range(n_dev)]
    while len(parts) > 1:
        parts = [parts[k] + parts[k + 1] for k in range(0, len(parts), 2)]
    total = parts[0]
    mean_s = pltpu.roll(total, 128 - n_mat, 1) / n_dev
    w_sum = pltpu.roll(total, 128 - 2 * n_mat, 1)
    n_total = float(len_a * len_b)
    upd_rms = jnp.sqrt(total * mean_s / (T_SCALE * n_total))
    w_rms = jnp.sqrt(w_sum / n_total)
    step_size = hp_ref[1] * jnp.maximum(EPS_TWO, w_rms) / jnp.maximum(1.0, upd_rms / hp_ref[2])
    fac_ref[...] = jnp.where(lane < n_mat, step_size * jnp.sqrt(mean_s), 0.0)


def update_kernel(dims, gi_ref, go_ref, wi_ref, wo_ref, sa_ref, sb_ref, fac_ref, na_ref, nb_ref,
                  w_in_new, row_in_new, col_in_new, w_out_new, row_out_new, col_out_new,
                  stage_i, stage_o, sem_i, sem_o, stat_sem):
    layers, m_loc, n_loc = dims
    lane = lax.broadcasted_iota(jnp.int32, (1, 128), 1)
    chunk_i = m_loc // CHUNKS
    chunk_o = n_loc // CHUNKS
    stat_copies = [pltpu.make_async_copy(src, dst, stat_sem.at[k]) for k, (src, dst) in enumerate(
        ((na_ref.at[1], row_in_new), (nb_ref.at[1], col_in_new), (nb_ref.at[0], row_out_new), (na_ref.at[0], col_out_new)))]

    def factor(mat):
        return jnp.sum(jnp.where(lane == mat, fac_ref[...], 0.0), axis=1, keepdims=True)

    def body(layer, carry):
        mat = 2 * layer + 1
        fac = factor(mat)
        for idx in range(CHUNKS):
            rows = pl.ds(chunk_i * idx, chunk_i)
            row_scale = sa_ref[mat, rows, :] * fac
            for blk in range(n_loc // 128):
                cols = pl.ds(128 * blk, 128)
                upd = gi_ref[layer, rows, cols] * row_scale * sb_ref[mat, :, cols]
                stage_i[layer, rows, cols] = wi_ref[layer, rows, cols] - upd
            pltpu.make_async_copy(stage_i.at[layer, rows], w_in_new.at[layer, rows], sem_i).start()
        mat = 2 * layer
        fac = factor(mat)
        for idx in range(CHUNKS):
            for sub in range(m_loc // 128):
                rows = pl.ds(128 * sub, 128)
                row_scale = sa_ref[mat, rows, :] * fac
                for blk in range(chunk_o // 128):
                    cols = pl.ds(chunk_o * idx + 128 * blk, 128)
                    upd = go_ref[layer, rows, cols] * row_scale * sb_ref[mat, :, cols]
                    stage_o[layer, cols, rows] = wo_ref[layer, cols, rows] - upd.T
            rows = pl.ds(chunk_o * idx, chunk_o)
            pltpu.make_async_copy(stage_o.at[layer, rows], w_out_new.at[layer, rows], sem_o).start()
        return carry

    with jax.named_scope('k2_body'):
        lax.fori_loop(0, layers, body, 0)
    for copy in stat_copies:
        copy.start()
    with jax.named_scope('k2_wait'):
        pltpu.make_async_copy(stage_i, w_in_new, sem_i).wait()
        pltpu.make_async_copy(stage_o, w_out_new, sem_o).wait()
    for copy in stat_copies:
        copy.wait()


def solution(mesh):
    n_col = mesh.shape['col']
    n_row = mesh.shape['row']
    n_dev = n_col * n_row
    tile_in = P(None, 'row', 'col')
    tile_out = P(None, 'col', 'row')
    lane_row = P(None, None, 'row')
    lane_col = P(None, None, 'col')
    vec_row = P(None, 'row')
    vec_col = P(None, 'col')

    def local_step(hyper_params, w_in, x_in, dy_in, row_in, col_in, w_out, x_out, dy_out, row_out, col_out):
        layers, m_loc, n_loc = w_in.shape
        tokens = x_in.shape[1]
        n_mat = 2 * layers
        len_a, len_b = m_loc * n_row, n_loc * n_col
        dims = (n_col, n_row, layers, m_loc, n_loc, tokens, len_a, len_b)
        hbm = pl.BlockSpec(memory_space=pl.ANY)
        vmem = pl.BlockSpec(memory_space=pltpu.VMEM)
        mid = pl.pallas_call(
            functools.partial(stats_kernel, dims),
            out_shape=[
                pltpu.VMEM((layers, m_loc, n_loc), F32),
                pltpu.VMEM((layers, m_loc, n_loc), F32),
                pltpu.VMEM((layers, m_loc, n_loc), F32),
                pltpu.VMEM((layers, n_loc, m_loc), F32),
                pltpu.VMEM((n_mat, m_loc, 128), F32),
                pltpu.VMEM((n_mat, 1, n_loc), F32),
                pltpu.VMEM((1, 128), F32),
                pltpu.VMEM((2, layers, m_loc), F32),
                pltpu.VMEM((2, layers, n_loc), F32),
            ],
            in_specs=[hbm] * 11,
            out_specs=[vmem] * 9,
            scratch_shapes=[
                pltpu.SMEM((3,), F32),
                pltpu.VMEM((SLOTS, tokens, m_loc), BF16),
                pltpu.VMEM((SLOTS, tokens, n_loc), BF16),
                pltpu.VMEM((2, m_loc, tokens), BF16),
                pltpu.VMEM((2, m_loc, 128), F32),
                pltpu.VMEM((n_mat, m_loc, 128), F32),
                pltpu.VMEM((n_mat, n_col, 1, m_loc), F32),
                pltpu.VMEM((n_mat, n_row, 1, n_loc), F32),
                pltpu.VMEM((n_dev, 1, 128), F32),
                pltpu.VMEM((1, 128), F32),
                pltpu.VMEM((layers, m_loc), F32),
                pltpu.VMEM((layers, n_loc), F32),
                pltpu.VMEM((layers, n_loc), F32),
                pltpu.VMEM((layers, m_loc), F32),
                pltpu.SemaphoreType.DMA((3,)),
                pltpu.SemaphoreType.DMA((LOOKAHEAD,)),
                pltpu.SemaphoreType.DMA((FIRST,)),
                pltpu.SemaphoreType.DMA((layers,)),
                pltpu.SemaphoreType.DMA((3,)),
                pltpu.SemaphoreType.DMA((3,)),
                pltpu.SemaphoreType.DMA((2,)),
                pltpu.SemaphoreType.DMA((n_mat,)),
                pltpu.SemaphoreType.DMA((1,)),
            ],
            compiler_params=pltpu.CompilerParams(collective_id=0, has_side_effects=True, vmem_limit_bytes=GRANT),
            name='adafactor_stats',
        )(*[pltpu.with_memory_space_constraint(item, pltpu.HBM) for item in (
            hyper_params, w_in, x_in, dy_in, row_in, col_in, w_out, x_out, dy_out, row_out, col_out)])
        mid = [pltpu.with_memory_space_constraint(item, pltpu.VMEM) for item in mid]
        out = pl.pallas_call(
            functools.partial(update_kernel, (layers, m_loc, n_loc)),
            out_shape=[
                jax.ShapeDtypeStruct(w_in.shape, F32),
                jax.ShapeDtypeStruct(row_in.shape, F32),
                jax.ShapeDtypeStruct(col_in.shape, F32),
                jax.ShapeDtypeStruct(w_out.shape, F32),
                jax.ShapeDtypeStruct(row_out.shape, F32),
                jax.ShapeDtypeStruct(col_out.shape, F32),
            ],
            in_specs=[vmem] * 9,
            out_specs=[hbm] * 6,
            scratch_shapes=[
                pltpu.VMEM((layers, m_loc, n_loc), F32),
                pltpu.VMEM((layers, n_loc, m_loc), F32),
                pltpu.SemaphoreType.DMA,
                pltpu.SemaphoreType.DMA,
                pltpu.SemaphoreType.DMA((4,)),
            ],
            compiler_params=pltpu.CompilerParams(vmem_limit_bytes=GRANT),
            name='adafactor_update',
        )(*mid)
        return tuple(out)

    return jax.shard_map(local_step, mesh=mesh, in_specs=(P(), tile_in, lane_row, lane_col, vec_row, vec_col, tile_out, lane_col, lane_row, vec_col, vec_row), out_specs=(tile_in, vec_row, vec_col, tile_out, vec_col, vec_row), check_vma=False)
```

```python
import functools

import jax
import jax.numpy as jnp
from jax import lax
from jax.experimental import pallas as pl
from jax.experimental.pallas import tpu as pltpu
from jax.sharding import PartitionSpec as P

EPS_ONE = 1e-30
EPS_TWO = 1e-3
F32 = jnp.float32
BF16 = jnp.bfloat16
MESH = pl.DeviceIdType.MESH
LOOKAHEAD = 2
SLOTS = 4
FIRST = 2
W_AT = {2: (0, 1), 1: (2, 3), 0: (4, 5, 6, 7)}
CHUNKS = 4
T_SCALE = 2.0 ** -16
GRANT = 24 * 2**20


def stats_kernel(dims, hp_hbm, w_in, x_in, dy_in, row_in, col_in, w_out, x_out, dy_out, row_out, col_out,
                 gi_ref, go_ref, wi_ref, wo_ref, sa_ref, sb_ref, fac_ref, na_ref, nb_ref,
                 hp_ref, small_ref, big_ref, xt_ref, acc_ref, tot_ref, row_ref, rec_a, rec_b, rec_s, pay_ref,
                 old_ri, old_ci, old_ro, old_co,
                 small_sem, big_sem, first_sem, w_sem, old_sem, send_sem, recv_a, recv_b, recv_s):
    n_col, n_row, layers, m_loc, n_loc, tokens, len_a, len_b = dims
    n_mat = 2 * layers
    n_dev = n_col * n_row
    my_col = lax.axis_index('col')
    my_row = lax.axis_index('row')
    me = my_col * n_row + my_row
    peer_col = [lax.rem(my_col + step, n_col) for step in range(n_col)]
    peer_row = [lax.rem(my_row + step, n_row) for step in range(n_row)]
    first_cols = n_loc // FIRST

    def small_copy(mat):
        src = (x_in if mat % 2 else dy_out).at[mat // 2]
        return pltpu.make_async_copy(src, small_ref.at[mat % SLOTS], small_sem.at[mat % 3])

    def big_copy(mat):
        src = (dy_in if mat % 2 else x_out).at[mat // 2]
        return pltpu.make_async_copy(src, big_ref.at[mat % SLOTS], big_sem.at[mat % LOOKAHEAD])

    def first_copy(idx):
        cols = pl.ds(first_cols * idx, first_cols)
        return pltpu.make_async_copy(x_out.at[0, :, cols], big_ref.at[0, :, cols], first_sem.at[idx])

    def w_copy(mat):
        src, dst = (w_in, wi_ref) if mat % 2 else (w_out, wo_ref)
        return pltpu.make_async_copy(src.at[mat // 2], dst.at[mat // 2], w_sem.at[(mat + 1) // 2 if mat == n_mat - 1 else mat // 2])

    small_copy(0).start()
    for idx in range(FIRST):
        first_copy(idx).start()
    small_copy(1).start()
    big_copy(1).start()
    small_copy(2).start()
    old_copies = [pltpu.make_async_copy(src, dst, old_sem.at[k]) for src, dst, k in (
        (row_in, old_ri, 0), (col_out, old_co, 0), (col_in, old_ci, 1), (row_out, old_ro, 1), (hp_hbm, hp_ref, 2))]
    for copy in old_copies:
        copy.start()
    barrier = pltpu.get_barrier_semaphore()
    for col in range(n_col):
        for row in range(n_row):
            pl.semaphore_signal(barrier, inc=1, device_id=(col, row), device_id_type=MESH)

    def send_round(mat):
        for step in range(1, n_col):
            pltpu.make_async_remote_copy(
                rec_a.at[mat, my_col], rec_a.at[mat, my_col], send_sem.at[0], recv_a.at[mat // (n_mat - 2)],
                device_id=(peer_col[step], my_row), device_id_type=MESH).start()
        for step in range(1, n_row):
            pltpu.make_async_remote_copy(
                rec_b.at[mat, my_row], rec_b.at[mat, my_row], send_sem.at[1], recv_b.at[mat],
                device_id=(my_col, peer_row[step]), device_id_type=MESH).start()

    def send_scalars():
        rec = rec_s.at[me]

        def send(col, row):
            pltpu.make_async_remote_copy(
                rec, rec, send_sem.at[2], recv_s.at[0], device_id=(col, row), device_id_type=MESH).start()

        for pair in range(n_col // 2):
            same = 2 * pair + lax.rem(my_col, 2)
            other = 2 * pair + 1 - lax.rem(my_col, 2)

            @pl.when(same != my_col)
            def _():
                send(same, my_row)

            for row in range(1, n_row):
                send(same, peer_row[row])
            for row in range(n_row):
                send(other, peer_row[row])

    def take(ref, sem):
        pltpu.make_async_copy(ref, ref, sem).wait()

    def take_a(group):
        first, count = (n_mat - 2, 2) if group else (0, n_mat - 2)
        take(rec_a.at[pl.ds(first, count), pl.ds(0, n_col - 1)], recv_a.at[group])

    def take_b(mat):
        take(rec_b.at[mat, pl.ds(0, n_row - 1)], recv_b.at[mat])

    lane = lax.broadcasted_iota(jnp.int32, (1, 128), 1)

    def put(place, val):
        pay_ref[...] = jnp.where(lane == place, val, pay_ref[...])

    pay_ref[...] = jnp.zeros_like(pay_ref)

    def g_of(mat):
        return (gi_ref if mat % 2 else go_ref).at[mat // 2]

    def row_sums(mat):
        rec_a[mat, my_col] = jnp.sum(acc_ref[mat % 2].T, axis=0, keepdims=True)

    def transpose_small(mat):
        xt_ref[mat % 2] = small_ref[mat % SLOTS].T

    def new_b(mat):
        beta = hp_ref[0]
        total = rec_b[mat, 0]
        for idx in range(1, n_row):
            total += rec_b[mat, idx]
        layer = mat // 2
        old = (old_ci if mat % 2 else old_ro)[pl.ds(layer, 1), :]
        new = beta * old + (1.0 - beta) * (total / len_a + EPS_ONE)
        nb_ref[mat % 2, pl.ds(layer, 1), :] = new
        sb_ref[mat] = lax.rsqrt(new)
        if mat % 2 == 0:
            put(n_mat + mat, jnp.sum(new, axis=1, keepdims=True) / n_loc)

    def square_piece(mat, idx):
        grad = g_of(mat)
        rows = pl.ds(m_loc // 8 * idx, m_loc // 8)
        acc = jnp.zeros((m_loc // 8, 128), F32)
        for blk in range(n_loc // 128):
            cols = pl.ds(128 * blk, 128)
            upd = grad[rows, cols] * sb_ref[mat, :, cols]
            acc += upd * upd
        tot_ref[mat % 2, rows, :] = acc

    def new_a(mat):
        beta = hp_ref[0]
        total = rec_a[mat, 0]
        for idx in range(1, n_col):
            total += rec_a[mat, idx]
        layer = mat // 2
        old = (old_ri if mat % 2 else old_co)[pl.ds(layer, 1), :]
        new = beta * old + (1.0 - beta) * (total / len_b + EPS_ONE)
        na_ref[mat % 2, pl.ds(layer, 1), :] = new
        inv = lax.rsqrt(new)
        put(mat, jnp.sum(row_ref[mat] * (inv * inv), axis=1, keepdims=True))
        if mat % 2:
            put(n_mat + mat, jnp.sum(new, axis=1, keepdims=True) / m_loc)

    def scale_a(mat):
        new = na_ref[mat % 2, pl.ds(mat // 2, 1), :]
        sa_ref[mat] = jnp.broadcast_to(lax.rsqrt(new), (128, m_loc)).T

    def weight_sum(mat):
        ref = (wi_ref if mat % 2 else wo_ref).at[mat // 2]
        rows_all, cols_all = ref.shape
        total = jnp.zeros((8, 128), F32)
        for idx in range(8):
            val = ref[pl.ds(rows_all // 8 * idx, rows_all // 8), :]
            sq = jnp.sum((val * val).reshape(rows_all // 64, 8, cols_all), axis=0)
            for blk in range(cols_all // 128):
                total += sq[:, 128 * blk:128 * (blk + 1)]
        one = jnp.sum(total, axis=0, keepdims=True)
        put(2 * n_mat + mat, jnp.sum(one, axis=1, keepdims=True))

    def product_piece(mat, blk):
        cols = pl.ds(256 * blk, 256)
        grad = jnp.dot(xt_ref[mat % 2], big_ref[mat % SLOTS, :, cols], preferred_element_type=F32)
        g_of(mat)[:, cols] = grad
        sq = grad * grad
        rec_b[mat, my_row, :, cols] = jnp.sum(sq, axis=0, keepdims=True)
        lanes = sq[:, :128] + sq[:, 128:]
        if blk == 0:
            acc_ref[mat % 2] = lanes
        else:
            acc_ref[mat % 2] += lanes

    def load_ahead(mat):
        if mat < n_mat:
            big_copy(mat).start()
        if mat + 1 < n_mat:
            small_copy(mat + 1).start()

    last = n_mat - 1
    pieces = n_loc // 256
    for mat in range(n_mat):
        with jax.named_scope(f'step#m={mat}'):
            with jax.named_scope(f'wait#m={mat}'):
                if mat == 0:
                    small_copy(0).wait()
                    transpose_small(0)
                    first_copy(0).wait()
                    load_ahead(2)
                else:
                    big_copy(mat).wait()
                    load_ahead(mat + LOOKAHEAD)
                    if mat < last:
                        small_copy(mat + 1).wait()
                if mat == 1:
                    pl.semaphore_wait(barrier, n_dev)
                if mat == last:
                    take(na_ref, old_sem.at[0])
                    take(nb_ref, old_sem.at[1])
                    old_copies[-1].wait()
            for idx in W_AT.get(last - mat, ()):
                w_copy(idx).start()
            if mat > 0:
                row_sums(mat - 1)
                if mat < last:
                    transpose_small(mat + 1)
            for blk in range(pieces):
                if mat == 0 and blk and (256 * blk) % first_cols == 0:
                    first_copy(256 * blk // first_cols).wait()
                    small_copy(1).wait()
                    transpose_small(1)
                product_piece(mat, blk)
            if mat > 0:
                send_round(mat - 1)
    with jax.named_scope('last_send'):
        row_sums(last)
        send_round(last)

    def second_pass(mat):
        new_b(mat)
        for idx in range(8):
            square_piece(mat, idx)
        row_ref[mat] = jnp.sum(tot_ref[mat % 2].T, axis=0, keepdims=True) * T_SCALE

    def take_w(mat):
        take(wi_ref.at[pl.ds(0, 1 if mat >= n_mat - 2 else 2)], w_sem.at[(mat + 1) // 2])

    for layer in range(layers):
        first, second = 2 * layer, 2 * layer + 1
        with jax.named_scope(f'left#m={layer}'):
            with jax.named_scope(f'wait_left#m={layer}'):
                take_b(first)
                take_b(second)
                if layer == layers - 1:
                    take_a(0)
                else:
                    take_w(first)
            second_pass(first)
            second_pass(second)
            if layer < layers - 1:
                weight_sum(first)
                weight_sum(second)
            else:
                for mat in range(n_mat - 2):
                    new_a(mat)
                with jax.named_scope('wait_w'):
                    take_w(first)
                weight_sum(first)
    with jax.named_scope('last_w'):
        take_w(last)
        weight_sum(last)

    with jax.named_scope('last_wait'):
        take_a(1)
    with jax.named_scope('last_stats'):
        new_a(last - 1)
        new_a(last)
    with jax.named_scope('s_send'):
        rec_s[me] = pay_ref[...]
        send_scalars()
    with jax.named_scope('scales'):
        for mat in range(n_mat):
            scale_a(mat)
        take(rec_a.at[:, pl.ds(0, n_col - 1)], send_sem.at[0])
        take(rec_b.at[:, pl.ds(0, n_row - 1)], send_sem.at[1])
        take(rec_s.at[pl.ds(0, n_dev - 1)], send_sem.at[2])
    with jax.named_scope('s_wait'):
        take(rec_s.at[pl.ds(0, n_dev - 1)], recv_s.at[0])
    parts = [rec_s[dev] for dev in range(n_dev)]
    while len(parts) > 1:
        parts = [parts[k] + parts[k + 1] for k in range(0, len(parts), 2)]
    total = parts[0]
    mean_s = pltpu.roll(total, 128 - n_mat, 1) / n_dev
    w_sum = pltpu.roll(total, 128 - 2 * n_mat, 1)
    n_total = float(len_a * len_b)
    upd_rms = jnp.sqrt(total * mean_s / (T_SCALE * n_total))
    w_rms = jnp.sqrt(w_sum / n_total)
    step_size = hp_ref[1] * jnp.maximum(EPS_TWO, w_rms) / jnp.maximum(1.0, upd_rms / hp_ref[2])
    fac_ref[...] = jnp.where(lane < n_mat, step_size * jnp.sqrt(mean_s), 0.0)


def update_kernel(dims, gi_ref, go_ref, wi_ref, wo_ref, sa_ref, sb_ref, fac_ref, na_ref, nb_ref,
                  w_in_new, row_in_new, col_in_new, w_out_new, row_out_new, col_out_new,
                  stage_i, stage_o, sem_i, sem_o, stat_sem):
    layers, m_loc, n_loc = dims
    lane = lax.broadcasted_iota(jnp.int32, (1, 128), 1)
    chunk_i = m_loc // CHUNKS
    chunk_o = n_loc // CHUNKS
    stat_copies = [pltpu.make_async_copy(src, dst, stat_sem.at[k]) for k, (src, dst) in enumerate(
        ((na_ref.at[1], row_in_new), (nb_ref.at[1], col_in_new), (nb_ref.at[0], row_out_new), (na_ref.at[0], col_out_new)))]

    def factor(mat):
        return jnp.sum(jnp.where(lane == mat, fac_ref[...], 0.0), axis=1, keepdims=True)

    def body(layer):
        mat = 2 * layer + 1
        fac = factor(mat)
        edges = ([0, 16] if layer == 0 else [0]) + [chunk_i * idx for idx in range(1, CHUNKS + 1)]
        for low, high in zip(edges, edges[1:]):
            rows = pl.ds(low, high - low)
            row_scale = sa_ref[mat, rows, :] * fac
            for blk in range(n_loc // 128):
                cols = pl.ds(128 * blk, 128)
                upd = gi_ref[layer, rows, cols] * row_scale * sb_ref[mat, :, cols]
                stage_i[layer, rows, cols] = wi_ref[layer, rows, cols] - upd
            pltpu.make_async_copy(stage_i.at[layer, rows], w_in_new.at[layer, rows], sem_i).start()
        mat = 2 * layer
        fac = factor(mat)
        for idx in range(CHUNKS):
            for sub in range(m_loc // 128):
                rows = pl.ds(128 * sub, 128)
                row_scale = sa_ref[mat, rows, :] * fac
                for blk in range(chunk_o // 128):
                    cols = pl.ds(chunk_o * idx + 128 * blk, 128)
                    upd = go_ref[layer, rows, cols] * row_scale * sb_ref[mat, :, cols]
                    stage_o[layer, cols, rows] = wo_ref[layer, cols, rows] - upd.T
            rows = pl.ds(chunk_o * idx, chunk_o)
            pltpu.make_async_copy(stage_o.at[layer, rows], w_out_new.at[layer, rows], sem_o).start()

    with jax.named_scope('k2_body'):
        for layer in range(layers):
            body(layer)
    for copy in stat_copies:
        copy.start()
    with jax.named_scope('k2_wait'):
        pltpu.make_async_copy(stage_i, w_in_new, sem_i).wait()
        pltpu.make_async_copy(stage_o, w_out_new, sem_o).wait()
    for copy in stat_copies:
        copy.wait()


def solution(mesh):
    n_col = mesh.shape['col']
    n_row = mesh.shape['row']
    n_dev = n_col * n_row
    tile_in = P(None, 'row', 'col')
    tile_out = P(None, 'col', 'row')
    lane_row = P(None, None, 'row')
    lane_col = P(None, None, 'col')
    vec_row = P(None, 'row')
    vec_col = P(None, 'col')

    def local_step(hyper_params, w_in, x_in, dy_in, row_in, col_in, w_out, x_out, dy_out, row_out, col_out):
        layers, m_loc, n_loc = w_in.shape
        tokens = x_in.shape[1]
        n_mat = 2 * layers
        len_a, len_b = m_loc * n_row, n_loc * n_col
        dims = (n_col, n_row, layers, m_loc, n_loc, tokens, len_a, len_b)
        hbm = pl.BlockSpec(memory_space=pl.ANY)
        vmem = pl.BlockSpec(memory_space=pltpu.VMEM)
        mid = pl.pallas_call(
            functools.partial(stats_kernel, dims),
            out_shape=[
                pltpu.VMEM((layers, m_loc, n_loc), F32),
                pltpu.VMEM((layers, m_loc, n_loc), F32),
                pltpu.VMEM((layers, m_loc, n_loc), F32),
                pltpu.VMEM((layers, n_loc, m_loc), F32),
                pltpu.VMEM((n_mat, m_loc, 128), F32),
                pltpu.VMEM((n_mat, 1, n_loc), F32),
                pltpu.VMEM((1, 128), F32),
                pltpu.VMEM((2, layers, m_loc), F32),
                pltpu.VMEM((2, layers, n_loc), F32),
            ],
            in_specs=[hbm] * 11,
            out_specs=[vmem] * 9,
            scratch_shapes=[
                pltpu.SMEM((3,), F32),
                pltpu.VMEM((SLOTS, tokens, m_loc), BF16),
                pltpu.VMEM((SLOTS, tokens, n_loc), BF16),
                pltpu.VMEM((2, m_loc, tokens), BF16),
                pltpu.VMEM((2, m_loc, 128), F32),
                pltpu.VMEM((2, m_loc, 128), F32),
                pltpu.VMEM((n_mat, 1, m_loc), F32),
                pltpu.VMEM((n_mat, n_col, 1, m_loc), F32),
                pltpu.VMEM((n_mat, n_row, 1, n_loc), F32),
                pltpu.VMEM((n_dev, 1, 128), F32),
                pltpu.VMEM((1, 128), F32),
                pltpu.VMEM((layers, m_loc), F32),
                pltpu.VMEM((layers, n_loc), F32),
                pltpu.VMEM((layers, n_loc), F32),
                pltpu.VMEM((layers, m_loc), F32),
                pltpu.SemaphoreType.DMA((3,)),
                pltpu.SemaphoreType.DMA((LOOKAHEAD,)),
                pltpu.SemaphoreType.DMA((FIRST,)),
                pltpu.SemaphoreType.DMA((layers + 1,)),
                pltpu.SemaphoreType.DMA((3,)),
                pltpu.SemaphoreType.DMA((3,)),
                pltpu.SemaphoreType.DMA((2,)),
                pltpu.SemaphoreType.DMA((n_mat,)),
                pltpu.SemaphoreType.DMA((1,)),
            ],
            compiler_params=pltpu.CompilerParams(collective_id=0, has_side_effects=True, vmem_limit_bytes=GRANT),
            name='adafactor_stats',
        )(*[pltpu.with_memory_space_constraint(item, pltpu.HBM) for item in (
            hyper_params, w_in, x_in, dy_in, row_in, col_in, w_out, x_out, dy_out, row_out, col_out)])
        mid = [pltpu.with_memory_space_constraint(item, pltpu.VMEM) for item in mid]
        out = pl.pallas_call(
            functools.partial(update_kernel, (layers, m_loc, n_loc)),
            out_shape=[
                jax.ShapeDtypeStruct(w_in.shape, F32),
                jax.ShapeDtypeStruct(row_in.shape, F32),
                jax.ShapeDtypeStruct(col_in.shape, F32),
                jax.ShapeDtypeStruct(w_out.shape, F32),
                jax.ShapeDtypeStruct(row_out.shape, F32),
                jax.ShapeDtypeStruct(col_out.shape, F32),
            ],
            in_specs=[vmem] * 9,
            out_specs=[hbm] * 6,
            scratch_shapes=[
                pltpu.VMEM((layers, m_loc, n_loc), F32),
                pltpu.VMEM((layers, n_loc, m_loc), F32),
                pltpu.SemaphoreType.DMA,
                pltpu.SemaphoreType.DMA,
                pltpu.SemaphoreType.DMA((4,)),
            ],
            compiler_params=pltpu.CompilerParams(vmem_limit_bytes=GRANT),
            name='adafactor_update',
        )(*mid)
        return tuple(out)

    return jax.shard_map(local_step, mesh=mesh, in_specs=(P(), tile_in, lane_row, lane_col, vec_row, vec_col, tile_out, lane_col, lane_row, vec_col, vec_row), out_specs=(tile_in, vec_row, vec_col, tile_out, vec_col, vec_row), check_vma=False)
```

```python
import functools

import jax
import jax.numpy as jnp
from jax import lax
from jax.experimental import pallas as pl
from jax.experimental.pallas import tpu as pltpu
from jax.sharding import PartitionSpec as P

EPS_ONE = 1e-30
EPS_TWO = 1e-3
F32 = jnp.float32
BF16 = jnp.bfloat16
MESH = pl.DeviceIdType.MESH
LOOKAHEAD = 2
SLOTS = 4
FIRST = 2
W_AT = {2: (0, 1), 1: (2, 3), 0: (4, 5, 6, 7)}
CHUNKS = 4
T_SCALE = 2.0 ** -16
GRANT = 24 * 2**20


def stats_kernel(dims, hp_hbm, w_in, x_in, dy_in, row_in, col_in, w_out, x_out, dy_out, row_out, col_out,
                 gi_ref, go_ref, wi_ref, wo_ref, sa_ref, sb_ref, fac_ref, na_ref, nb_ref,
                 hp_ref, small_ref, big_ref, xt_ref, acc_ref, tot_ref, row_ref, rec_a, rec_b, rec_s, pay_ref,
                 old_ri, old_ci, old_ro, old_co,
                 small_sem, big_sem, first_sem, w_sem, old_sem, send_sem, recv_a, recv_b, recv_s):
    n_col, n_row, layers, m_loc, n_loc, tokens, len_a, len_b = dims
    n_mat = 2 * layers
    n_dev = n_col * n_row
    my_col = lax.axis_index('col')
    my_row = lax.axis_index('row')
    me = my_col * n_row + my_row
    peer_col = [lax.rem(my_col + step, n_col) for step in range(n_col)]
    peer_row = [lax.rem(my_row + step, n_row) for step in range(n_row)]
    first_cols = n_loc // FIRST

    def small_copy(mat):
        src = (x_in if mat % 2 else dy_out).at[mat // 2]
        return pltpu.make_async_copy(src, small_ref.at[mat % SLOTS], small_sem.at[mat % 3])

    def big_copy(mat):
        src = (dy_in if mat % 2 else x_out).at[mat // 2]
        return pltpu.make_async_copy(src, big_ref.at[mat % SLOTS], big_sem.at[mat % LOOKAHEAD])

    def first_copy(idx):
        cols = pl.ds(first_cols * idx, first_cols)
        return pltpu.make_async_copy(x_out.at[0, :, cols], big_ref.at[0, :, cols], first_sem.at[idx])

    half = m_loc // 2

    def start_w(mat):
        src, dst = (w_in, wi_ref) if mat % 2 else (w_out, wo_ref)
        src, dst = src.at[mat // 2], dst.at[mat // 2]
        if mat < n_mat - 1:
            sem = 0 if mat < n_mat - 4 else 1 if mat < n_mat - 2 else 2
            pltpu.make_async_copy(src, dst, w_sem.at[sem]).start()
        else:
            for idx in range(2):
                rows = pl.ds(half * idx, half)
                pltpu.make_async_copy(src.at[rows], dst.at[rows], w_sem.at[3 + idx]).start()

    small_copy(0).start()
    for idx in range(FIRST):
        first_copy(idx).start()
    small_copy(1).start()
    big_copy(1).start()
    small_copy(2).start()
    old_copies = [pltpu.make_async_copy(src, dst, old_sem.at[k]) for src, dst, k in (
        (row_in, old_ri, 0), (col_out, old_co, 0), (col_in, old_ci, 1), (row_out, old_ro, 1), (hp_hbm, hp_ref, 2))]
    for copy in old_copies:
        copy.start()
    barrier = pltpu.get_barrier_semaphore()
    for col in range(n_col):
        for row in range(n_row):
            pl.semaphore_signal(barrier, inc=1, device_id=(col, row), device_id_type=MESH)

    def send_round(mat):
        for step in range(1, n_col):
            pltpu.make_async_remote_copy(
                rec_a.at[mat, my_col], rec_a.at[mat, my_col], send_sem.at[0], recv_a.at[mat // (n_mat - 2)],
                device_id=(peer_col[step], my_row), device_id_type=MESH).start()
        for step in range(1, n_row):
            pltpu.make_async_remote_copy(
                rec_b.at[mat, my_row], rec_b.at[mat, my_row], send_sem.at[1], recv_b.at[mat // (n_mat - 2)],
                device_id=(my_col, peer_row[step]), device_id_type=MESH).start()

    def send_scalars():
        rec = rec_s.at[me]

        def send(col, row):
            pltpu.make_async_remote_copy(
                rec, rec, send_sem.at[2], recv_s.at[0], device_id=(col, row), device_id_type=MESH).start()

        for pair in range(n_col // 2):
            same = 2 * pair + lax.rem(my_col, 2)
            other = 2 * pair + 1 - lax.rem(my_col, 2)

            @pl.when(same != my_col)
            def _():
                send(same, my_row)

            for row in range(1, n_row):
                send(same, peer_row[row])
            for row in range(n_row):
                send(other, peer_row[row])

    def take(ref, sem):
        pltpu.make_async_copy(ref, ref, sem).wait()

    def take_a(group):
        first, count = (n_mat - 2, 2) if group else (0, n_mat - 2)
        take(rec_a.at[pl.ds(first, count), pl.ds(0, n_col - 1)], recv_a.at[group])

    def take_b(group):
        first, count = (n_mat - 2, 2) if group else (0, n_mat - 2)
        take(rec_b.at[pl.ds(first, count), pl.ds(0, n_row - 1)], recv_b.at[group])

    lane = lax.broadcasted_iota(jnp.int32, (1, 128), 1)

    def put(place, val):
        pay_ref[...] = jnp.where(lane == place, val, pay_ref[...])

    pay_ref[...] = jnp.zeros_like(pay_ref)

    def g_of(mat):
        return (gi_ref if mat % 2 else go_ref).at[mat // 2]

    def row_sums(mat):
        rec_a[mat, my_col] = jnp.sum(acc_ref[mat % 2].T, axis=0, keepdims=True)

    def transpose_small(mat):
        xt_ref[mat % 2] = small_ref[mat % SLOTS].T

    def new_b(mat):
        beta = hp_ref[0]
        total = rec_b[mat, 0]
        for idx in range(1, n_row):
            total += rec_b[mat, idx]
        layer = mat // 2
        old = (old_ci if mat % 2 else old_ro)[pl.ds(layer, 1), :]
        new = beta * old + (1.0 - beta) * (total / len_a + EPS_ONE)
        nb_ref[mat % 2, pl.ds(layer, 1), :] = new
        sb_ref[mat] = lax.rsqrt(new)
        if mat % 2 == 0:
            put(n_mat + mat, jnp.sum(new, axis=1, keepdims=True) / n_loc)

    def square_piece(mat, idx):
        grad = g_of(mat)
        rows = pl.ds(m_loc // 8 * idx, m_loc // 8)
        acc = jnp.zeros((m_loc // 8, 128), F32)
        for blk in range(n_loc // 128):
            cols = pl.ds(128 * blk, 128)
            upd = grad[rows, cols] * sb_ref[mat, :, cols]
            acc += upd * upd
        tot_ref[mat % 2, rows, :] = acc

    def new_a(mat):
        beta = hp_ref[0]
        total = rec_a[mat, 0]
        for idx in range(1, n_col):
            total += rec_a[mat, idx]
        layer = mat // 2
        old = (old_ri if mat % 2 else old_co)[pl.ds(layer, 1), :]
        new = beta * old + (1.0 - beta) * (total / len_b + EPS_ONE)
        na_ref[mat % 2, pl.ds(layer, 1), :] = new
        inv = lax.rsqrt(new)
        put(mat, jnp.sum(row_ref[mat] * (inv * inv), axis=1, keepdims=True))
        if mat % 2:
            put(n_mat + mat, jnp.sum(new, axis=1, keepdims=True) / m_loc)

    def scale_a(mat):
        new = na_ref[mat % 2, pl.ds(mat // 2, 1), :]
        sa_ref[mat] = jnp.broadcast_to(lax.rsqrt(new), (128, m_loc)).T

    def weight_sum(mat, part=None):
        ref = (wi_ref if mat % 2 else wo_ref).at[mat // 2]
        if part is not None:
            ref = ref.at[pl.ds(half * part, half)]
        rows_all, cols_all = ref.shape
        total = jnp.zeros((8, 128), F32)
        for idx in range(rows_all // 32):
            val = ref[pl.ds(32 * idx, 32), :]
            sq = jnp.sum((val * val).reshape(4, 8, cols_all), axis=0)
            for blk in range(cols_all // 128):
                total += sq[:, 128 * blk:128 * (blk + 1)]
        return total

    def put_weight(mat, total):
        one = jnp.sum(total, axis=0, keepdims=True)
        put(2 * n_mat + mat, jnp.sum(one, axis=1, keepdims=True))

    def product_piece(mat, blk):
        cols = pl.ds(256 * blk, 256)
        grad = jnp.dot(xt_ref[mat % 2], big_ref[mat % SLOTS, :, cols], preferred_element_type=F32)
        g_of(mat)[:, cols] = grad
        sq = grad * grad
        rec_b[mat, my_row, :, cols] = jnp.sum(sq, axis=0, keepdims=True)
        lanes = sq[:, :128] + sq[:, 128:]
        if blk == 0:
            acc_ref[mat % 2] = lanes
        else:
            acc_ref[mat % 2] += lanes

    def load_ahead(mat):
        if mat < n_mat:
            big_copy(mat).start()
        if mat + 1 < n_mat:
            small_copy(mat + 1).start()

    last = n_mat - 1
    pieces = n_loc // 256
    for mat in range(n_mat):
        with jax.named_scope(f'step#m={mat}'):
            with jax.named_scope(f'wait#m={mat}'):
                if mat == 0:
                    small_copy(0).wait()
                    transpose_small(0)
                    first_copy(0).wait()
                    load_ahead(2)
                else:
                    big_copy(mat).wait()
                    load_ahead(mat + LOOKAHEAD)
                    if mat < last:
                        small_copy(mat + 1).wait()
                if mat == 1:
                    pl.semaphore_wait(barrier, n_dev)
                if mat == last:
                    take(na_ref, old_sem.at[0])
                    take(nb_ref, old_sem.at[1])
                    old_copies[-1].wait()
            for idx in W_AT.get(last - mat, ()):
                start_w(idx)
            if mat > 0:
                row_sums(mat - 1)
                if mat < last:
                    transpose_small(mat + 1)
            for blk in range(pieces):
                if mat == 0 and blk and (256 * blk) % first_cols == 0:
                    first_copy(256 * blk // first_cols).wait()
                    small_copy(1).wait()
                    transpose_small(1)
                product_piece(mat, blk)
            if mat > 0:
                send_round(mat - 1)
    with jax.named_scope('last_send'):
        row_sums(last)
        send_round(last)

    def second_pass(mat):
        new_b(mat)
        for idx in range(8):
            square_piece(mat, idx)
        row_ref[mat] = jnp.sum(tot_ref[mat % 2].T, axis=0, keepdims=True) * T_SCALE

    with jax.named_scope('left#m=0'):
        with jax.named_scope('wait_b#m=0'):
            take_b(0)
        for mat in range(n_mat - 2):
            second_pass(mat)
    with jax.named_scope('left#m=1'):
        with jax.named_scope('wait_w#m=0'):
            take(wi_ref.at[pl.ds(0, n_mat - 4)], w_sem.at[0])
        for mat in range(n_mat - 4):
            put_weight(mat, weight_sum(mat))
    with jax.named_scope('left#m=2'):
        with jax.named_scope('wait_b#m=1'):
            take_b(1)
        with jax.named_scope('wait_w#m=1'):
            take(wi_ref.at[pl.ds(0, 2)], w_sem.at[1])
        for mat in (n_mat - 2, n_mat - 1):
            second_pass(mat)
        for mat in (n_mat - 4, n_mat - 3):
            put_weight(mat, weight_sum(mat))
    with jax.named_scope('left#m=3'):
        with jax.named_scope('wait_a#m=0'):
            take_a(0)
        with jax.named_scope('wait_w#m=2'):
            take(wi_ref.at[pl.ds(0, 1)], w_sem.at[2])
        for mat in range(n_mat - 2):
            new_a(mat)
        put_weight(last - 1, weight_sum(last - 1))
    with jax.named_scope('left#m=4'):
        with jax.named_scope('wait_w#m=3'):
            take(wi_ref.at[0, pl.ds(0, half)], w_sem.at[3])
        part = weight_sum(last, 0)
        acc_ref[0, 0:8, :] = part
    with jax.named_scope('last_w'):
        with jax.named_scope('wait_w#m=4'):
            take(wi_ref.at[0, pl.ds(0, half)], w_sem.at[4])
        put_weight(last, acc_ref[0, 0:8, :] + weight_sum(last, 1))

    with jax.named_scope('last_wait'):
        take_a(1)
    with jax.named_scope('last_stats'):
        new_a(last - 1)
        new_a(last)
    with jax.named_scope('s_send'):
        rec_s[me] = pay_ref[...]
        send_scalars()
    with jax.named_scope('scales'):
        for mat in range(n_mat):
            scale_a(mat)
        take(rec_a.at[:, pl.ds(0, n_col - 1)], send_sem.at[0])
        take(rec_b.at[:, pl.ds(0, n_row - 1)], send_sem.at[1])
        take(rec_s.at[pl.ds(0, n_dev - 1)], send_sem.at[2])
    with jax.named_scope('s_wait'):
        take(rec_s.at[pl.ds(0, n_dev - 1)], recv_s.at[0])
    parts = [rec_s[dev] for dev in range(n_dev)]
    while len(parts) > 1:
        parts = [parts[k] + parts[k + 1] for k in range(0, len(parts), 2)]
    total = parts[0]
    mean_s = pltpu.roll(total, 128 - n_mat, 1) / n_dev
    w_sum = pltpu.roll(total, 128 - 2 * n_mat, 1)
    n_total = float(len_a * len_b)
    upd_rms = jnp.sqrt(total * mean_s / (T_SCALE * n_total))
    w_rms = jnp.sqrt(w_sum / n_total)
    step_size = hp_ref[1] * jnp.maximum(EPS_TWO, w_rms) / jnp.maximum(1.0, upd_rms / hp_ref[2])
    fac_ref[...] = jnp.where(lane < n_mat, step_size * jnp.sqrt(mean_s), 0.0)


def update_kernel(dims, gi_ref, go_ref, wi_ref, wo_ref, sa_ref, sb_ref, fac_ref, na_ref, nb_ref,
                  w_in_new, row_in_new, col_in_new, w_out_new, row_out_new, col_out_new,
                  stage_i, stage_o, sem_i, sem_o, stat_sem):
    layers, m_loc, n_loc = dims
    lane = lax.broadcasted_iota(jnp.int32, (1, 128), 1)
    chunk_i = m_loc // CHUNKS
    chunk_o = n_loc // CHUNKS
    stat_copies = [pltpu.make_async_copy(src, dst, stat_sem.at[k]) for k, (src, dst) in enumerate(
        ((na_ref.at[1], row_in_new), (nb_ref.at[1], col_in_new), (nb_ref.at[0], row_out_new), (na_ref.at[0], col_out_new)))]

    def factor(mat):
        return jnp.sum(jnp.where(lane == mat, fac_ref[...], 0.0), axis=1, keepdims=True)

    def body(layer):
        mat = 2 * layer + 1
        fac = factor(mat)
        edges = ([0, 16] if layer == 0 else [0]) + [chunk_i * idx for idx in range(1, CHUNKS + 1)]
        for low, high in zip(edges, edges[1:]):
            rows = pl.ds(low, high - low)
            row_scale = sa_ref[mat, rows, :] * fac
            for blk in range(n_loc // 128):
                cols = pl.ds(128 * blk, 128)
                upd = gi_ref[layer, rows, cols] * row_scale * sb_ref[mat, :, cols]
                stage_i[layer, rows, cols] = wi_ref[layer, rows, cols] - upd
            pltpu.make_async_copy(stage_i.at[layer, rows], w_in_new.at[layer, rows], sem_i).start()
        mat = 2 * layer
        fac = factor(mat)
        for idx in range(CHUNKS):
            for sub in range(m_loc // 128):
                rows = pl.ds(128 * sub, 128)
                row_scale = sa_ref[mat, rows, :] * fac
                for blk in range(chunk_o // 128):
                    cols = pl.ds(chunk_o * idx + 128 * blk, 128)
                    upd = go_ref[layer, rows, cols] * row_scale * sb_ref[mat, :, cols]
                    stage_o[layer, cols, rows] = wo_ref[layer, cols, rows] - upd.T
            rows = pl.ds(chunk_o * idx, chunk_o)
            pltpu.make_async_copy(stage_o.at[layer, rows], w_out_new.at[layer, rows], sem_o).start()

    with jax.named_scope('k2_body'):
        for layer in range(layers):
            body(layer)
    for copy in stat_copies:
        copy.start()
    with jax.named_scope('k2_wait'):
        pltpu.make_async_copy(stage_i, w_in_new, sem_i).wait()
        pltpu.make_async_copy(stage_o, w_out_new, sem_o).wait()
    for copy in stat_copies:
        copy.wait()


def solution(mesh):
    n_col = mesh.shape['col']
    n_row = mesh.shape['row']
    n_dev = n_col * n_row
    tile_in = P(None, 'row', 'col')
    tile_out = P(None, 'col', 'row')
    lane_row = P(None, None, 'row')
    lane_col = P(None, None, 'col')
    vec_row = P(None, 'row')
    vec_col = P(None, 'col')

    def local_step(hyper_params, w_in, x_in, dy_in, row_in, col_in, w_out, x_out, dy_out, row_out, col_out):
        layers, m_loc, n_loc = w_in.shape
        tokens = x_in.shape[1]
        n_mat = 2 * layers
        len_a, len_b = m_loc * n_row, n_loc * n_col
        dims = (n_col, n_row, layers, m_loc, n_loc, tokens, len_a, len_b)
        hbm = pl.BlockSpec(memory_space=pl.ANY)
        vmem = pl.BlockSpec(memory_space=pltpu.VMEM)
        mid = pl.pallas_call(
            functools.partial(stats_kernel, dims),
            out_shape=[
                pltpu.VMEM((layers, m_loc, n_loc), F32),
                pltpu.VMEM((layers, m_loc, n_loc), F32),
                pltpu.VMEM((layers, m_loc, n_loc), F32),
                pltpu.VMEM((layers, n_loc, m_loc), F32),
                pltpu.VMEM((n_mat, m_loc, 128), F32),
                pltpu.VMEM((n_mat, 1, n_loc), F32),
                pltpu.VMEM((1, 128), F32),
                pltpu.VMEM((2, layers, m_loc), F32),
                pltpu.VMEM((2, layers, n_loc), F32),
            ],
            in_specs=[hbm] * 11,
            out_specs=[vmem] * 9,
            scratch_shapes=[
                pltpu.SMEM((3,), F32),
                pltpu.VMEM((SLOTS, tokens, m_loc), BF16),
                pltpu.VMEM((SLOTS, tokens, n_loc), BF16),
                pltpu.VMEM((2, m_loc, tokens), BF16),
                pltpu.VMEM((2, m_loc, 128), F32),
                pltpu.VMEM((2, m_loc, 128), F32),
                pltpu.VMEM((n_mat, 1, m_loc), F32),
                pltpu.VMEM((n_mat, n_col, 1, m_loc), F32),
                pltpu.VMEM((n_mat, n_row, 1, n_loc), F32),
                pltpu.VMEM((n_dev, 1, 128), F32),
                pltpu.VMEM((1, 128), F32),
                pltpu.VMEM((layers, m_loc), F32),
                pltpu.VMEM((layers, n_loc), F32),
                pltpu.VMEM((layers, n_loc), F32),
                pltpu.VMEM((layers, m_loc), F32),
                pltpu.SemaphoreType.DMA((3,)),
                pltpu.SemaphoreType.DMA((LOOKAHEAD,)),
                pltpu.SemaphoreType.DMA((FIRST,)),
                pltpu.SemaphoreType.DMA((layers + 1,)),
                pltpu.SemaphoreType.DMA((3,)),
                pltpu.SemaphoreType.DMA((3,)),
                pltpu.SemaphoreType.DMA((2,)),
                pltpu.SemaphoreType.DMA((2,)),
                pltpu.SemaphoreType.DMA((1,)),
            ],
            compiler_params=pltpu.CompilerParams(collective_id=0, has_side_effects=True, vmem_limit_bytes=GRANT),
            name='adafactor_stats',
        )(*[pltpu.with_memory_space_constraint(item, pltpu.HBM) for item in (
            hyper_params, w_in, x_in, dy_in, row_in, col_in, w_out, x_out, dy_out, row_out, col_out)])
        mid = [pltpu.with_memory_space_constraint(item, pltpu.VMEM) for item in mid]
        out = pl.pallas_call(
            functools.partial(update_kernel, (layers, m_loc, n_loc)),
            out_shape=[
                jax.ShapeDtypeStruct(w_in.shape, F32),
                jax.ShapeDtypeStruct(row_in.shape, F32),
                jax.ShapeDtypeStruct(col_in.shape, F32),
                jax.ShapeDtypeStruct(w_out.shape, F32),
                jax.ShapeDtypeStruct(row_out.shape, F32),
                jax.ShapeDtypeStruct(col_out.shape, F32),
            ],
            in_specs=[vmem] * 9,
            out_specs=[hbm] * 6,
            scratch_shapes=[
                pltpu.VMEM((layers, m_loc, n_loc), F32),
                pltpu.VMEM((layers, n_loc, m_loc), F32),
                pltpu.SemaphoreType.DMA,
                pltpu.SemaphoreType.DMA,
                pltpu.SemaphoreType.DMA((4,)),
            ],
            compiler_params=pltpu.CompilerParams(vmem_limit_bytes=GRANT),
            name='adafactor_update',
        )(*mid)
        return tuple(out)

    return jax.shard_map(local_step, mesh=mesh, in_specs=(P(), tile_in, lane_row, lane_col, vec_row, vec_col, tile_out, lane_col, lane_row, vec_col, vec_row), out_specs=(tile_in, vec_row, vec_col, tile_out, vec_col, vec_row), check_vma=False)
```

```python
import functools

import jax
import jax.numpy as jnp
from jax import lax
from jax.experimental import pallas as pl
from jax.experimental.pallas import tpu as pltpu
from jax.sharding import PartitionSpec as P

EPS_ONE = 1e-30
EPS_TWO = 1e-3
F32 = jnp.float32
BF16 = jnp.bfloat16
MESH = pl.DeviceIdType.MESH
LOOKAHEAD = 2
SLOTS = 4
FIRST = 2
W_AT = {2: (0, 1), 1: (2, 3), 0: (4, 5, 6, 7)}
CHUNKS = 4
T_SCALE = 2.0 ** -16
GRANT = 24 * 2**20


def stats_kernel(dims, hp_hbm, w_in, x_in, dy_in, row_in, col_in, w_out, x_out, dy_out, row_out, col_out,
                 gi_ref, go_ref, wi_ref, wo_ref, sa_ref, sb_ref, fac_ref, na_ref, nb_ref,
                 hp_ref, small_ref, big_ref, xt_ref, acc_ref, tot_ref, row_ref, rec_a, rec_b, rec_s, pay_ref,
                 old_ri, old_ci, old_ro, old_co,
                 small_sem, big_sem, first_sem, w_sem, old_sem, send_sem, recv_a, recv_b, recv_s):
    n_col, n_row, layers, m_loc, n_loc, tokens, len_a, len_b = dims
    n_mat = 2 * layers
    n_dev = n_col * n_row
    my_col = lax.axis_index('col')
    my_row = lax.axis_index('row')
    me = my_col * n_row + my_row
    peer_col = [lax.rem(my_col + step, n_col) for step in range(n_col)]
    peer_row = [lax.rem(my_row + step, n_row) for step in range(n_row)]
    first_cols = n_loc // FIRST

    def small_copy(mat):
        src = (x_in if mat % 2 else dy_out).at[mat // 2]
        return pltpu.make_async_copy(src, small_ref.at[mat % SLOTS], small_sem.at[mat % 3])

    def big_copy(mat):
        src = (dy_in if mat % 2 else x_out).at[mat // 2]
        return pltpu.make_async_copy(src, big_ref.at[mat % SLOTS], big_sem.at[mat % LOOKAHEAD])

    def first_copy(idx):
        cols = pl.ds(first_cols * idx, first_cols)
        return pltpu.make_async_copy(x_out.at[0, :, cols], big_ref.at[0, :, cols], first_sem.at[idx])

    half = m_loc // 2

    def start_w(mat):
        src, dst = (w_in, wi_ref) if mat % 2 else (w_out, wo_ref)
        src, dst = src.at[mat // 2], dst.at[mat // 2]
        if mat < n_mat - 1:
            sem = 0 if mat < n_mat - 4 else 1 if mat < n_mat - 2 else 2
            pltpu.make_async_copy(src, dst, w_sem.at[sem]).start()
        else:
            for idx in range(2):
                rows = pl.ds(half * idx, half)
                pltpu.make_async_copy(src.at[rows], dst.at[rows], w_sem.at[3 + idx]).start()

    small_copy(0).start()
    for idx in range(FIRST):
        first_copy(idx).start()
    small_copy(1).start()
    big_copy(1).start()
    small_copy(2).start()
    old_copies = [pltpu.make_async_copy(src, dst, old_sem.at[k]) for src, dst, k in (
        (row_in, old_ri, 0), (col_out, old_co, 0), (col_in, old_ci, 1), (row_out, old_ro, 1), (hp_hbm, hp_ref, 2))]
    for copy in old_copies:
        copy.start()
    barrier = pltpu.get_barrier_semaphore()
    for col in range(n_col):
        for row in range(n_row):
            pl.semaphore_signal(barrier, inc=1, device_id=(col, row), device_id_type=MESH)

    def send_round(mat):
        for step in range(1, n_col):
            pltpu.make_async_remote_copy(
                rec_a.at[mat, my_col], rec_a.at[mat, my_col], send_sem.at[0], recv_a.at[mat // (n_mat - 2)],
                device_id=(peer_col[step], my_row), device_id_type=MESH).start()
        for step in range(1, n_row):
            pltpu.make_async_remote_copy(
                rec_b.at[mat, my_row], rec_b.at[mat, my_row], send_sem.at[1], recv_b.at[mat // (n_mat - 3)],
                device_id=(my_col, peer_row[step]), device_id_type=MESH).start()

    def send_scalars():
        rec = rec_s.at[me]

        def send(col, row):
            pltpu.make_async_remote_copy(
                rec, rec, send_sem.at[2], recv_s.at[0], device_id=(col, row), device_id_type=MESH).start()

        for pair in range(n_col // 2):
            same = 2 * pair + lax.rem(my_col, 2)
            other = 2 * pair + 1 - lax.rem(my_col, 2)

            @pl.when(same != my_col)
            def _():
                send(same, my_row)

            for row in range(1, n_row):
                send(same, peer_row[row])
            for row in range(n_row):
                send(other, peer_row[row])

    def take(ref, sem):
        pltpu.make_async_copy(ref, ref, sem).wait()

    def take_a(group):
        first, count = (n_mat - 2, 2) if group else (0, n_mat - 2)
        take(rec_a.at[pl.ds(first, count), pl.ds(0, n_col - 1)], recv_a.at[group])

    def take_b(group):
        first, count = (n_mat - 3, 3) if group else (0, n_mat - 3)
        take(rec_b.at[pl.ds(first, count), pl.ds(0, n_row - 1)], recv_b.at[group])

    lane = lax.broadcasted_iota(jnp.int32, (1, 128), 1)

    def put(place, val):
        pay_ref[...] = jnp.where(lane == place, val, pay_ref[...])

    pay_ref[...] = jnp.zeros_like(pay_ref)

    def g_of(mat):
        return (gi_ref if mat % 2 else go_ref).at[mat // 2]

    def row_sums(mat):
        rec_a[mat, my_col] = jnp.sum(acc_ref[mat % 2].T, axis=0, keepdims=True)

    def transpose_small(mat):
        xt_ref[mat % 2] = small_ref[mat % SLOTS].T

    def new_b(mat):
        beta = hp_ref[0]
        total = rec_b[mat, 0]
        for idx in range(1, n_row):
            total += rec_b[mat, idx]
        layer = mat // 2
        old = (old_ci if mat % 2 else old_ro)[pl.ds(layer, 1), :]
        new = beta * old + (1.0 - beta) * (total / len_a + EPS_ONE)
        nb_ref[mat % 2, pl.ds(layer, 1), :] = new
        sb_ref[mat] = lax.rsqrt(new)
        if mat % 2 == 0:
            put(n_mat + mat, jnp.sum(new, axis=1, keepdims=True) / n_loc)

    def square_piece(mat, idx):
        grad = g_of(mat)
        rows = pl.ds(m_loc // 8 * idx, m_loc // 8)
        acc = jnp.zeros((m_loc // 8, 128), F32)
        for blk in range(n_loc // 128):
            cols = pl.ds(128 * blk, 128)
            upd = grad[rows, cols] * sb_ref[mat, :, cols]
            acc += upd * upd
        tot_ref[mat % 2, rows, :] = acc

    def new_a(mat):
        beta = hp_ref[0]
        total = rec_a[mat, 0]
        for idx in range(1, n_col):
            total += rec_a[mat, idx]
        layer = mat // 2
        old = (old_ri if mat % 2 else old_co)[pl.ds(layer, 1), :]
        new = beta * old + (1.0 - beta) * (total / len_b + EPS_ONE)
        na_ref[mat % 2, pl.ds(layer, 1), :] = new
        inv = lax.rsqrt(new)
        put(mat, jnp.sum(row_ref[mat] * (inv * inv), axis=1, keepdims=True))
        if mat % 2:
            put(n_mat + mat, jnp.sum(new, axis=1, keepdims=True) / m_loc)

    def scale_a(mat):
        new = na_ref[mat % 2, pl.ds(mat // 2, 1), :]
        sa_ref[mat] = jnp.broadcast_to(lax.rsqrt(new), (128, m_loc)).T

    def weight_sum(mat, part=None):
        ref = (wi_ref if mat % 2 else wo_ref).at[mat // 2]
        if part is not None:
            ref = ref.at[pl.ds(half * part, half)]
        rows_all, cols_all = ref.shape
        total = jnp.zeros((8, 128), F32)
        for idx in range(rows_all // 32):
            val = ref[pl.ds(32 * idx, 32), :]
            sq = jnp.sum((val * val).reshape(4, 8, cols_all), axis=0)
            for blk in range(cols_all // 128):
                total += sq[:, 128 * blk:128 * (blk + 1)]
        return total

    def put_weight(mat, total):
        one = jnp.sum(total, axis=0, keepdims=True)
        put(2 * n_mat + mat, jnp.sum(one, axis=1, keepdims=True))

    def product_piece(mat, blk):
        cols = pl.ds(256 * blk, 256)
        grad = jnp.dot(xt_ref[mat % 2], big_ref[mat % SLOTS, :, cols], preferred_element_type=F32)
        g_of(mat)[:, cols] = grad
        sq = grad * grad
        rec_b[mat, my_row, :, cols] = jnp.sum(sq, axis=0, keepdims=True)
        lanes = sq[:, :128] + sq[:, 128:]
        if blk == 0:
            acc_ref[mat % 2] = lanes
        else:
            acc_ref[mat % 2] += lanes

    def load_ahead(mat):
        if mat < n_mat:
            big_copy(mat).start()
        if mat + 1 < n_mat:
            small_copy(mat + 1).start()

    last = n_mat - 1
    pieces = n_loc // 256
    for mat in range(n_mat):
        with jax.named_scope(f'step#m={mat}'):
            with jax.named_scope(f'wait#m={mat}'):
                if mat == 0:
                    small_copy(0).wait()
                    transpose_small(0)
                    first_copy(0).wait()
                    load_ahead(2)
                else:
                    big_copy(mat).wait()
                    load_ahead(mat + LOOKAHEAD)
                    if mat < last:
                        small_copy(mat + 1).wait()
                if mat == 1:
                    pl.semaphore_wait(barrier, n_dev)
                if mat == last:
                    take(na_ref, old_sem.at[0])
                    take(nb_ref, old_sem.at[1])
                    old_copies[-1].wait()
            for idx in W_AT.get(last - mat, ()):
                start_w(idx)
            if mat > 0:
                row_sums(mat - 1)
                if mat < last:
                    transpose_small(mat + 1)
            for blk in range(pieces):
                if mat == 0 and blk and (256 * blk) % first_cols == 0:
                    first_copy(256 * blk // first_cols).wait()
                    small_copy(1).wait()
                    transpose_small(1)
                product_piece(mat, blk)
            if mat > 0:
                send_round(mat - 1)
    with jax.named_scope('last_send'):
        row_sums(last)
        send_round(last)

    def second_pass(mat):
        new_b(mat)
        for idx in range(8):
            square_piece(mat, idx)
        row_ref[mat] = jnp.sum(tot_ref[mat % 2].T, axis=0, keepdims=True) * T_SCALE

    with jax.named_scope('left#m=0'):
        with jax.named_scope('wait_b#m=0'):
            take_b(0)
        for mat in range(n_mat - 3):
            second_pass(mat)
    with jax.named_scope('left#m=1'):
        with jax.named_scope('wait_w#m=0'):
            take(wi_ref.at[pl.ds(0, n_mat - 4)], w_sem.at[0])
        for mat in range(n_mat - 4):
            put_weight(mat, weight_sum(mat))
    with jax.named_scope('left#m=2'):
        with jax.named_scope('wait_b#m=1'):
            take_b(1)
        for mat in range(n_mat - 3, n_mat):
            second_pass(mat)
        with jax.named_scope('wait_w#m=1'):
            take(wi_ref.at[pl.ds(0, 2)], w_sem.at[1])
        for mat in (n_mat - 4, n_mat - 3):
            put_weight(mat, weight_sum(mat))
    with jax.named_scope('left#m=3'):
        with jax.named_scope('wait_a#m=0'):
            take_a(0)
        with jax.named_scope('wait_w#m=2'):
            take(wi_ref.at[pl.ds(0, 1)], w_sem.at[2])
        for mat in range(n_mat - 2):
            new_a(mat)
        put_weight(last - 1, weight_sum(last - 1))
    with jax.named_scope('left#m=4'):
        with jax.named_scope('wait_w#m=3'):
            take(wi_ref.at[0, pl.ds(0, half)], w_sem.at[3])
        part = weight_sum(last, 0)
        acc_ref[0, 0:8, :] = part
    with jax.named_scope('last_w'):
        with jax.named_scope('wait_w#m=4'):
            take(wi_ref.at[0, pl.ds(0, half)], w_sem.at[4])
        put_weight(last, acc_ref[0, 0:8, :] + weight_sum(last, 1))

    with jax.named_scope('last_wait'):
        take_a(1)
    with jax.named_scope('last_stats'):
        new_a(last - 1)
        new_a(last)
    with jax.named_scope('s_send'):
        rec_s[me] = pay_ref[...]
        send_scalars()
    with jax.named_scope('scales'):
        for mat in range(n_mat):
            scale_a(mat)
        take(rec_a.at[:, pl.ds(0, n_col - 1)], send_sem.at[0])
        take(rec_b.at[:, pl.ds(0, n_row - 1)], send_sem.at[1])
        take(rec_s.at[pl.ds(0, n_dev - 1)], send_sem.at[2])
    with jax.named_scope('s_wait'):
        take(rec_s.at[pl.ds(0, n_dev - 1)], recv_s.at[0])
    parts = [rec_s[dev] for dev in range(n_dev)]
    while len(parts) > 1:
        parts = [parts[k] + parts[k + 1] for k in range(0, len(parts), 2)]
    total = parts[0]
    mean_s = pltpu.roll(total, 128 - n_mat, 1) / n_dev
    w_sum = pltpu.roll(total, 128 - 2 * n_mat, 1)
    n_total = float(len_a * len_b)
    upd_rms = jnp.sqrt(total * mean_s / (T_SCALE * n_total))
    w_rms = jnp.sqrt(w_sum / n_total)
    step_size = hp_ref[1] * jnp.maximum(EPS_TWO, w_rms) / jnp.maximum(1.0, upd_rms / hp_ref[2])
    fac_ref[...] = jnp.where(lane < n_mat, step_size * jnp.sqrt(mean_s), 0.0)


def update_kernel(dims, gi_ref, go_ref, wi_ref, wo_ref, sa_ref, sb_ref, fac_ref, na_ref, nb_ref,
                  w_in_new, row_in_new, col_in_new, w_out_new, row_out_new, col_out_new,
                  stage_i, stage_o, sem_i, sem_o, stat_sem):
    layers, m_loc, n_loc = dims
    lane = lax.broadcasted_iota(jnp.int32, (1, 128), 1)
    chunk_i = m_loc // CHUNKS
    chunk_o = n_loc // CHUNKS
    stat_copies = [pltpu.make_async_copy(src, dst, stat_sem.at[k]) for k, (src, dst) in enumerate(
        ((na_ref.at[1], row_in_new), (nb_ref.at[1], col_in_new), (nb_ref.at[0], row_out_new), (na_ref.at[0], col_out_new)))]

    def factor(mat):
        return jnp.sum(jnp.where(lane == mat, fac_ref[...], 0.0), axis=1, keepdims=True)

    def body(layer):
        mat = 2 * layer + 1
        fac = factor(mat)
        edges = ([0, 16] if layer == 0 else [0]) + [chunk_i * idx for idx in range(1, CHUNKS + 1)]
        for low, high in zip(edges, edges[1:]):
            rows = pl.ds(low, high - low)
            row_scale = sa_ref[mat, rows, :] * fac
            for blk in range(n_loc // 128):
                cols = pl.ds(128 * blk, 128)
                upd = gi_ref[layer, rows, cols] * row_scale * sb_ref[mat, :, cols]
                stage_i[layer, rows, cols] = wi_ref[layer, rows, cols] - upd
            pltpu.make_async_copy(stage_i.at[layer, rows], w_in_new.at[layer, rows], sem_i).start()
        mat = 2 * layer
        fac = factor(mat)
        for idx in range(CHUNKS):
            for sub in range(m_loc // 128):
                rows = pl.ds(128 * sub, 128)
                row_scale = sa_ref[mat, rows, :] * fac
                for blk in range(chunk_o // 128):
                    cols = pl.ds(chunk_o * idx + 128 * blk, 128)
                    upd = go_ref[layer, rows, cols] * row_scale * sb_ref[mat, :, cols]
                    stage_o[layer, cols, rows] = wo_ref[layer, cols, rows] - upd.T
            rows = pl.ds(chunk_o * idx, chunk_o)
            pltpu.make_async_copy(stage_o.at[layer, rows], w_out_new.at[layer, rows], sem_o).start()

    with jax.named_scope('k2_body'):
        for layer in range(layers):
            body(layer)
    for copy in stat_copies:
        copy.start()
    with jax.named_scope('k2_wait'):
        pltpu.make_async_copy(stage_i, w_in_new, sem_i).wait()
        pltpu.make_async_copy(stage_o, w_out_new, sem_o).wait()
    for copy in stat_copies:
        copy.wait()


def solution(mesh):
    n_col = mesh.shape['col']
    n_row = mesh.shape['row']
    n_dev = n_col * n_row
    tile_in = P(None, 'row', 'col')
    tile_out = P(None, 'col', 'row')
    lane_row = P(None, None, 'row')
    lane_col = P(None, None, 'col')
    vec_row = P(None, 'row')
    vec_col = P(None, 'col')

    def local_step(hyper_params, w_in, x_in, dy_in, row_in, col_in, w_out, x_out, dy_out, row_out, col_out):
        layers, m_loc, n_loc = w_in.shape
        tokens = x_in.shape[1]
        n_mat = 2 * layers
        len_a, len_b = m_loc * n_row, n_loc * n_col
        dims = (n_col, n_row, layers, m_loc, n_loc, tokens, len_a, len_b)
        hbm = pl.BlockSpec(memory_space=pl.ANY)
        vmem = pl.BlockSpec(memory_space=pltpu.VMEM)
        mid = pl.pallas_call(
            functools.partial(stats_kernel, dims),
            out_shape=[
                pltpu.VMEM((layers, m_loc, n_loc), F32),
                pltpu.VMEM((layers, m_loc, n_loc), F32),
                pltpu.VMEM((layers, m_loc, n_loc), F32),
                pltpu.VMEM((layers, n_loc, m_loc), F32),
                pltpu.VMEM((n_mat, m_loc, 128), F32),
                pltpu.VMEM((n_mat, 1, n_loc), F32),
                pltpu.VMEM((1, 128), F32),
                pltpu.VMEM((2, layers, m_loc), F32),
                pltpu.VMEM((2, layers, n_loc), F32),
            ],
            in_specs=[hbm] * 11,
            out_specs=[vmem] * 9,
            scratch_shapes=[
                pltpu.SMEM((3,), F32),
                pltpu.VMEM((SLOTS, tokens, m_loc), BF16),
                pltpu.VMEM((SLOTS, tokens, n_loc), BF16),
                pltpu.VMEM((2, m_loc, tokens), BF16),
                pltpu.VMEM((2, m_loc, 128), F32),
                pltpu.VMEM((2, m_loc, 128), F32),
                pltpu.VMEM((n_mat, 1, m_loc), F32),
                pltpu.VMEM((n_mat, n_col, 1, m_loc), F32),
                pltpu.VMEM((n_mat, n_row, 1, n_loc), F32),
                pltpu.VMEM((n_dev, 1, 128), F32),
                pltpu.VMEM((1, 128), F32),
                pltpu.VMEM((layers, m_loc), F32),
                pltpu.VMEM((layers, n_loc), F32),
                pltpu.VMEM((layers, n_loc), F32),
                pltpu.VMEM((layers, m_loc), F32),
                pltpu.SemaphoreType.DMA((3,)),
                pltpu.SemaphoreType.DMA((LOOKAHEAD,)),
                pltpu.SemaphoreType.DMA((FIRST,)),
                pltpu.SemaphoreType.DMA((layers + 1,)),
                pltpu.SemaphoreType.DMA((3,)),
                pltpu.SemaphoreType.DMA((3,)),
                pltpu.SemaphoreType.DMA((2,)),
                pltpu.SemaphoreType.DMA((2,)),
                pltpu.SemaphoreType.DMA((1,)),
            ],
            compiler_params=pltpu.CompilerParams(collective_id=0, has_side_effects=True, vmem_limit_bytes=GRANT),
            name='adafactor_stats',
        )(*[pltpu.with_memory_space_constraint(item, pltpu.HBM) for item in (
            hyper_params, w_in, x_in, dy_in, row_in, col_in, w_out, x_out, dy_out, row_out, col_out)])
        mid = [pltpu.with_memory_space_constraint(item, pltpu.VMEM) for item in mid]
        out = pl.pallas_call(
            functools.partial(update_kernel, (layers, m_loc, n_loc)),
            out_shape=[
                jax.ShapeDtypeStruct(w_in.shape, F32),
                jax.ShapeDtypeStruct(row_in.shape, F32),
                jax.ShapeDtypeStruct(col_in.shape, F32),
                jax.ShapeDtypeStruct(w_out.shape, F32),
                jax.ShapeDtypeStruct(row_out.shape, F32),
                jax.ShapeDtypeStruct(col_out.shape, F32),
            ],
            in_specs=[vmem] * 9,
            out_specs=[hbm] * 6,
            scratch_shapes=[
                pltpu.VMEM((layers, m_loc, n_loc), F32),
                pltpu.VMEM((layers, n_loc, m_loc), F32),
                pltpu.SemaphoreType.DMA,
                pltpu.SemaphoreType.DMA,
                pltpu.SemaphoreType.DMA((4,)),
            ],
            compiler_params=pltpu.CompilerParams(vmem_limit_bytes=GRANT),
            name='adafactor_update',
        )(*mid)
        return tuple(out)

    return jax.shard_map(local_step, mesh=mesh, in_specs=(P(), tile_in, lane_row, lane_col, vec_row, vec_col, tile_out, lane_col, lane_row, vec_col, vec_row), out_specs=(tile_in, vec_row, vec_col, tile_out, vec_col, vec_row), check_vma=False)
```

```python
import functools

import jax
import jax.numpy as jnp
from jax import lax
from jax.experimental import pallas as pl
from jax.experimental.pallas import tpu as pltpu
from jax.sharding import PartitionSpec as P

EPS_ONE = 1e-30
EPS_TWO = 1e-3
F32 = jnp.float32
BF16 = jnp.bfloat16
MESH = pl.DeviceIdType.MESH
LOOKAHEAD = 2
SLOTS = 4
FIRST = 2
W_AT = {2: (0, 1), 1: (2, 3), 0: (4, 5, 6, 7)}
CHUNKS = 4
T_SCALE = 2.0 ** -16
GRANT = 24 * 2**20


def stats_kernel(dims, hp_hbm, w_in, x_in, dy_in, row_in, col_in, w_out, x_out, dy_out, row_out, col_out,
                 gi_ref, go_ref, wi_ref, wo_ref, sa_ref, sb_ref, fac_ref, na_ref, nb_ref,
                 hp_ref, small_ref, big_ref, xt_ref, acc_ref, tot_ref, row_ref, rec_a, rec_b, rec_s, pay_ref,
                 old_ri, old_ci, old_ro, old_co,
                 small_sem, big_sem, first_sem, w_sem, old_sem, send_sem, recv_a, recv_b, recv_s):
    n_col, n_row, layers, m_loc, n_loc, tokens, len_a, len_b = dims
    n_mat = 2 * layers
    n_dev = n_col * n_row
    my_col = lax.axis_index('col')
    my_row = lax.axis_index('row')
    me = my_col * n_row + my_row
    peer_col = [lax.rem(my_col + step, n_col) for step in range(n_col)]
    peer_row = [lax.rem(my_row + step, n_row) for step in range(n_row)]
    first_cols = n_loc // FIRST

    def small_copy(mat):
        src = (x_in if mat % 2 else dy_out).at[mat // 2]
        return pltpu.make_async_copy(src, small_ref.at[mat % SLOTS], small_sem.at[mat % 3])

    def big_copy(mat):
        src = (dy_in if mat % 2 else x_out).at[mat // 2]
        return pltpu.make_async_copy(src, big_ref.at[mat % SLOTS], big_sem.at[mat % LOOKAHEAD])

    def first_copy(idx):
        cols = pl.ds(first_cols * idx, first_cols)
        return pltpu.make_async_copy(x_out.at[0, :, cols], big_ref.at[0, :, cols], first_sem.at[idx])

    half = m_loc // 2

    def start_w(mat):
        src, dst = (w_in, wi_ref) if mat % 2 else (w_out, wo_ref)
        src, dst = src.at[mat // 2], dst.at[mat // 2]
        if mat < n_mat - 1:
            sem = 0 if mat < n_mat - 4 else 1 if mat < n_mat - 2 else 2
            pltpu.make_async_copy(src, dst, w_sem.at[sem]).start()
        else:
            for idx in range(2):
                rows = pl.ds(half * idx, half)
                pltpu.make_async_copy(src.at[rows], dst.at[rows], w_sem.at[3 + idx]).start()

    small_copy(0).start()
    for idx in range(FIRST):
        first_copy(idx).start()
    small_copy(1).start()
    big_copy(1).start()
    small_copy(2).start()
    old_copies = [pltpu.make_async_copy(src, dst, old_sem.at[k]) for src, dst, k in (
        (row_in, old_ri, 0), (col_out, old_co, 0), (col_in, old_ci, 1), (row_out, old_ro, 1), (hp_hbm, hp_ref, 2))]
    for copy in old_copies:
        copy.start()
    barrier = pltpu.get_barrier_semaphore()
    for col in range(n_col):
        for row in range(n_row):
            pl.semaphore_signal(barrier, inc=1, device_id=(col, row), device_id_type=MESH)

    def send_a(mat):
        for step in range(1, n_col):
            pltpu.make_async_remote_copy(
                rec_a.at[mat, my_col], rec_a.at[mat, my_col], send_sem.at[0], recv_a.at[mat // (n_mat - 2)],
                device_id=(peer_col[step], my_row), device_id_type=MESH).start()

    def send_b(mat):
        for step in range(1, n_row):
            pltpu.make_async_remote_copy(
                rec_b.at[mat, my_row], rec_b.at[mat, my_row], send_sem.at[1], recv_b.at[mat // (n_mat - 3)],
                device_id=(my_col, peer_row[step]), device_id_type=MESH).start()

    def send_scalars():
        rec = rec_s.at[me]

        def send(col, row):
            pltpu.make_async_remote_copy(
                rec, rec, send_sem.at[2], recv_s.at[0], device_id=(col, row), device_id_type=MESH).start()

        for pair in range(n_col // 2):
            same = 2 * pair + lax.rem(my_col, 2)
            other = 2 * pair + 1 - lax.rem(my_col, 2)

            @pl.when(same != my_col)
            def _():
                send(same, my_row)

            for row in range(1, n_row):
                send(same, peer_row[row])
            for row in range(n_row):
                send(other, peer_row[row])

    def take(ref, sem):
        pltpu.make_async_copy(ref, ref, sem).wait()

    def take_a(group):
        first, count = (n_mat - 2, 2) if group else (0, n_mat - 2)
        take(rec_a.at[pl.ds(first, count), pl.ds(0, n_col - 1)], recv_a.at[group])

    def take_b(group):
        first, count = (n_mat - 3, 3) if group else (0, n_mat - 3)
        take(rec_b.at[pl.ds(first, count), pl.ds(0, n_row - 1)], recv_b.at[group])

    lane = lax.broadcasted_iota(jnp.int32, (1, 128), 1)

    def put(place, val):
        pay_ref[...] = jnp.where(lane == place, val, pay_ref[...])

    pay_ref[...] = jnp.zeros_like(pay_ref)

    def g_of(mat):
        return (gi_ref if mat % 2 else go_ref).at[mat // 2]

    def row_sums(mat):
        rec_a[mat, my_col] = jnp.sum(acc_ref[mat % 2].T, axis=0, keepdims=True)

    def transpose_small(mat):
        xt_ref[mat % 2] = small_ref[mat % SLOTS].T

    def new_b(mat):
        beta = hp_ref[0]
        total = rec_b[mat, 0]
        for idx in range(1, n_row):
            total += rec_b[mat, idx]
        layer = mat // 2
        old = (old_ci if mat % 2 else old_ro)[pl.ds(layer, 1), :]
        new = beta * old + (1.0 - beta) * (total / len_a + EPS_ONE)
        nb_ref[mat % 2, pl.ds(layer, 1), :] = new
        sb_ref[mat] = lax.rsqrt(new)
        if mat % 2 == 0:
            put(n_mat + mat, jnp.sum(new, axis=1, keepdims=True) / n_loc)

    def square_piece(mat, idx):
        grad = g_of(mat)
        rows = pl.ds(m_loc // 8 * idx, m_loc // 8)
        acc = jnp.zeros((m_loc // 8, 128), F32)
        for blk in range(n_loc // 128):
            cols = pl.ds(128 * blk, 128)
            upd = grad[rows, cols] * sb_ref[mat, :, cols]
            acc += upd * upd
        tot_ref[mat % 2, rows, :] = acc

    def new_a(mat):
        beta = hp_ref[0]
        total = rec_a[mat, 0]
        for idx in range(1, n_col):
            total += rec_a[mat, idx]
        layer = mat // 2
        old = (old_ri if mat % 2 else old_co)[pl.ds(layer, 1), :]
        new = beta * old + (1.0 - beta) * (total / len_b + EPS_ONE)
        na_ref[mat % 2, pl.ds(layer, 1), :] = new
        inv = lax.rsqrt(new)
        put(mat, jnp.sum(row_ref[mat] * (inv * inv), axis=1, keepdims=True))
        if mat % 2:
            put(n_mat + mat, jnp.sum(new, axis=1, keepdims=True) / m_loc)

    def scale_a(mat):
        new = na_ref[mat % 2, pl.ds(mat // 2, 1), :]
        sa_ref[mat] = jnp.broadcast_to(lax.rsqrt(new), (128, m_loc)).T

    def weight_sum(mat, part=None):
        ref = (wi_ref if mat % 2 else wo_ref).at[mat // 2]
        if part is not None:
            ref = ref.at[pl.ds(half * part, half)]
        rows_all, cols_all = ref.shape
        total = jnp.zeros((8, 128), F32)
        for idx in range(rows_all // 32):
            val = ref[pl.ds(32 * idx, 32), :]
            sq = jnp.sum((val * val).reshape(4, 8, cols_all), axis=0)
            for blk in range(cols_all // 128):
                total += sq[:, 128 * blk:128 * (blk + 1)]
        return total

    def put_weight(mat, total):
        one = jnp.sum(total, axis=0, keepdims=True)
        put(2 * n_mat + mat, jnp.sum(one, axis=1, keepdims=True))

    def product_piece(mat, blk):
        cols = pl.ds(256 * blk, 256)
        grad = jnp.dot(xt_ref[mat % 2], big_ref[mat % SLOTS, :, cols], preferred_element_type=F32)
        g_of(mat)[:, cols] = grad
        sq = grad * grad
        rec_b[mat, my_row, :, cols] = jnp.sum(sq, axis=0, keepdims=True)
        lanes = sq[:, :128] + sq[:, 128:]
        if blk == 0:
            acc_ref[mat % 2] = lanes
        else:
            acc_ref[mat % 2] += lanes

    def load_ahead(mat):
        if mat < n_mat:
            big_copy(mat).start()
        if mat + 1 < n_mat:
            small_copy(mat + 1).start()

    last = n_mat - 1
    pieces = n_loc // 256
    for mat in range(n_mat):
        with jax.named_scope(f'step#m={mat}'):
            with jax.named_scope(f'wait#m={mat}'):
                if mat == 0:
                    small_copy(0).wait()
                    transpose_small(0)
                    first_copy(0).wait()
                    load_ahead(2)
                else:
                    big_copy(mat).wait()
                    load_ahead(mat + LOOKAHEAD)
                    if mat < last:
                        small_copy(mat + 1).wait()
                if mat == 1:
                    pl.semaphore_wait(barrier, n_dev)
                if mat == last:
                    take(na_ref, old_sem.at[0])
                    take(nb_ref, old_sem.at[1])
                    old_copies[-1].wait()
            for idx in W_AT.get(last - mat, ()):
                start_w(idx)
            if mat > 0:
                row_sums(mat - 1)
                if mat < last:
                    transpose_small(mat + 1)
            for blk in range(pieces):
                if mat == 0 and blk and (256 * blk) % first_cols == 0:
                    first_copy(256 * blk // first_cols).wait()
                    small_copy(1).wait()
                    transpose_small(1)
                product_piece(mat, blk)
            if mat == 1:
                send_b(0)
            if mat > 0:
                send_b(mat)
                send_a(mat - 1)
    with jax.named_scope('last_send'):
        row_sums(last)
        send_a(last)

    def second_pass(mat):
        new_b(mat)
        for idx in range(8):
            square_piece(mat, idx)
        row_ref[mat] = jnp.sum(tot_ref[mat % 2].T, axis=0, keepdims=True) * T_SCALE

    with jax.named_scope('left#m=0'):
        with jax.named_scope('wait_b#m=0'):
            take_b(0)
        for mat in range(n_mat - 3):
            second_pass(mat)
    with jax.named_scope('left#m=1'):
        with jax.named_scope('wait_w#m=0'):
            take(wi_ref.at[pl.ds(0, n_mat - 4)], w_sem.at[0])
        for mat in range(n_mat - 4):
            put_weight(mat, weight_sum(mat))
    with jax.named_scope('left#m=2'):
        with jax.named_scope('wait_w#m=1'):
            take(wi_ref.at[pl.ds(0, 2)], w_sem.at[1])
        for mat in (n_mat - 4, n_mat - 3):
            put_weight(mat, weight_sum(mat))
        with jax.named_scope('wait_b#m=1'):
            take_b(1)
        for mat in range(n_mat - 3, n_mat):
            second_pass(mat)
    with jax.named_scope('left#m=3'):
        with jax.named_scope('wait_a#m=0'):
            take_a(0)
        with jax.named_scope('wait_w#m=2'):
            take(wi_ref.at[pl.ds(0, 1)], w_sem.at[2])
        for mat in range(n_mat - 2):
            new_a(mat)
        put_weight(last - 1, weight_sum(last - 1))
    with jax.named_scope('left#m=4'):
        with jax.named_scope('wait_w#m=3'):
            take(wi_ref.at[0, pl.ds(0, half)], w_sem.at[3])
        part = weight_sum(last, 0)
        acc_ref[0, 0:8, :] = part
    with jax.named_scope('last_w'):
        with jax.named_scope('wait_w#m=4'):
            take(wi_ref.at[0, pl.ds(0, half)], w_sem.at[4])
        put_weight(last, acc_ref[0, 0:8, :] + weight_sum(last, 1))

    with jax.named_scope('last_wait'):
        take_a(1)
    with jax.named_scope('last_stats'):
        new_a(last - 1)
        new_a(last)
    with jax.named_scope('s_send'):
        rec_s[me] = pay_ref[...]
        send_scalars()
    with jax.named_scope('scales'):
        for mat in range(n_mat):
            scale_a(mat)
        take(rec_a.at[:, pl.ds(0, n_col - 1)], send_sem.at[0])
        take(rec_b.at[:, pl.ds(0, n_row - 1)], send_sem.at[1])
        take(rec_s.at[pl.ds(0, n_dev - 1)], send_sem.at[2])
    with jax.named_scope('s_wait'):
        take(rec_s.at[pl.ds(0, n_dev - 1)], recv_s.at[0])
    parts = [rec_s[dev] for dev in range(n_dev)]
    while len(parts) > 1:
        parts = [parts[k] + parts[k + 1] for k in range(0, len(parts), 2)]
    total = parts[0]
    mean_s = pltpu.roll(total, 128 - n_mat, 1) / n_dev
    w_sum = pltpu.roll(total, 128 - 2 * n_mat, 1)
    n_total = float(len_a * len_b)
    upd_rms = jnp.sqrt(total * mean_s / (T_SCALE * n_total))
    w_rms = jnp.sqrt(w_sum / n_total)
    step_size = hp_ref[1] * jnp.maximum(EPS_TWO, w_rms) / jnp.maximum(1.0, upd_rms / hp_ref[2])
    fac_ref[...] = jnp.where(lane < n_mat, step_size * jnp.sqrt(mean_s), 0.0)


def update_kernel(dims, gi_ref, go_ref, wi_ref, wo_ref, sa_ref, sb_ref, fac_ref, na_ref, nb_ref,
                  w_in_new, row_in_new, col_in_new, w_out_new, row_out_new, col_out_new,
                  stage_i, stage_o, sem_i, sem_o, stat_sem):
    layers, m_loc, n_loc = dims
    lane = lax.broadcasted_iota(jnp.int32, (1, 128), 1)
    chunk_i = m_loc // CHUNKS
    chunk_o = n_loc // CHUNKS
    stat_copies = [pltpu.make_async_copy(src, dst, stat_sem.at[k]) for k, (src, dst) in enumerate(
        ((na_ref.at[1], row_in_new), (nb_ref.at[1], col_in_new), (nb_ref.at[0], row_out_new), (na_ref.at[0], col_out_new)))]

    def factor(mat):
        return jnp.sum(jnp.where(lane == mat, fac_ref[...], 0.0), axis=1, keepdims=True)

    def body(layer):
        mat = 2 * layer + 1
        fac = factor(mat)
        edges = ([0, 16] if layer == 0 else [0]) + [chunk_i * idx for idx in range(1, CHUNKS + 1)]
        for low, high in zip(edges, edges[1:]):
            rows = pl.ds(low, high - low)
            row_scale = sa_ref[mat, rows, :] * fac
            for blk in range(n_loc // 128):
                cols = pl.ds(128 * blk, 128)
                upd = gi_ref[layer, rows, cols] * row_scale * sb_ref[mat, :, cols]
                stage_i[layer, rows, cols] = wi_ref[layer, rows, cols] - upd
            pltpu.make_async_copy(stage_i.at[layer, rows], w_in_new.at[layer, rows], sem_i).start()
        mat = 2 * layer
        fac = factor(mat)
        for idx in range(CHUNKS):
            for sub in range(m_loc // 128):
                rows = pl.ds(128 * sub, 128)
                row_scale = sa_ref[mat, rows, :] * fac
                for blk in range(chunk_o // 128):
                    cols = pl.ds(chunk_o * idx + 128 * blk, 128)
                    upd = go_ref[layer, rows, cols] * row_scale * sb_ref[mat, :, cols]
                    stage_o[layer, cols, rows] = wo_ref[layer, cols, rows] - upd.T
            rows = pl.ds(chunk_o * idx, chunk_o)
            pltpu.make_async_copy(stage_o.at[layer, rows], w_out_new.at[layer, rows], sem_o).start()

    with jax.named_scope('k2_body'):
        for layer in range(layers):
            body(layer)
    for copy in stat_copies:
        copy.start()
    with jax.named_scope('k2_wait'):
        pltpu.make_async_copy(stage_i, w_in_new, sem_i).wait()
        pltpu.make_async_copy(stage_o, w_out_new, sem_o).wait()
    for copy in stat_copies:
        copy.wait()


def solution(mesh):
    n_col = mesh.shape['col']
    n_row = mesh.shape['row']
    n_dev = n_col * n_row
    tile_in = P(None, 'row', 'col')
    tile_out = P(None, 'col', 'row')
    lane_row = P(None, None, 'row')
    lane_col = P(None, None, 'col')
    vec_row = P(None, 'row')
    vec_col = P(None, 'col')

    def local_step(hyper_params, w_in, x_in, dy_in, row_in, col_in, w_out, x_out, dy_out, row_out, col_out):
        layers, m_loc, n_loc = w_in.shape
        tokens = x_in.shape[1]
        n_mat = 2 * layers
        len_a, len_b = m_loc * n_row, n_loc * n_col
        dims = (n_col, n_row, layers, m_loc, n_loc, tokens, len_a, len_b)
        hbm = pl.BlockSpec(memory_space=pl.ANY)
        vmem = pl.BlockSpec(memory_space=pltpu.VMEM)
        mid = pl.pallas_call(
            functools.partial(stats_kernel, dims),
            out_shape=[
                pltpu.VMEM((layers, m_loc, n_loc), F32),
                pltpu.VMEM((layers, m_loc, n_loc), F32),
                pltpu.VMEM((layers, m_loc, n_loc), F32),
                pltpu.VMEM((layers, n_loc, m_loc), F32),
                pltpu.VMEM((n_mat, m_loc, 128), F32),
                pltpu.VMEM((n_mat, 1, n_loc), F32),
                pltpu.VMEM((1, 128), F32),
                pltpu.VMEM((2, layers, m_loc), F32),
                pltpu.VMEM((2, layers, n_loc), F32),
            ],
            in_specs=[hbm] * 11,
            out_specs=[vmem] * 9,
            scratch_shapes=[
                pltpu.SMEM((3,), F32),
                pltpu.VMEM((SLOTS, tokens, m_loc), BF16),
                pltpu.VMEM((SLOTS, tokens, n_loc), BF16),
                pltpu.VMEM((2, m_loc, tokens), BF16),
                pltpu.VMEM((2, m_loc, 128), F32),
                pltpu.VMEM((2, m_loc, 128), F32),
                pltpu.VMEM((n_mat, 1, m_loc), F32),
                pltpu.VMEM((n_mat, n_col, 1, m_loc), F32),
                pltpu.VMEM((n_mat, n_row, 1, n_loc), F32),
                pltpu.VMEM((n_dev, 1, 128), F32),
                pltpu.VMEM((1, 128), F32),
                pltpu.VMEM((layers, m_loc), F32),
                pltpu.VMEM((layers, n_loc), F32),
                pltpu.VMEM((layers, n_loc), F32),
                pltpu.VMEM((layers, m_loc), F32),
                pltpu.SemaphoreType.DMA((3,)),
                pltpu.SemaphoreType.DMA((LOOKAHEAD,)),
                pltpu.SemaphoreType.DMA((FIRST,)),
                pltpu.SemaphoreType.DMA((layers + 1,)),
                pltpu.SemaphoreType.DMA((3,)),
                pltpu.SemaphoreType.DMA((3,)),
                pltpu.SemaphoreType.DMA((2,)),
                pltpu.SemaphoreType.DMA((2,)),
                pltpu.SemaphoreType.DMA((1,)),
            ],
            compiler_params=pltpu.CompilerParams(collective_id=0, has_side_effects=True, vmem_limit_bytes=GRANT),
            name='adafactor_stats',
        )(*[pltpu.with_memory_space_constraint(item, pltpu.HBM) for item in (
            hyper_params, w_in, x_in, dy_in, row_in, col_in, w_out, x_out, dy_out, row_out, col_out)])
        mid = [pltpu.with_memory_space_constraint(item, pltpu.VMEM) for item in mid]
        out = pl.pallas_call(
            functools.partial(update_kernel, (layers, m_loc, n_loc)),
            out_shape=[
                jax.ShapeDtypeStruct(w_in.shape, F32),
                jax.ShapeDtypeStruct(row_in.shape, F32),
                jax.ShapeDtypeStruct(col_in.shape, F32),
                jax.ShapeDtypeStruct(w_out.shape, F32),
                jax.ShapeDtypeStruct(row_out.shape, F32),
                jax.ShapeDtypeStruct(col_out.shape, F32),
            ],
            in_specs=[vmem] * 9,
            out_specs=[hbm] * 6,
            scratch_shapes=[
                pltpu.VMEM((layers, m_loc, n_loc), F32),
                pltpu.VMEM((layers, n_loc, m_loc), F32),
                pltpu.SemaphoreType.DMA,
                pltpu.SemaphoreType.DMA,
                pltpu.SemaphoreType.DMA((4,)),
            ],
            compiler_params=pltpu.CompilerParams(vmem_limit_bytes=GRANT),
            name='adafactor_update',
        )(*mid)
        return tuple(out)

    return jax.shard_map(local_step, mesh=mesh, in_specs=(P(), tile_in, lane_row, lane_col, vec_row, vec_col, tile_out, lane_col, lane_row, vec_col, vec_row), out_specs=(tile_in, vec_row, vec_col, tile_out, vec_col, vec_row), check_vma=False)
```

```python
import functools

import jax
import jax.numpy as jnp
from jax import lax
from jax.experimental import pallas as pl
from jax.experimental.pallas import tpu as pltpu
from jax.sharding import PartitionSpec as P

EPS_ONE = 1e-30
EPS_TWO = 1e-3
F32 = jnp.float32
BF16 = jnp.bfloat16
MESH = pl.DeviceIdType.MESH
LOOKAHEAD = 2
SLOTS = 4
FIRST = 2
W_AT = {2: (0, 1), 1: (2, 3), 0: (4, 5, 6, 7)}
CHUNKS = 4
T_SCALE = 2.0 ** -16
GRANT = 24 * 2**20


def stats_kernel(dims, hp_hbm, w_in, x_in, dy_in, row_in, col_in, w_out, x_out, dy_out, row_out, col_out,
                 gi_ref, go_ref, wi_ref, wo_ref, sa_ref, sb_ref, fac_ref, na_ref, nb_ref,
                 hp_ref, small_ref, big_ref, xt_ref, acc_ref, tot_ref, row_ref, rec_a, rec_b, rec_s, pay_ref,
                 old_ri, old_ci, old_ro, old_co,
                 small_sem, big_sem, first_sem, w_sem, old_sem, send_sem, recv_a, recv_b, recv_s):
    n_col, n_row, layers, m_loc, n_loc, tokens, len_a, len_b = dims
    n_mat = 2 * layers
    n_dev = n_col * n_row
    my_col = lax.axis_index('col')
    my_row = lax.axis_index('row')
    me = my_col * n_row + my_row
    peer_col = [lax.rem(my_col + step, n_col) for step in range(n_col)]
    peer_row = [lax.rem(my_row + step, n_row) for step in range(n_row)]
    first_cols = n_loc // FIRST

    def small_copy(mat):
        src = (x_in if mat % 2 else dy_out).at[mat // 2]
        return pltpu.make_async_copy(src, small_ref.at[mat % SLOTS], small_sem.at[mat % 3])

    def big_copy(mat):
        src = (dy_in if mat % 2 else x_out).at[mat // 2]
        return pltpu.make_async_copy(src, big_ref.at[mat % SLOTS], big_sem.at[mat % LOOKAHEAD])

    def first_copy(idx):
        cols = pl.ds(first_cols * idx, first_cols)
        return pltpu.make_async_copy(x_out.at[0, :, cols], big_ref.at[0, :, cols], first_sem.at[idx])

    half = m_loc // 2

    def start_w(mat):
        src, dst = (w_in, wi_ref) if mat % 2 else (w_out, wo_ref)
        src, dst = src.at[mat // 2], dst.at[mat // 2]
        if mat < n_mat - 1:
            sem = 0 if mat < n_mat - 4 else 1 if mat < n_mat - 2 else 2
            pltpu.make_async_copy(src, dst, w_sem.at[sem]).start()
        else:
            for idx in range(2):
                rows = pl.ds(half * idx, half)
                pltpu.make_async_copy(src.at[rows], dst.at[rows], w_sem.at[3 + idx]).start()

    small_copy(0).start()
    for idx in range(FIRST):
        first_copy(idx).start()
    small_copy(1).start()
    big_copy(1).start()
    small_copy(2).start()
    old_copies = [pltpu.make_async_copy(src, dst, old_sem.at[k]) for src, dst, k in (
        (row_in, old_ri, 0), (col_out, old_co, 0), (col_in, old_ci, 1), (row_out, old_ro, 1), (hp_hbm, hp_ref, 2))]
    for copy in old_copies:
        copy.start()
    barrier = pltpu.get_barrier_semaphore()
    for col in range(n_col):
        for row in range(n_row):
            pl.semaphore_signal(barrier, inc=1, device_id=(col, row), device_id_type=MESH)

    def send_a(mat):
        for step in range(1, n_col):
            pltpu.make_async_remote_copy(
                rec_a.at[mat, my_col], rec_a.at[mat, my_col], send_sem.at[0], recv_a.at[mat // (n_mat - 2)],
                device_id=(peer_col[step], my_row), device_id_type=MESH).start()

    def send_b(mat):
        for step in range(1, n_row):
            pltpu.make_async_remote_copy(
                rec_b.at[mat, my_row], rec_b.at[mat, my_row], send_sem.at[1], recv_b.at[max(0, mat - n_mat + 3)],
                device_id=(my_col, peer_row[step]), device_id_type=MESH).start()

    def send_scalars():
        rec = rec_s.at[me]

        def send(col, row):
            pltpu.make_async_remote_copy(
                rec, rec, send_sem.at[2], recv_s.at[0], device_id=(col, row), device_id_type=MESH).start()

        for pair in range(n_col // 2):
            same = 2 * pair + lax.rem(my_col, 2)
            other = 2 * pair + 1 - lax.rem(my_col, 2)

            @pl.when(same != my_col)
            def _():
                send(same, my_row)

            for row in range(1, n_row):
                send(same, peer_row[row])
            for row in range(n_row):
                send(other, peer_row[row])

    def take(ref, sem):
        pltpu.make_async_copy(ref, ref, sem).wait()

    def take_a(group):
        first, count = (n_mat - 2, 2) if group else (0, n_mat - 2)
        take(rec_a.at[pl.ds(first, count), pl.ds(0, n_col - 1)], recv_a.at[group])

    def take_b(group):
        first, count = (n_mat - 3 + group, 1) if group else (0, n_mat - 2)
        take(rec_b.at[pl.ds(first, count), pl.ds(0, n_row - 1)], recv_b.at[group])

    lane = lax.broadcasted_iota(jnp.int32, (1, 128), 1)

    def put(place, val):
        pay_ref[...] = jnp.where(lane == place, val, pay_ref[...])

    pay_ref[...] = jnp.zeros_like(pay_ref)

    def g_of(mat):
        return (gi_ref if mat % 2 else go_ref).at[mat // 2]

    def row_sums(mat):
        rec_a[mat, my_col] = jnp.sum(acc_ref[mat % 2].T, axis=0, keepdims=True)

    def transpose_small(mat):
        xt_ref[mat % 2] = small_ref[mat % SLOTS].T

    def new_b(mat):
        beta = hp_ref[0]
        total = rec_b[mat, 0]
        for idx in range(1, n_row):
            total += rec_b[mat, idx]
        layer = mat // 2
        old = (old_ci if mat % 2 else old_ro)[pl.ds(layer, 1), :]
        new = beta * old + (1.0 - beta) * (total / len_a + EPS_ONE)
        nb_ref[mat % 2, pl.ds(layer, 1), :] = new
        sb_ref[mat] = lax.rsqrt(new)
        if mat % 2 == 0:
            put(n_mat + mat, jnp.sum(new, axis=1, keepdims=True) / n_loc)

    def square_piece(mat, idx):
        grad = g_of(mat)
        rows = pl.ds(m_loc // 8 * idx, m_loc // 8)
        acc = jnp.zeros((m_loc // 8, 128), F32)
        for blk in range(n_loc // 128):
            cols = pl.ds(128 * blk, 128)
            upd = grad[rows, cols] * sb_ref[mat, :, cols]
            acc += upd * upd
        tot_ref[mat % 2, rows, :] = acc

    def new_a(mat):
        beta = hp_ref[0]
        total = rec_a[mat, 0]
        for idx in range(1, n_col):
            total += rec_a[mat, idx]
        layer = mat // 2
        old = (old_ri if mat % 2 else old_co)[pl.ds(layer, 1), :]
        new = beta * old + (1.0 - beta) * (total / len_b + EPS_ONE)
        na_ref[mat % 2, pl.ds(layer, 1), :] = new
        inv = lax.rsqrt(new)
        put(mat, jnp.sum(row_ref[mat] * (inv * inv), axis=1, keepdims=True))
        if mat % 2:
            put(n_mat + mat, jnp.sum(new, axis=1, keepdims=True) / m_loc)

    def scale_a(mat):
        new = na_ref[mat % 2, pl.ds(mat // 2, 1), :]
        sa_ref[mat] = jnp.broadcast_to(lax.rsqrt(new), (128, m_loc)).T

    def weight_sum(mat, part=None):
        ref = (wi_ref if mat % 2 else wo_ref).at[mat // 2]
        if part is not None:
            ref = ref.at[pl.ds(half * part, half)]
        rows_all, cols_all = ref.shape
        total = jnp.zeros((8, 128), F32)
        for idx in range(rows_all // 32):
            val = ref[pl.ds(32 * idx, 32), :]
            sq = jnp.sum((val * val).reshape(4, 8, cols_all), axis=0)
            for blk in range(cols_all // 128):
                total += sq[:, 128 * blk:128 * (blk + 1)]
        return total

    def put_weight(mat, total):
        one = jnp.sum(total, axis=0, keepdims=True)
        put(2 * n_mat + mat, jnp.sum(one, axis=1, keepdims=True))

    def product_piece(mat, blk):
        cols = pl.ds(256 * blk, 256)
        grad = jnp.dot(xt_ref[mat % 2], big_ref[mat % SLOTS, :, cols], preferred_element_type=F32)
        g_of(mat)[:, cols] = grad
        sq = grad * grad
        rec_b[mat, my_row, :, cols] = jnp.sum(sq, axis=0, keepdims=True)
        lanes = sq[:, :128] + sq[:, 128:]
        if blk == 0:
            acc_ref[mat % 2] = lanes
        else:
            acc_ref[mat % 2] += lanes

    def load_ahead(mat):
        if mat < n_mat:
            big_copy(mat).start()
        if mat + 1 < n_mat:
            small_copy(mat + 1).start()

    last = n_mat - 1
    pieces = n_loc // 256
    for mat in range(n_mat):
        with jax.named_scope(f'step#m={mat}'):
            with jax.named_scope(f'wait#m={mat}'):
                if mat == 0:
                    small_copy(0).wait()
                    transpose_small(0)
                    first_copy(0).wait()
                    load_ahead(2)
                else:
                    big_copy(mat).wait()
                    load_ahead(mat + LOOKAHEAD)
                    if mat < last:
                        small_copy(mat + 1).wait()
                if mat == 1:
                    pl.semaphore_wait(barrier, n_dev)
                if mat == last:
                    take(na_ref, old_sem.at[0])
                    take(nb_ref, old_sem.at[1])
                    old_copies[-1].wait()
            for idx in W_AT.get(last - mat, ()):
                start_w(idx)
            if mat > 0:
                row_sums(mat - 1)
                if mat < last:
                    transpose_small(mat + 1)
            for blk in range(pieces):
                if mat == 0 and blk and (256 * blk) % first_cols == 0:
                    first_copy(256 * blk // first_cols).wait()
                    small_copy(1).wait()
                    transpose_small(1)
                product_piece(mat, blk)
            if mat == 1:
                send_b(0)
            if mat > 0:
                send_b(mat)
                send_a(mat - 1)
    with jax.named_scope('last_send'):
        row_sums(last)
        send_a(last)

    def second_pass(mat):
        new_b(mat)
        for idx in range(8):
            square_piece(mat, idx)
        row_ref[mat] = jnp.sum(tot_ref[mat % 2].T, axis=0, keepdims=True) * T_SCALE

    with jax.named_scope('left#m=0'):
        with jax.named_scope('wait_b#m=0'):
            take_b(0)
        for mat in range(n_mat - 2):
            second_pass(mat)
    with jax.named_scope('left#m=1'):
        with jax.named_scope('wait_w#m=0'):
            take(wi_ref.at[pl.ds(0, n_mat - 4)], w_sem.at[0])
        for mat in range(n_mat - 4):
            put_weight(mat, weight_sum(mat))
    with jax.named_scope('left#m=2'):
        with jax.named_scope('wait_b#m=1'):
            take_b(1)
        second_pass(n_mat - 2)
        with jax.named_scope('wait_w#m=1'):
            take(wi_ref.at[pl.ds(0, 2)], w_sem.at[1])
        for mat in (n_mat - 4, n_mat - 3):
            put_weight(mat, weight_sum(mat))
        with jax.named_scope('wait_b#m=2'):
            take_b(2)
        second_pass(last)
    with jax.named_scope('left#m=3'):
        with jax.named_scope('wait_a#m=0'):
            take_a(0)
        with jax.named_scope('wait_w#m=2'):
            take(wi_ref.at[pl.ds(0, 1)], w_sem.at[2])
        for mat in range(n_mat - 2):
            new_a(mat)
        put_weight(last - 1, weight_sum(last - 1))
    with jax.named_scope('left#m=4'):
        with jax.named_scope('wait_w#m=3'):
            take(wi_ref.at[0, pl.ds(0, half)], w_sem.at[3])
        part = weight_sum(last, 0)
        acc_ref[0, 0:8, :] = part
    with jax.named_scope('last_w'):
        with jax.named_scope('wait_w#m=4'):
            take(wi_ref.at[0, pl.ds(0, half)], w_sem.at[4])
        put_weight(last, acc_ref[0, 0:8, :] + weight_sum(last, 1))

    with jax.named_scope('last_wait'):
        take_a(1)
    with jax.named_scope('last_stats'):
        new_a(last - 1)
        new_a(last)
    with jax.named_scope('s_send'):
        rec_s[me] = pay_ref[...]
        send_scalars()
    with jax.named_scope('scales'):
        for mat in range(n_mat):
            scale_a(mat)
        take(rec_a.at[:, pl.ds(0, n_col - 1)], send_sem.at[0])
        take(rec_b.at[:, pl.ds(0, n_row - 1)], send_sem.at[1])
        take(rec_s.at[pl.ds(0, n_dev - 1)], send_sem.at[2])
    with jax.named_scope('s_wait'):
        take(rec_s.at[pl.ds(0, n_dev - 1)], recv_s.at[0])
    parts = [rec_s[dev] for dev in range(n_dev)]
    while len(parts) > 1:
        parts = [parts[k] + parts[k + 1] for k in range(0, len(parts), 2)]
    total = parts[0]
    mean_s = pltpu.roll(total, 128 - n_mat, 1) / n_dev
    w_sum = pltpu.roll(total, 128 - 2 * n_mat, 1)
    n_total = float(len_a * len_b)
    upd_rms = jnp.sqrt(total * mean_s / (T_SCALE * n_total))
    w_rms = jnp.sqrt(w_sum / n_total)
    step_size = hp_ref[1] * jnp.maximum(EPS_TWO, w_rms) / jnp.maximum(1.0, upd_rms / hp_ref[2])
    fac_ref[...] = jnp.where(lane < n_mat, step_size * jnp.sqrt(mean_s), 0.0)


def update_kernel(dims, gi_ref, go_ref, wi_ref, wo_ref, sa_ref, sb_ref, fac_ref, na_ref, nb_ref,
                  w_in_new, row_in_new, col_in_new, w_out_new, row_out_new, col_out_new,
                  stage_i, stage_o, sem_i, sem_o, stat_sem):
    layers, m_loc, n_loc = dims
    lane = lax.broadcasted_iota(jnp.int32, (1, 128), 1)
    chunk_i = m_loc // CHUNKS
    chunk_o = n_loc // CHUNKS
    stat_copies = [pltpu.make_async_copy(src, dst, stat_sem.at[k]) for k, (src, dst) in enumerate(
        ((na_ref.at[1], row_in_new), (nb_ref.at[1], col_in_new), (nb_ref.at[0], row_out_new), (na_ref.at[0], col_out_new)))]

    def factor(mat):
        return jnp.sum(jnp.where(lane == mat, fac_ref[...], 0.0), axis=1, keepdims=True)

    def body(layer):
        mat = 2 * layer + 1
        fac = factor(mat)
        edges = ([0, 16] if layer == 0 else [0]) + [chunk_i * idx for idx in range(1, CHUNKS + 1)]
        for low, high in zip(edges, edges[1:]):
            rows = pl.ds(low, high - low)
            row_scale = sa_ref[mat, rows, :] * fac
            for blk in range(n_loc // 128):
                cols = pl.ds(128 * blk, 128)
                upd = gi_ref[layer, rows, cols] * row_scale * sb_ref[mat, :, cols]
                stage_i[layer, rows, cols] = wi_ref[layer, rows, cols] - upd
            pltpu.make_async_copy(stage_i.at[layer, rows], w_in_new.at[layer, rows], sem_i).start()
        mat = 2 * layer
        fac = factor(mat)
        for idx in range(CHUNKS):
            for sub in range(m_loc // 128):
                rows = pl.ds(128 * sub, 128)
                row_scale = sa_ref[mat, rows, :] * fac
                for blk in range(chunk_o // 128):
                    cols = pl.ds(chunk_o * idx + 128 * blk, 128)
                    upd = go_ref[layer, rows, cols] * row_scale * sb_ref[mat, :, cols]
                    stage_o[layer, cols, rows] = wo_ref[layer, cols, rows] - upd.T
            rows = pl.ds(chunk_o * idx, chunk_o)
            pltpu.make_async_copy(stage_o.at[layer, rows], w_out_new.at[layer, rows], sem_o).start()

    with jax.named_scope('k2_body'):
        for layer in range(layers):
            body(layer)
    for copy in stat_copies:
        copy.start()
    with jax.named_scope('k2_wait'):
        pltpu.make_async_copy(stage_i, w_in_new, sem_i).wait()
        pltpu.make_async_copy(stage_o, w_out_new, sem_o).wait()
    for copy in stat_copies:
        copy.wait()


def solution(mesh):
    n_col = mesh.shape['col']
    n_row = mesh.shape['row']
    n_dev = n_col * n_row
    tile_in = P(None, 'row', 'col')
    tile_out = P(None, 'col', 'row')
    lane_row = P(None, None, 'row')
    lane_col = P(None, None, 'col')
    vec_row = P(None, 'row')
    vec_col = P(None, 'col')

    def local_step(hyper_params, w_in, x_in, dy_in, row_in, col_in, w_out, x_out, dy_out, row_out, col_out):
        layers, m_loc, n_loc = w_in.shape
        tokens = x_in.shape[1]
        n_mat = 2 * layers
        len_a, len_b = m_loc * n_row, n_loc * n_col
        dims = (n_col, n_row, layers, m_loc, n_loc, tokens, len_a, len_b)
        hbm = pl.BlockSpec(memory_space=pl.ANY)
        vmem = pl.BlockSpec(memory_space=pltpu.VMEM)
        mid = pl.pallas_call(
            functools.partial(stats_kernel, dims),
            out_shape=[
                pltpu.VMEM((layers, m_loc, n_loc), F32),
                pltpu.VMEM((layers, m_loc, n_loc), F32),
                pltpu.VMEM((layers, m_loc, n_loc), F32),
                pltpu.VMEM((layers, n_loc, m_loc), F32),
                pltpu.VMEM((n_mat, m_loc, 128), F32),
                pltpu.VMEM((n_mat, 1, n_loc), F32),
                pltpu.VMEM((1, 128), F32),
                pltpu.VMEM((2, layers, m_loc), F32),
                pltpu.VMEM((2, layers, n_loc), F32),
            ],
            in_specs=[hbm] * 11,
            out_specs=[vmem] * 9,
            scratch_shapes=[
                pltpu.SMEM((3,), F32),
                pltpu.VMEM((SLOTS, tokens, m_loc), BF16),
                pltpu.VMEM((SLOTS, tokens, n_loc), BF16),
                pltpu.VMEM((2, m_loc, tokens), BF16),
                pltpu.VMEM((2, m_loc, 128), F32),
                pltpu.VMEM((2, m_loc, 128), F32),
                pltpu.VMEM((n_mat, 1, m_loc), F32),
                pltpu.VMEM((n_mat, n_col, 1, m_loc), F32),
                pltpu.VMEM((n_mat, n_row, 1, n_loc), F32),
                pltpu.VMEM((n_dev, 1, 128), F32),
                pltpu.VMEM((1, 128), F32),
                pltpu.VMEM((layers, m_loc), F32),
                pltpu.VMEM((layers, n_loc), F32),
                pltpu.VMEM((layers, n_loc), F32),
                pltpu.VMEM((layers, m_loc), F32),
                pltpu.SemaphoreType.DMA((3,)),
                pltpu.SemaphoreType.DMA((LOOKAHEAD,)),
                pltpu.SemaphoreType.DMA((FIRST,)),
                pltpu.SemaphoreType.DMA((layers + 1,)),
                pltpu.SemaphoreType.DMA((3,)),
                pltpu.SemaphoreType.DMA((3,)),
                pltpu.SemaphoreType.DMA((2,)),
                pltpu.SemaphoreType.DMA((3,)),
                pltpu.SemaphoreType.DMA((1,)),
            ],
            compiler_params=pltpu.CompilerParams(collective_id=0, has_side_effects=True, vmem_limit_bytes=GRANT),
            name='adafactor_stats',
        )(*[pltpu.with_memory_space_constraint(item, pltpu.HBM) for item in (
            hyper_params, w_in, x_in, dy_in, row_in, col_in, w_out, x_out, dy_out, row_out, col_out)])
        mid = [pltpu.with_memory_space_constraint(item, pltpu.VMEM) for item in mid]
        out = pl.pallas_call(
            functools.partial(update_kernel, (layers, m_loc, n_loc)),
            out_shape=[
                jax.ShapeDtypeStruct(w_in.shape, F32),
                jax.ShapeDtypeStruct(row_in.shape, F32),
                jax.ShapeDtypeStruct(col_in.shape, F32),
                jax.ShapeDtypeStruct(w_out.shape, F32),
                jax.ShapeDtypeStruct(row_out.shape, F32),
                jax.ShapeDtypeStruct(col_out.shape, F32),
            ],
            in_specs=[vmem] * 9,
            out_specs=[hbm] * 6,
            scratch_shapes=[
                pltpu.VMEM((layers, m_loc, n_loc), F32),
                pltpu.VMEM((layers, n_loc, m_loc), F32),
                pltpu.SemaphoreType.DMA,
                pltpu.SemaphoreType.DMA,
                pltpu.SemaphoreType.DMA((4,)),
            ],
            compiler_params=pltpu.CompilerParams(vmem_limit_bytes=GRANT),
            name='adafactor_update',
        )(*mid)
        return tuple(out)

    return jax.shard_map(local_step, mesh=mesh, in_specs=(P(), tile_in, lane_row, lane_col, vec_row, vec_col, tile_out, lane_col, lane_row, vec_col, vec_row), out_specs=(tile_in, vec_row, vec_col, tile_out, vec_col, vec_row), check_vma=False)
```
